128 devices in a mesh: gx: 4 (over x_lo, core), gy: 4 (over y), gz: 8 (over z, x_hi).
Axes of the slice: x: 4 (x_hi: 2, x_lo: 2; x = x_hi * 2 + x_lo), y: 4, z: 4, core: 2. Of those that a mesh axis runs over, the one named last changes fastest.
Arguments:
- orbitals: float32 [64, 32, 32, 1024], P(None, 'gx', 'gy', 'gz'), may hold values from -6 to 6
- potential: float32 [32, 32, 1024], P('gx', 'gy', 'gz'), may hold values from 0 to 0.5
- centre: float32 [64], replicated, may hold values from 3 to 5
- half_width: float32 [64], replicated, may hold values from 3 to 5
Outputs:
- filtered: float32 [64, 32, 32, 1024], P(None, 'gx', 'gy', 'gz')
The draws below stay inside these ranges and needn't reach their ends.
All inputs are finite; a program needn't handle non-finite values.
Results may differ from the reference program's by a relative error of at most 0.00002.
Values sent between devices are 32-bit elements; how exact they have to be, the bound alone decides.
A program may use at most 64 MiB of HBM per device.

```python
import jax
import jax.numpy as jnp
from jax import lax

BANDS = 64
NX = 32
NY = 32
NZ = 1024


def block_levels(rng, shape, split, least, top_value):
    def one(axis_at, blocks):
        heights = jax.random.uniform(jax.random.fold_in(jax.random.fold_in(rng, 6), axis_at), (blocks,), jnp.float32, least / len(split), top_value / len(split))
        return jnp.repeat(jnp.exp(heights), shape[axis_at] // blocks).reshape((-1,) + (1,) * (len(shape) - axis_at - 1))

    level = one(*split[0])
    for cut in split[1:]:
        level = level * one(*cut)
    return level


def gaussian(stream_key, dims, scale, bound, split=(), dtype=jnp.bfloat16):
    result = jax.random.normal(stream_key, dims, jnp.float32) * scale
    if len(split) > 0:
        result = block_levels(stream_key, dims, split, -0.22, 0.18) * result
    return jnp.clip(result, min=-bound, max=bound).astype(dtype)


def setup_inputs(seed: int = 0) -> dict:
    key_of = jax.random.split(jax.random.key(seed), 5)
    orbitals = gaussian(key_of[0], (BANDS, NX, NY, NZ), 1.0, 6.0, ((1, 4), (2, 4), (3, 8)), jnp.float32)
    potential = jnp.clip(0.5 * jax.random.uniform(key_of[1], (NX, NY, NZ), jnp.float32) ** block_levels(key_of[1], (NX, NY, NZ), ((0, 4), (1, 4), (2, 8)), -0.2, 0.2), 0.0, 0.5)
    centre = jnp.clip(jax.random.uniform(key_of[2], (BANDS,), jnp.float32, 3.0, 5.0), 3.0, 5.0)
    half_width = jnp.clip(jax.random.uniform(key_of[3], (BANDS,), jnp.float32, 3.0, 5.0), 3.0, 5.0)
    return {"orbitals": orbitals, "potential": potential, "centre": centre, "half_width": half_width}


shift_mass = 0.05
jacobi_weight = 2.0 / 3.0


def neighbour_sum(field):
    total = jnp.roll(field, 1, 0) + jnp.roll(field, -1, 0)
    total = total + jnp.roll(field, 1, 1) + jnp.roll(field, -1, 1)
    return total + jnp.roll(field, 1, 2) + jnp.roll(field, -1, 2)


def operate(field, diagonal, coupling):
    return diagonal * field - coupling * neighbour_sum(field)


def restrict(field):
    shape = field.shape
    return 0.5 * field.reshape(shape[0] // 2, 2, shape[1] // 2, 2, shape[2] // 2, 2).sum(axis=(1, 3, 5))


def average_cells(field):
    shape = field.shape
    return 0.125 * field.reshape(shape[0] // 2, 2, shape[1] // 2, 2, shape[2] // 2, 2).sum(axis=(1, 3, 5))


def prolong(field):
    return jnp.repeat(jnp.repeat(jnp.repeat(field, 2, 0), 2, 1), 2, 2)


def relax(level, source, diagonal, coupling):
    return level + jacobi_weight * (source - operate(level, diagonal, coupling)) / diagonal


def reference(orbitals, potential, centre, half_width):
    potential_one = average_cells(potential)
    potential_two = average_cells(potential_one)
    diagonal_fine = 3.0 + potential
    diagonal_one = 0.75 + potential_one + shift_mass
    diagonal_two = 0.1875 + potential_two + shift_mass

    def one_band(packed):
        orbital, middle, spread = packed
        first_image = operate(orbital, diagonal_fine, 0.5)
        first_order = (first_image - middle * orbital) / spread
        second_image = operate(first_order, diagonal_fine, 0.5)
        second_order = 2.0 * (second_image - middle * first_order) / spread - orbital
        source_one = restrict(second_order)
        level_one = jacobi_weight * source_one / diagonal_one
        level_one = relax(level_one, source_one, diagonal_one, 0.125)
        residue = source_one - operate(level_one, diagonal_one, 0.125)
        source_two = restrict(residue)
        level_two = jacobi_weight * source_two / diagonal_two
        for sweep_index in range(2):
            level_two = relax(level_two, source_two, diagonal_two, 0.03125)
        level_one = level_one + prolong(level_two)
        level_one = relax(level_one, source_one, diagonal_one, 0.125)
        return second_order + prolong(level_one)

    return lax.map(one_band, (orbitals, centre, half_width))
```

```python
import jax
import jax.numpy as jnp
from jax import lax
from jax.experimental import pallas as pl
from jax.experimental.pallas import tpu as pltpu
from jax.sharding import PartitionSpec as P

MESH = pl.DeviceIdType.MESH
shift_mass = 0.05
jacobi_weight = 2.0 / 3.0
SUB, LANES = 8, 128
AXES = ("gx", "gy", "gz")
SIDES = (("gx", 1), ("gx", -1), ("gy", 1), ("gy", -1), ("gz", 1), ("gz", -1))


def lane():
    return lax.broadcasted_iota(jnp.int32, (SUB, LANES), 1)


def sublane():
    return lax.broadcasted_iota(jnp.int32, (SUB, LANES), 0)


def roll(value, shift):
    shift = shift % LANES
    return value if shift == 0 else pltpu.roll(value, shift, 1)


def turn(rows):
    at, rows = sublane(), list(rows)
    for d in (4, 2, 1):
        low = (at & d) == 0
        for i in range(SUB):
            if i & d == 0:
                a, b = rows[i], rows[i + d]
                rows[i] = jnp.where(low, a, pltpu.roll(b, d, 0))
                rows[i + d] = jnp.where(low, pltpu.roll(a, SUB - d, 0), b)
    return rows


def packed(total, value, start, width):
    at = lane()
    moved = roll(value, start + width // 2)
    if total is None:
        return moved
    return jnp.where((at >= start) & (at < start + width), moved, total)


def along_z(value, rims, start, width):
    at, half = lane(), width // 2
    outer = roll(rims, -(start + half))
    left = jnp.where(at < half, outer, roll(value, half))
    right = jnp.where(at >= LANES - half, outer, roll(value, -half))
    return left + right


def met(from_left, from_right, width):
    half = width // 2
    return jnp.where((lane() & half) != 0, roll(from_left, half), roll(from_right, -half))


def pair_sum(value, cell):
    at = lane()
    return value + jnp.where((at & cell) == 0, roll(value, -cell), roll(value, cell))


def kernel(bands, nx, ny, chunks, orb_hbm, pot_ref, mid_ref, half_ref, out_ref,
           stage, A, F, S2, DG, D1, W1, W2, D2, MID, INV, FZS, FZR,
           B1, U1a, U1b, U1c, V1, U2a, U2b, B2, X1S, X1R, Z1S, Z1R, X2S, X2R, Z2S, Z2R,
           in_sem, out_sem, fs, fr, as_, ar, bs, br):
    deep = bands // chunks
    inner = deep // SUB
    groups = bands // SUB
    cx, cy = nx // 2, ny // 2
    ex, ey = nx // 4, ny // 4
    peers = []
    for axis, step in SIDES:
        n = lax.axis_size(axis)
        peers.append({axis: lax.rem(lax.axis_index(axis) + (n + step), n)})

    def load(c):
        part = pl.ds(c * deep, deep)
        return pltpu.make_async_copy(orb_hbm.at[part], stage.at[part], in_sem.at[c])

    for c in range(chunks):
        load(c).start()
    barrier = pltpu.get_barrier_semaphore()
    for peer in peers:
        pl.semaphore_signal(barrier, inc=1, device_id=peer, device_id_type=MESH)

    def shape(value):
        return jnp.broadcast_to(value, (SUB, LANES))

    at = sublane()
    for g in range(groups):
        mid = jnp.full((SUB, LANES), mid_ref[g * SUB], jnp.float32)
        half = jnp.full((SUB, LANES), half_ref[g * SUB], jnp.float32)
        for s in range(1, SUB):
            mid = jnp.where(at == s, mid_ref[g * SUB + s], mid)
            half = jnp.where(at == s, half_ref[g * SUB + s], half)
        MID[g] = 3.0 - mid
        INV[g] = 1.0 / half
    ones = {}
    for X in range(cx):
        for Y in range(cy):
            total = None
            for dx in range(2):
                for dy in range(2):
                    k = (2 * X + dx) * ny + 2 * Y + dy
                    row = shape(pot_ref[pl.ds(k, 1), :])
                    DG[k] = row
                    total = row if total is None else total + row
            one = 0.125 * pair_sum(total, 1)
            ones[X, Y] = one
            diagonal = 0.75 + one + shift_mass
            D1[X * cy + Y] = diagonal
            W1[X * cy + Y] = jacobi_weight / diagonal
    for X in range(ex):
        for Y in range(ey):
            total = (ones[2 * X, 2 * Y] + ones[2 * X + 1, 2 * Y]) + (ones[2 * X, 2 * Y + 1] + ones[2 * X + 1, 2 * Y + 1])
            diagonal = 0.1875 + 0.125 * pair_sum(total, 2) + shift_mass
            D2[X * ey + Y] = diagonal
            W2[X * ey + Y] = jacobi_weight / diagonal

    def send(src, dst, s, r, d):
        return pltpu.make_async_remote_copy(
            src_ref=src, dst_ref=dst, send_sem=s, recv_sem=r, device_id=peers[d], device_id_type=MESH)

    def fine(buffer, rnd, c):
        ends = (
            (buffer.at[c, nx, pl.ds(1, ny)], buffer.at[c, 0, pl.ds(1, ny)]),
            (buffer.at[c, 1, pl.ds(1, ny)], buffer.at[c, nx + 1, pl.ds(1, ny)]),
            (buffer.at[c, pl.ds(1, nx), ny], buffer.at[c, pl.ds(1, nx), 0]),
            (buffer.at[c, pl.ds(1, nx), 1], buffer.at[c, pl.ds(1, nx), ny + 1]),
            (FZS.at[rnd, 0, c], FZR.at[rnd, 0, c]),
            (FZS.at[rnd, 1, c], FZR.at[rnd, 1, c]),
        )
        return [send(a, b, fs.at[rnd, c, d], fr.at[rnd, c, d], d) for d, (a, b) in enumerate(ends)]

    def fine_edges(rnd, c, totals):
        odd = (lane() & 1) != 0
        for i in range(inner // 2):
            a, b = totals[2 * i], totals[2 * i + 1]
            FZS[rnd, 0, c, i] = jnp.where(odd, roll(a, 1), b)
            FZS[rnd, 1, c, i] = jnp.where(odd, b, roll(a, -1))

    def fine_rims(rnd, c):
        odd = (lane() & 1) != 0
        rims = []
        for i in range(inner // 2):
            low, high = FZR[rnd, 0, c, i], FZR[rnd, 1, c, i]
            rims.append(jnp.where(odd, low, high))
            rims.append(jnp.where(odd, roll(low, 1), roll(high, -1)))
        return rims

    def start_fine(c):
        load(c).wait()
        totals = [None] * inner
        for j in range(inner):
            for x in range(nx):
                rows = turn([stage[c * deep + j * SUB + i, x * ny:(x + 1) * ny, :] for i in range(SUB)])
                for y in range(ny):
                    A[c, x + 1, y + 1, j * SUB:(j + 1) * SUB, :] = rows[y]
                    totals[j] = packed(totals[j], rows[y], 2 * (x * ny + y), 2)
        fine_edges(0, c, totals)

    def apply(buffer, c, x, y, j, rims):
        band = slice(j * SUB, (j + 1) * SUB)
        v = buffer[c, x + 1, y + 1, band, :]
        total = buffer[c, x, y + 1, band, :] + buffer[c, x + 2, y + 1, band, :]
        total = total + buffer[c, x + 1, y, band, :] + buffer[c, x + 1, y + 2, band, :]
        total = total + along_z(v, rims[j], 2 * (x * ny + y), 2)
        return v, (DG[x * ny + y] + MID[c * inner + j]) * v - 0.5 * total

    def first_pass(c):
        rims, totals = fine_rims(0, c), [None] * inner
        for j in range(inner):
            inv = INV[c * inner + j]
            for x in range(nx):
                for y in range(ny):
                    _, image = apply(A, c, x, y, j, rims)
                    value = image * inv
                    F[c, x + 1, y + 1, j * SUB:(j + 1) * SUB, :] = value
                    totals[j] = packed(totals[j], value, 2 * (x * ny + y), 2)
        fine_edges(1, c, totals)

    def faces(buffer, n, m, tile, count):
        even = (lane() & 1) == 0
        rows = pl.ds(tile, SUB)
        lines = ([(n, y) for y in range(1, m + 1)], [(1, y) for y in range(1, m + 1)],
                 [(x, m) for x in range(1, n + 1)], [(x, 1) for x in range(1, n + 1)])
        return [[jnp.where(even, buffer[l[2 * p][0], l[2 * p][1], rows, :], buffer[l[2 * p + 1][0], l[2 * p + 1][1], rows, :])
                 for p in range(count)] for l in lines]

    def unfaces(buffer, received, rnd, n, m, count, g):
        even = (lane() & 1) == 0
        rows = slice(g * SUB, (g + 1) * SUB)
        lines = ([(0, y) for y in range(1, m + 1)], [(n + 1, y) for y in range(1, m + 1)],
                 [(x, 0) for x in range(1, n + 1)], [(x, m + 1) for x in range(1, n + 1)])
        for d, l in enumerate(lines):
            for p in range(count):
                both = received[rnd, d, p, rows, :]
                buffer[l[2 * p][0], l[2 * p][1], rows, :] = jnp.where(even, both, roll(both, 1))
                buffer[l[2 * p + 1][0], l[2 * p + 1][1], rows, :] = jnp.where(even, roll(both, -1), both)

    def second_pass(c):
        rims = fine_rims(1, c)
        zs = None
        for j in range(inner):
            band = slice(j * SUB, (j + 1) * SUB)
            rows = pl.ds(c * deep + j * SUB, SUB)
            scale = 2.0 * INV[c * inner + j]
            for X in range(cx):
                for Y in range(cy):
                    total = None
                    for dx in range(2):
                        for dy in range(2):
                            x, y = 2 * X + dx, 2 * Y + dy
                            _, image = apply(F, c, x, y, j, rims)
                            value = image * scale - A[c, x + 1, y + 1, band, :]
                            S2[c, x, y, band, :] = value
                            total = value if total is None else total + value
                    source = 0.5 * pair_sum(total, 1)
                    B1[X * cy + Y, rows, :] = source
                    level = W1[X * cy + Y] * source
                    U1a[X + 1, Y + 1, rows, :] = level
                    zs = packed(zs, level, j * 64 + 4 * (X * cy + Y), 4)
            for d, line in enumerate(faces(U1a, cx, cy, c * deep + j * SUB, cy // 2)):
                for p, value in enumerate(line):
                    X1S[0, d, p, rows, :] = value
        Z1S[0, c] = zs

    def one_chunk(c):
        rows = pl.ds(c * deep, deep)
        copies = [send(X1S.at[0, d, :, rows], X1R.at[0, d, :, rows], as_.at[c, d], ar.at[c, d], d) for d in range(4)]
        return copies + [send(Z1S.at[0, c], Z1R.at[0, d - 4, c], as_.at[c, d], ar.at[c, d], d) for d in (4, 5)]

    def one(rnd):
        k = rnd - 1
        copies = [send(X1S.at[rnd, d], X1R.at[rnd, d], bs.at[k, d], br.at[k, d], d) for d in range(4)]
        return copies + [send(Z1S.at[rnd], Z1R.at[rnd, d - 4], bs.at[k, d], br.at[k, d], d) for d in (4, 5)]

    def two(rnd):
        k = 2 + rnd
        copies = [send(X2S.at[rnd, d], X2R.at[rnd, d], bs.at[k, d], br.at[k, d], d) for d in range(4)]
        return copies + [send(Z2S.at[rnd], Z2R.at[rnd, d - 4], bs.at[k, d], br.at[k, d], d) for d in (4, 5)]

    def around(buffer, X, Y, g, rims, start, width):
        rows = slice(g * SUB, (g + 1) * SUB)
        u = buffer[X + 1, Y + 1, rows, :]
        total = buffer[X, Y + 1, rows, :] + buffer[X + 2, Y + 1, rows, :]
        total = total + buffer[X + 1, Y, rows, :] + buffer[X + 1, Y + 2, rows, :]
        return u, total + along_z(u, rims, start, width)

    def send_faces(buffer, out, rnd, n, m, g):
        rows = slice(g * SUB, (g + 1) * SUB)
        for d, line in enumerate(faces(buffer, n, m, g * SUB, m // 2)):
            for p, value in enumerate(line):
                out[rnd, d, p, rows, :] = value

    def start1(g, X, Y):
        return (g % 2) * 64 + 4 * (X * cy + Y)

    def start2(g, X, Y):
        return (g % 4) * 32 + 8 * (X * ey + Y)

    def sweep_one(buffer, rnd, g, rims, put):
        rows = slice(g * SUB, (g + 1) * SUB)
        for X in range(cx):
            for Y in range(cy):
                u, total = around(buffer, X, Y, g, rims, start1(g, X, Y), 4)
                source = B1[X * cy + Y, rows, :]
                put(X, Y, u * (1.0 - jacobi_weight) + W1[X * cy + Y] * (source + 0.125 * total))

    pl.semaphore_wait(barrier, 6)

    @pl.loop(0, chunks)
    def _(c):
        start_fine(c)
        for copy in fine(A, 0, c):
            copy.start()

    @pl.loop(0, chunks)
    def _(c):
        for copy in fine(A, 0, c):
            copy.wait_recv()
        first_pass(c)
        for copy in fine(F, 1, c):
            copy.start()

    @pl.loop(0, chunks)
    def _(c):
        for copy in fine(F, 1, c):
            copy.wait_recv()
        second_pass(c)
        for copy in one_chunk(c):
            copy.start()

    for c in range(chunks):
        for copy in one_chunk(c):
            copy.wait_recv()
    zs = None
    for g in range(groups):
        rows = slice(g * SUB, (g + 1) * SUB)
        unfaces(U1a, X1R, 0, cx, cy, cy // 2, g)
        rims = met(Z1R[0, 0, g // 2], Z1R[0, 1, g // 2], 4)
        zs = None if g % 2 == 0 else zs
        for X in range(cx):
            for Y in range(cy):
                u, total = around(U1a, X, Y, g, rims, start1(g, X, Y), 4)
                value = u * (1.0 - jacobi_weight) + W1[X * cy + Y] * (B1[X * cy + Y, rows, :] + 0.125 * total)
                U1b[X + 1, Y + 1, rows, :] = value
                zs = packed(zs, value, start1(g, X, Y), 4)
        send_faces(U1b, X1S, 1, cx, cy, g)
        if g % 2 == 1:
            Z1S[1, g // 2] = zs
    for copy in one(1):
        copy.start()
    for copy in one(1):
        copy.wait_recv()
    for g in range(groups):
        rows = slice(g * SUB, (g + 1) * SUB)
        unfaces(U1b, X1R, 1, cx, cy, cy // 2, g)
        rims = met(Z1R[1, 0, g // 2], Z1R[1, 1, g // 2], 4)
        zs = None if g % 4 == 0 else zs
        for X in range(ex):
            for Y in range(ey):
                sums = None
                for dx in range(2):
                    for dy in range(2):
                        x, y = 2 * X + dx, 2 * Y + dy
                        u, total = around(U1b, x, y, g, rims, start1(g, x, y), 4)
                        residue = B1[x * cy + y, rows, :] - D1[x * cy + y] * u + 0.125 * total
                        sums = residue if sums is None else sums + residue
                source = 0.5 * pair_sum(sums, 2)
                B2[X * ey + Y, rows, :] = source
                level = W2[X * ey + Y] * source
                U2a[X + 1, Y + 1, rows, :] = level
                zs = packed(zs, level, start2(g, X, Y), 8)
        send_faces(U2a, X2S, 0, ex, ey, g)
        if g % 4 == 3:
            Z2S[0, g // 4] = zs
    for copy in two(0):
        copy.start()
    for copy in two(0):
        copy.wait_recv()
    for g in range(groups):
        rows = slice(g * SUB, (g + 1) * SUB)
        unfaces(U2a, X2R, 0, ex, ey, ey // 2, g)
        rims = met(Z2R[0, 0, g // 4], Z2R[0, 1, g // 4], 8)
        zs = None if g % 4 == 0 else zs
        for X in range(ex):
            for Y in range(ey):
                u, total = around(U2a, X, Y, g, rims, start2(g, X, Y), 8)
                value = u * (1.0 - jacobi_weight) + W2[X * ey + Y] * (B2[X * ey + Y, rows, :] + 0.03125 * total)
                U2b[X + 1, Y + 1, rows, :] = value
                zs = packed(zs, value, start2(g, X, Y), 8)
        send_faces(U2b, X2S, 1, ex, ey, g)
        if g % 4 == 3:
            Z2S[1, g // 4] = zs
    for copy in two(1):
        copy.start()
    for copy in two(1):
        copy.wait_recv()
    for g in range(groups):
        rows = slice(g * SUB, (g + 1) * SUB)
        unfaces(U2b, X2R, 1, ex, ey, ey // 2, g)
        rims = met(Z2R[1, 0, g // 4], Z2R[1, 1, g // 4], 8)
        zs = None if g % 2 == 0 else zs
        for X in range(ex):
            for Y in range(ey):
                u, total = around(U2b, X, Y, g, rims, start2(g, X, Y), 8)
                value = u * (1.0 - jacobi_weight) + W2[X * ey + Y] * (B2[X * ey + Y, rows, :] + 0.03125 * total)
                for dx in range(2):
                    for dy in range(2):
                        x, y = 2 * X + dx, 2 * Y + dy
                        level = U1b[x + 1, y + 1, rows, :] + value
                        U1c[x + 1, y + 1, rows, :] = level
                        zs = packed(zs, level, start1(g, x, y), 4)
        send_faces(U1c, X1S, 2, cx, cy, g)
        if g % 2 == 1:
            Z1S[2, g // 2] = zs
    for copy in one(2):
        copy.start()
    for copy in one(2):
        copy.wait_recv()
    for g in range(groups):
        rows = slice(g * SUB, (g + 1) * SUB)
        unfaces(U1c, X1R, 2, cx, cy, cy // 2, g)
        rims = met(Z1R[2, 0, g // 2], Z1R[2, 1, g // 2], 4)

        def keep(X, Y, value, rows=rows):
            V1[X * cy + Y, rows, :] = value

        sweep_one(U1c, 2, g, rims, keep)

    def store(c):
        part = pl.ds(c * deep, deep)
        return pltpu.make_async_copy(stage.at[part], out_ref.at[part], out_sem.at[c])

    @pl.loop(0, chunks)
    def _(c):
        for j in range(inner):
            rows = pl.ds(c * deep + j * SUB, SUB)
            for x in range(nx):
                values = turn([S2[c, x, y, j * SUB:(j + 1) * SUB, :] + V1[(x // 2) * cy + y // 2, rows, :] for y in range(ny)])
                for i in range(SUB):
                    stage[c * deep + j * SUB + i, x * ny:(x + 1) * ny, :] = values[i]
        store(c).start()

    for c in range(chunks):
        for copy in fine(A, 0, c) + fine(F, 1, c) + one_chunk(c):
            copy.wait_send()
        store(c).wait()
    for copy in one(1) + one(2) + two(0) + two(1):
        copy.wait_send()


def local(orbitals, potential, centre, half_width):
    bands, nx, ny, nz = orbitals.shape
    chunks = 4
    deep = bands // chunks
    cx, cy, ex, ey = nx // 2, ny // 2, nx // 4, ny // 4
    groups = bands // SUB
    vmem = lambda *s: pltpu.VMEM(s, jnp.float32)
    dma = lambda *s: pltpu.SemaphoreType.DMA(s)
    import functools

    out = pl.pallas_call(
        functools.partial(kernel, bands, nx, ny, chunks),
        name="filter_orbitals",
        out_shape=jax.ShapeDtypeStruct((bands, nx * ny, nz), jnp.float32),
        in_specs=[pl.BlockSpec(memory_space=pl.ANY), pl.BlockSpec(memory_space=pltpu.VMEM),
                  pl.BlockSpec(memory_space=pltpu.SMEM), pl.BlockSpec(memory_space=pltpu.SMEM)],
        out_specs=pl.BlockSpec(memory_space=pl.ANY),
        scratch_shapes=[
            vmem(bands, nx * ny, nz),
            vmem(chunks, nx + 2, ny + 2, deep, nz), vmem(chunks, nx + 2, ny + 2, deep, nz), vmem(chunks, nx, ny, deep, nz),
            vmem(nx * ny, SUB, nz), vmem(cx * cy, SUB, nz), vmem(cx * cy, SUB, nz), vmem(ex * ey, SUB, nz), vmem(ex * ey, SUB, nz),
            vmem(groups, SUB, nz), vmem(groups, SUB, nz),
            vmem(2, 2, chunks, deep // 16, SUB, nz), vmem(2, 2, chunks, deep // 16, SUB, nz),
            vmem(cx * cy, bands, nz),
            vmem(cx + 2, cy + 2, bands, nz), vmem(cx + 2, cy + 2, bands, nz), vmem(cx + 2, cy + 2, bands, nz),
            vmem(cx * cy, bands, nz),
            vmem(ex + 2, ey + 2, bands, nz), vmem(ex + 2, ey + 2, bands, nz), vmem(ex * ey, bands, nz),
            vmem(3, 4, cy // 2, bands, nz), vmem(3, 4, cy // 2, bands, nz),
            vmem(3, groups // 2, SUB, nz), vmem(3, 2, groups // 2, SUB, nz),
            vmem(2, 4, ey // 2, bands, nz), vmem(2, 4, ey // 2, bands, nz),
            vmem(2, groups // 4, SUB, nz), vmem(2, 2, groups // 4, SUB, nz),
            dma(chunks), dma(chunks), dma(2, chunks, 6), dma(2, chunks, 6), dma(chunks, 6), dma(chunks, 6),
            dma(4, 6), dma(4, 6),
        ],
        compiler_params=pltpu.CompilerParams(collective_id=0, has_side_effects=True, vmem_limit_bytes=48 * 1024 * 1024),
    )(orbitals.reshape(bands, nx * ny, nz), potential.reshape(nx * ny, nz), centre, half_width)
    return out.reshape(bands, nx, ny, nz)


def solution(mesh):
    in_specs = (P(None, "gx", "gy", "gz"), P("gx", "gy", "gz"), P(), P())
    out_specs = P(None, "gx", "gy", "gz")
    return jax.shard_map(local, mesh=mesh, in_specs=in_specs, out_specs=out_specs, check_vma=False)
```

```python
import functools

import jax
import jax.numpy as jnp
from jax import lax
from jax.experimental import pallas as pl
from jax.experimental.pallas import tpu as pltpu
from jax.sharding import PartitionSpec as P

MESH = pl.DeviceIdType.MESH
shift_mass = 0.05
jacobi_weight = 2.0 / 3.0
SUB, LANES = 8, 128
AXES = ("gx", "gy", "gz")
SIDES = (("gx", 1), ("gx", -1), ("gy", 1), ("gy", -1), ("gz", 1), ("gz", -1))


def lane():
    return lax.broadcasted_iota(jnp.int32, (SUB, LANES), 1)


def sublane():
    return lax.broadcasted_iota(jnp.int32, (SUB, LANES), 0)


def roll(value, shift):
    shift = shift % LANES
    return value if shift == 0 else pltpu.roll(value, shift, 1)


def turn(rows):
    at, rows = sublane(), list(rows)
    for d in (4, 2, 1):
        low = (at & d) == 0
        for i in range(SUB):
            if i & d == 0:
                a, b = rows[i], rows[i + d]
                rows[i] = jnp.where(low, a, pltpu.roll(b, d, 0))
                rows[i + d] = jnp.where(low, pltpu.roll(a, SUB - d, 0), b)
    return rows


def packed(total, value, start, width):
    at = lane()
    moved = roll(value, start + width // 2)
    if total is None:
        return moved
    return jnp.where((at >= start) & (at < start + width), moved, total)


def along_z(value, rims, start, width):
    at, half = lane(), width // 2
    outer = roll(rims, -(start + half))
    left = jnp.where(at < half, outer, roll(value, half))
    right = jnp.where(at >= LANES - half, outer, roll(value, -half))
    return left + right


def met(from_left, from_right, width):
    half = width // 2
    return jnp.where((lane() & half) != 0, roll(from_left, half), roll(from_right, -half))


def pair_sum(value, cell):
    at = lane()
    return value + jnp.where((at & cell) == 0, roll(value, -cell), roll(value, cell))


def kernel(bands, nx, ny, chunks, orb_hbm, pot_hbm, mid_hbm, half_hbm, out_ref,
           stage, pot_ref, mid_ref, half_ref, ZS, TS, A, F, S2, DG, D1, W1, W2, D2, MID, INV, FZS, FZR,
           B1, U1a, U1b, U1c, U2a, U2b, B2, X1S, X1R, Z1S, Z1R, X2S, X2R, Z2S, Z2R,
           in_sem, par_sem, fs, fr, as_, ar, bs, br):
    deep = bands // chunks
    inner = deep // SUB
    groups = bands // SUB
    cx, cy = nx // 2, ny // 2
    ex, ey = nx // 4, ny // 4
    peers = []
    for axis, step in SIDES:
        n = lax.axis_size(axis)
        peers.append({axis: lax.rem(lax.axis_index(axis) + (n + step), n)})

    def load(c):
        part = pl.ds(c * deep, deep)
        return pltpu.make_async_copy(orb_hbm.at[part], stage.at[part], in_sem.at[c])

    params = [pltpu.make_async_copy(a, b, par_sem.at[i])
              for i, (a, b) in enumerate(((pot_hbm, pot_ref), (mid_hbm, mid_ref), (half_hbm, half_ref)))]
    for copy in params:
        copy.start()
    for c in range(chunks):
        load(c).start()
    barrier = pltpu.get_barrier_semaphore()
    for peer in peers:
        pl.semaphore_signal(barrier, inc=1, device_id=peer, device_id_type=MESH)

    def shape(value):
        return jnp.broadcast_to(value, (SUB, LANES))

    for copy in params:
        copy.wait()
    at = sublane()
    for g in range(groups):
        mid = jnp.full((SUB, LANES), mid_ref[g * SUB], jnp.float32)
        half = jnp.full((SUB, LANES), half_ref[g * SUB], jnp.float32)
        for s in range(1, SUB):
            mid = jnp.where(at == s, mid_ref[g * SUB + s], mid)
            half = jnp.where(at == s, half_ref[g * SUB + s], half)
        MID[g] = 6.0 - 2.0 * mid
        INV[g] = 0.5 / half
    ones = {}
    for X in range(cx):
        for Y in range(cy):
            total = None
            for dx in range(2):
                for dy in range(2):
                    k = (2 * X + dx) * ny + 2 * Y + dy
                    row = shape(pot_ref[pl.ds(k, 1), :])
                    DG[k] = 2.0 * row
                    total = row if total is None else total + row
            one = 0.125 * pair_sum(total, 1)
            ones[X, Y] = one
            diagonal = 0.75 + one + shift_mass
            D1[X * cy + Y] = diagonal
            W1[X * cy + Y] = jacobi_weight / diagonal
    for X in range(ex):
        for Y in range(ey):
            total = (ones[2 * X, 2 * Y] + ones[2 * X + 1, 2 * Y]) + (ones[2 * X, 2 * Y + 1] + ones[2 * X + 1, 2 * Y + 1])
            diagonal = 0.1875 + 0.125 * pair_sum(total, 2) + shift_mass
            D2[X * ey + Y] = diagonal
            W2[X * ey + Y] = jacobi_weight / diagonal

    def send(src, dst, s, r, d):
        return pltpu.make_async_remote_copy(
            src_ref=src, dst_ref=dst, send_sem=s, recv_sem=r, device_id=peers[d], device_id_type=MESH)

    def fine(buffer, rnd, c):
        ends = (
            (buffer.at[c, nx, pl.ds(1, ny)], buffer.at[c, 0, pl.ds(1, ny)]),
            (buffer.at[c, 1, pl.ds(1, ny)], buffer.at[c, nx + 1, pl.ds(1, ny)]),
            (buffer.at[c, pl.ds(1, nx), ny], buffer.at[c, pl.ds(1, nx), 0]),
            (buffer.at[c, pl.ds(1, nx), 1], buffer.at[c, pl.ds(1, nx), ny + 1]),
            (FZS.at[rnd, 0, c], FZR.at[rnd, 0, c]),
            (FZS.at[rnd, 1, c], FZR.at[rnd, 1, c]),
        )
        return [send(a, b, fs.at[rnd, c, d], fr.at[rnd, c, d], d) for d, (a, b) in enumerate(ends)]

    def fine_edges(rnd, c, totals):
        odd = (lane() & 1) != 0
        for i in range(inner // 2):
            a, b = totals[2 * i], totals[2 * i + 1]
            FZS[rnd, 0, c, i] = jnp.where(odd, roll(a, 1), b)
            FZS[rnd, 1, c, i] = jnp.where(odd, b, roll(a, -1))

    def fine_rims(rnd, c):
        odd = (lane() & 1) != 0
        rims = []
        for i in range(inner // 2):
            low, high = FZR[rnd, 0, c, i], FZR[rnd, 1, c, i]
            rims.append(jnp.where(odd, low, high))
            rims.append(jnp.where(odd, roll(low, 1), roll(high, -1)))
        return rims

    def start_fine(c):
        load(c).wait()
        totals = [None] * inner
        for j in range(inner):
            for x in range(nx):
                rows = turn([stage[c * deep + j * SUB + i, x * ny:(x + 1) * ny, :] for i in range(SUB)])
                for y in range(ny):
                    A[c, x + 1, y + 1, j * SUB:(j + 1) * SUB, :] = rows[y]
                    totals[j] = packed(totals[j], rows[y], 2 * (x * ny + y), 2)
        fine_edges(0, c, totals)

    def fine_z(buffer, rnd, c):
        rims = fine_rims(rnd, c)
        for j in range(inner):
            band = slice(j * SUB, (j + 1) * SUB)
            for x in range(nx):
                for y in range(ny):
                    k = x * ny + y
                    ZS[k, band, :] = along_z(buffer[c, x + 1, y + 1, band, :], rims[j], 2 * k, 2)

    def apply(buffer, c, x, y, j):
        band = pl.ds(pl.multiple_of(j * SUB, SUB), SUB)
        v = buffer[c, x + 1, y + 1, band, :]
        total = buffer[c, x, y + 1, band, :] + buffer[c, x + 2, y + 1, band, :]
        total = total + buffer[c, x + 1, y, band, :] + buffer[c, x + 1, y + 2, band, :]
        total = total + ZS[x * ny + y, band, :]
        return (DG[x * ny + y] + MID[c * inner + j]) * v - total

    def first_pass(c):
        fine_z(A, 0, c)

        @pl.loop(0, inner)
        def _(j):
            inv = INV[c * inner + j]
            for x in range(nx):
                for y in range(ny):
                    F[c, x + 1, y + 1, pl.ds(pl.multiple_of(j * SUB, SUB), SUB), :] = apply(A, c, x, y, j) * inv

        totals = [None] * inner
        for j in range(inner):
            for x in range(nx):
                for y in range(ny):
                    totals[j] = packed(totals[j], F[c, x + 1, y + 1, j * SUB:(j + 1) * SUB, :], 2 * (x * ny + y), 2)
        fine_edges(1, c, totals)

    def faces(buffer, n, m, tile, count):
        even = (lane() & 1) == 0
        rows = pl.ds(tile, SUB)
        lines = ([(n, y) for y in range(1, m + 1)], [(1, y) for y in range(1, m + 1)],
                 [(x, m) for x in range(1, n + 1)], [(x, 1) for x in range(1, n + 1)])
        return [[jnp.where(even, buffer[l[2 * p][0], l[2 * p][1], rows, :], buffer[l[2 * p + 1][0], l[2 * p + 1][1], rows, :])
                 for p in range(count)] for l in lines]

    def unfaces(buffer, received, rnd, n, m, count, g):
        even = (lane() & 1) == 0
        rows = slice(g * SUB, (g + 1) * SUB)
        lines = ([(0, y) for y in range(1, m + 1)], [(n + 1, y) for y in range(1, m + 1)],
                 [(x, 0) for x in range(1, n + 1)], [(x, m + 1) for x in range(1, n + 1)])
        for d, l in enumerate(lines):
            for p in range(count):
                both = received[rnd, d, p, rows, :]
                buffer[l[2 * p][0], l[2 * p][1], rows, :] = jnp.where(even, both, roll(both, 1))
                buffer[l[2 * p + 1][0], l[2 * p + 1][1], rows, :] = jnp.where(even, roll(both, -1), both)

    def second_pass(c):
        fine_z(F, 1, c)

        @pl.loop(0, inner)
        def _(j):
            band = pl.ds(pl.multiple_of(j * SUB, SUB), SUB)
            scale = 2.0 * INV[c * inner + j]
            for X in range(cx):
                for Y in range(cy):
                    total = None
                    for dx in range(2):
                        for dy in range(2):
                            x, y = 2 * X + dx, 2 * Y + dy
                            value = apply(F, c, x, y, j) * scale - A[c, x + 1, y + 1, band, :]
                            S2[c, x, y, band, :] = value
                            total = value if total is None else total + value
                    TS[X * cy + Y, band, :] = total

        zs = None
        for j in range(inner):
            rows = pl.ds(pl.multiple_of(c * deep + j * SUB, SUB), SUB)
            for X in range(cx):
                for Y in range(cy):
                    source = 0.5 * pair_sum(TS[X * cy + Y, j * SUB:(j + 1) * SUB, :], 1)
                    B1[X * cy + Y, rows, :] = source
                    level = W1[X * cy + Y] * source
                    U1a[X + 1, Y + 1, rows, :] = level
                    zs = packed(zs, level, j * 64 + 4 * (X * cy + Y), 4)
            for d, line in enumerate(faces(U1a, cx, cy, c * deep + j * SUB, cy // 2)):
                for p, value in enumerate(line):
                    X1S[0, d, p, rows, :] = value
        Z1S[0, c] = zs

    def one_chunk(c):
        rows = pl.ds(c * deep, deep)
        copies = [send(X1S.at[0, d, :, rows], X1R.at[0, d, :, rows], as_.at[c, d], ar.at[c, d], d) for d in range(4)]
        return copies + [send(Z1S.at[0, c], Z1R.at[0, d - 4, c], as_.at[c, d], ar.at[c, d], d) for d in (4, 5)]

    def one(rnd):
        k = rnd - 1
        copies = [send(X1S.at[rnd, d], X1R.at[rnd, d], bs.at[k, d], br.at[k, d], d) for d in range(4)]
        return copies + [send(Z1S.at[rnd], Z1R.at[rnd, d - 4], bs.at[k, d], br.at[k, d], d) for d in (4, 5)]

    def two(rnd):
        k = 2 + rnd
        copies = [send(X2S.at[rnd, d], X2R.at[rnd, d], bs.at[k, d], br.at[k, d], d) for d in range(4)]
        return copies + [send(Z2S.at[rnd], Z2R.at[rnd, d - 4], bs.at[k, d], br.at[k, d], d) for d in (4, 5)]

    def tile(g):
        return pl.ds(g * SUB if isinstance(g, int) else pl.multiple_of(g * SUB, SUB), SUB)

    def coarse_z(buffer, received, rnd, n, m, width):
        per = LANES // (n * m * width)
        for g in range(groups):
            rims = met(received[rnd, 0, g // per], received[rnd, 1, g // per], width)
            for X in range(n):
                for Y in range(m):
                    start = (g % per) * n * m * width + width * (X * m + Y)
                    ZS[X * m + Y, tile(g), :] = along_z(buffer[X + 1, Y + 1, tile(g), :], rims, start, width)

    def coarse_edges(buffer, out, rnd, n, m, width):
        per = LANES // (n * m * width)
        for g in range(groups):
            zs = None if g % per == 0 else zs
            for X in range(n):
                for Y in range(m):
                    start = (g % per) * n * m * width + width * (X * m + Y)
                    zs = packed(zs, buffer[X + 1, Y + 1, tile(g), :], start, width)
            if g % per == per - 1:
                out[rnd, g // per] = zs

    def around(buffer, X, Y, m, g):
        rows = tile(g)
        u = buffer[X + 1, Y + 1, rows, :]
        total = buffer[X, Y + 1, rows, :] + buffer[X + 2, Y + 1, rows, :]
        total = total + buffer[X + 1, Y, rows, :] + buffer[X + 1, Y + 2, rows, :]
        return u, total + ZS[X * m + Y, rows, :]

    def send_faces(buffer, out, rnd, n, m, g):
        rows = tile(g)
        for d, line in enumerate(faces(buffer, n, m, rows.start, m // 2)):
            for p, value in enumerate(line):
                out[rnd, d, p, rows, :] = value

    def sweep_one(buffer, g, X, Y):
        u, total = around(buffer, X, Y, cy, g)
        return u * (1.0 - jacobi_weight) + W1[X * cy + Y] * (B1[X * cy + Y, tile(g), :] + 0.125 * total)

    def sweep_two(buffer, g, X, Y):
        u, total = around(buffer, X, Y, ey, g)
        return u * (1.0 - jacobi_weight) + W2[X * ey + Y] * (B2[X * ey + Y, tile(g), :] + 0.03125 * total)

    with jax.named_scope('barrier'):
        pl.semaphore_wait(barrier, 6)

    @pl.loop(0, chunks)
    def _(c):
        with jax.named_scope('load'):
            start_fine(c)
        for copy in fine(A, 0, c):
            copy.start()

    @pl.loop(0, chunks)
    def _(c):
        with jax.named_scope('w0'):
            for copy in fine(A, 0, c):
                copy.wait_recv()
        with jax.named_scope('first'):
            first_pass(c)
        for copy in fine(F, 1, c):
            copy.start()

    @pl.loop(0, chunks)
    def _(c):
        with jax.named_scope('w1'):
            for copy in fine(F, 1, c):
                copy.wait_recv()
        with jax.named_scope('second'):
            second_pass(c)
        for copy in one_chunk(c):
            copy.start()

    with jax.named_scope('w2'):
        for c in range(chunks):
            for copy in one_chunk(c):
                copy.wait_recv()
    for g in range(groups):
        unfaces(U1a, X1R, 0, cx, cy, cy // 2, g)
    coarse_z(U1a, Z1R, 0, cx, cy, 4)

    @pl.loop(0, groups)
    def _(g):
        for X in range(cx):
            for Y in range(cy):
                U1b[X + 1, Y + 1, tile(g), :] = sweep_one(U1a, g, X, Y)
        send_faces(U1b, X1S, 1, cx, cy, g)

    coarse_edges(U1b, Z1S, 1, cx, cy, 4)
    for copy in one(1):
        copy.start()
    with jax.named_scope('w3'):
        for copy in one(1):
            copy.wait_recv()
    for g in range(groups):
        unfaces(U1b, X1R, 1, cx, cy, cy // 2, g)
    coarse_z(U1b, Z1R, 1, cx, cy, 4)

    @pl.loop(0, groups)
    def _(g):
        for X in range(ex):
            for Y in range(ey):
                sums = None
                for dx in range(2):
                    for dy in range(2):
                        x, y = 2 * X + dx, 2 * Y + dy
                        u, total = around(U1b, x, y, cy, g)
                        residue = B1[x * cy + y, tile(g), :] - D1[x * cy + y] * u + 0.125 * total
                        sums = residue if sums is None else sums + residue
                B2[X * ey + Y, tile(g), :] = sums

    for g in range(groups):
        for X in range(ex):
            for Y in range(ey):
                source = 0.5 * pair_sum(B2[X * ey + Y, tile(g), :], 2)
                B2[X * ey + Y, tile(g), :] = source
                U2a[X + 1, Y + 1, tile(g), :] = W2[X * ey + Y] * source
        send_faces(U2a, X2S, 0, ex, ey, g)
    coarse_edges(U2a, Z2S, 0, ex, ey, 8)
    for copy in two(0):
        copy.start()
    with jax.named_scope('w4'):
        for copy in two(0):
            copy.wait_recv()
    for g in range(groups):
        unfaces(U2a, X2R, 0, ex, ey, ey // 2, g)
    coarse_z(U2a, Z2R, 0, ex, ey, 8)

    @pl.loop(0, groups)
    def _(g):
        for X in range(ex):
            for Y in range(ey):
                U2b[X + 1, Y + 1, tile(g), :] = sweep_two(U2a, g, X, Y)
        send_faces(U2b, X2S, 1, ex, ey, g)

    coarse_edges(U2b, Z2S, 1, ex, ey, 8)
    for copy in two(1):
        copy.start()
    with jax.named_scope('w5'):
        for copy in two(1):
            copy.wait_recv()
    for g in range(groups):
        unfaces(U2b, X2R, 1, ex, ey, ey // 2, g)
    coarse_z(U2b, Z2R, 1, ex, ey, 8)

    @pl.loop(0, groups)
    def _(g):
        for X in range(ex):
            for Y in range(ey):
                value = sweep_two(U2b, g, X, Y)
                for dx in range(2):
                    for dy in range(2):
                        x, y = 2 * X + dx, 2 * Y + dy
                        U1c[x + 1, y + 1, tile(g), :] = U1b[x + 1, y + 1, tile(g), :] + value
        send_faces(U1c, X1S, 2, cx, cy, g)

    coarse_edges(U1c, Z1S, 2, cx, cy, 4)
    for copy in one(2):
        copy.start()
    with jax.named_scope('w6'):
        for copy in one(2):
            copy.wait_recv()
    for g in range(groups):
        unfaces(U1c, X1R, 2, cx, cy, cy // 2, g)
    coarse_z(U1c, Z1R, 2, cx, cy, 4)

    @pl.loop(0, groups)
    def _(g):
        c, j = g // inner, g % inner
        band = pl.ds(pl.multiple_of(j * SUB, SUB), SUB)
        for X in range(cx):
            levels = [sweep_one(U1c, g, X, Y) for Y in range(cy)]
            for x in (2 * X, 2 * X + 1):
                values = turn([S2[c, x, y, band, :] + levels[y // 2] for y in range(ny)])
                for i in range(SUB):
                    out_ref[g * SUB + i, x * ny:(x + 1) * ny, :] = values[i]

    with jax.named_scope('sent'):
        for c in range(chunks):
            for copy in fine(A, 0, c) + fine(F, 1, c) + one_chunk(c):
                copy.wait_send()
        for copy in one(1) + one(2) + two(0) + two(1):
            copy.wait_send()


def local(orbitals, potential, centre, half_width):
    bands, nx, ny, nz = orbitals.shape
    chunks = 4
    deep = bands // chunks
    cx, cy, ex, ey = nx // 2, ny // 2, nx // 4, ny // 4
    groups = bands // SUB
    vmem = lambda *s: pltpu.VMEM(s, jnp.float32)
    dma = lambda *s: pltpu.SemaphoreType.DMA(s)
    out = pl.pallas_call(
        functools.partial(kernel, bands, nx, ny, chunks),
        name="filter_orbitals",
        out_shape=jax.ShapeDtypeStruct((bands, nx * ny, nz), jnp.float32),
        in_specs=[pl.BlockSpec(memory_space=pltpu.HBM)] * 4,
        out_specs=pl.BlockSpec(memory_space=pltpu.VMEM),
        scratch_shapes=[
            vmem(bands, nx * ny, nz), vmem(nx * ny, nz), pltpu.SMEM((bands,), jnp.float32), pltpu.SMEM((bands,), jnp.float32),
            vmem(nx * ny, bands, nz), vmem(cx * cy, deep, nz),
            vmem(chunks, nx + 2, ny + 2, deep, nz), vmem(chunks, nx + 2, ny + 2, deep, nz), vmem(chunks, nx, ny, deep, nz),
            vmem(nx * ny, SUB, nz), vmem(cx * cy, SUB, nz), vmem(cx * cy, SUB, nz), vmem(ex * ey, SUB, nz), vmem(ex * ey, SUB, nz),
            vmem(groups, SUB, nz), vmem(groups, SUB, nz),
            vmem(2, 2, chunks, deep // 16, SUB, nz), vmem(2, 2, chunks, deep // 16, SUB, nz),
            vmem(cx * cy, bands, nz),
            vmem(cx + 2, cy + 2, bands, nz), vmem(cx + 2, cy + 2, bands, nz), vmem(cx + 2, cy + 2, bands, nz),
            vmem(ex + 2, ey + 2, bands, nz), vmem(ex + 2, ey + 2, bands, nz), vmem(ex * ey, bands, nz),
            vmem(3, 4, cy // 2, bands, nz), vmem(3, 4, cy // 2, bands, nz),
            vmem(3, groups // 2, SUB, nz), vmem(3, 2, groups // 2, SUB, nz),
            vmem(2, 4, ey // 2, bands, nz), vmem(2, 4, ey // 2, bands, nz),
            vmem(2, groups // 4, SUB, nz), vmem(2, 2, groups // 4, SUB, nz),
            dma(chunks), dma(3), dma(2, chunks, 6), dma(2, chunks, 6), dma(chunks, 6), dma(chunks, 6),
            dma(4, 6), dma(4, 6),
        ],
        compiler_params=pltpu.CompilerParams(collective_id=0, has_side_effects=True, vmem_limit_bytes=48 * 1024 * 1024),
    )(*(pltpu.with_memory_space_constraint(a, pltpu.HBM) for a in (orbitals.reshape(bands, nx * ny, nz), potential.reshape(nx * ny, nz), centre, half_width)))
    return out.reshape(bands, nx, ny, nz)


def solution(mesh):
    in_specs = (P(None, "gx", "gy", "gz"), P("gx", "gy", "gz"), P(), P())
    out_specs = P(None, "gx", "gy", "gz")
    return jax.shard_map(local, mesh=mesh, in_specs=in_specs, out_specs=out_specs, check_vma=False)
```

```python
import functools

import jax
import jax.numpy as jnp
from jax import lax
from jax.experimental import pallas as pl
from jax.experimental.pallas import tpu as pltpu
from jax.sharding import PartitionSpec as P

MESH = pl.DeviceIdType.MESH
shift_mass = 0.05
jacobi_weight = 2.0 / 3.0
SUB, LANES = 8, 128
AXES = ("gx", "gy", "gz")
SIDES = (("gx", 1), ("gx", -1), ("gy", 1), ("gy", -1), ("gz", 1), ("gz", -1))
RING = ((1, 0), (-1, 0), (0, 1), (0, -1), (1, 1), (1, -1), (-1, 1), (-1, -1), (2, 0), (0, 2))
NEAR = RING[:8]
CROSS = RING[:4]
EDGE = 16


def lane():
    return lax.broadcasted_iota(jnp.int32, (SUB, LANES), 1)


def sublane():
    return lax.broadcasted_iota(jnp.int32, (SUB, LANES), 0)


def roll(value, shift):
    shift = shift % LANES
    return value if shift == 0 else pltpu.roll(value, shift, 1)


def turn(rows):
    at, rows = sublane(), list(rows)
    for d in (4, 2, 1):
        low = (at & d) == 0
        for i in range(SUB):
            if i & d == 0:
                a, b = rows[i], rows[i + d]
                rows[i] = jnp.where(low, a, pltpu.roll(b, d, 0))
                rows[i + d] = jnp.where(low, pltpu.roll(a, SUB - d, 0), b)
    return rows


def woven(columns):
    at = lane() & 3
    total = columns[3]
    for q in range(3):
        total = jnp.where(at == q, columns[q], total)
    return total


def spread(low, high, q):
    at = lane() & 3
    total = roll(high, 3 - q)
    for i, value in ((0, low), (1, low), (2, high)):
        total = jnp.where(at == i, roll(value, i - q), total)
    return total


def beside(own, low, high, bit):
    return jnp.where((lane() & bit) == 0, roll(own + low, -bit), roll(own + high, bit))


def below(main, other):
    return jnp.where(lane() < 4, roll(other, 4), roll(main, 4))


def above(main, other):
    return jnp.where(lane() >= LANES - 4, roll(other, -4), roll(main, -4))


def packed(total, value, start, width):
    at = lane()
    moved = roll(value, start + width // 2)
    if total is None:
        return moved
    return jnp.where((at >= start) & (at < start + width), moved, total)


def along_z(value, rims, start, width):
    at, half = lane(), width // 2
    outer = roll(rims, -(start + half))
    left = jnp.where(at < half, outer, roll(value, half))
    right = jnp.where(at >= LANES - half, outer, roll(value, -half))
    return left + right


def met(from_left, from_right, width):
    half = width // 2
    return jnp.where((lane() & half) != 0, roll(from_left, half), roll(from_right, -half))


def pair_sum(value, cell):
    at = lane()
    return value + jnp.where((at & cell) == 0, roll(value, -cell), roll(value, cell))


def kernel(bands, nx, ny, chunks, orb_hbm, pot_hbm, mid_hbm, half_hbm, out_ref,
           stage, pot_ref, mid_ref, half_ref, ZS, TS, A, F, S2, DG, D1, W1, MID, INV, FZS, FZR,
           B1, U1a, U1b, B2, X1S, X1R, Z1S, Z1R, MPS, MPR, WPS, WPR, EPS, EPR, XPR, XE, PA, PB, TT, TZ,
           in_sem, par_sem, sent, fine_got, one_got, got, got_w):
    deep = bands // chunks
    inner = deep // SUB
    groups = bands // SUB
    halves = 2
    share = groups // halves
    cx, cy = nx // 2, ny // 2
    ex, ey = nx // 4, ny // 4
    peers = []
    for axis, step in SIDES:
        n = lax.axis_size(axis)
        peers.append({axis: lax.rem(lax.axis_index(axis) + (n + step), n)})
    around_xy = []
    for step in RING:
        place = {}
        for axis, k in zip(AXES, step):
            n = lax.axis_size(axis)
            place[axis] = lax.rem(lax.axis_index(axis) + (n + k), n)
        around_xy.append(place)

    def load(c):
        part = pl.ds(c * deep, deep)
        return pltpu.make_async_copy(orb_hbm.at[part], stage.at[part], in_sem.at[c])

    params = [pltpu.make_async_copy(a, b, par_sem.at[i])
              for i, (a, b) in enumerate(((pot_hbm, pot_ref), (mid_hbm, mid_ref), (half_hbm, half_ref)))]
    for copy in params:
        copy.start()
    for c in range(chunks):
        load(c).start()
    barrier = pltpu.get_barrier_semaphore()
    for peer in peers + around_xy[4:]:
        pl.semaphore_signal(barrier, inc=1, device_id=peer, device_id_type=MESH)

    def shape(value):
        return jnp.broadcast_to(value, (SUB, LANES))

    def prologue():
        for copy in params:
            copy.wait()
        at = sublane()
        for g in range(groups):
            mid = jnp.full((SUB, LANES), mid_ref[g * SUB], jnp.float32)
            half = jnp.full((SUB, LANES), half_ref[g * SUB], jnp.float32)
            for s in range(1, SUB):
                mid = jnp.where(at == s, mid_ref[g * SUB + s], mid)
                half = jnp.where(at == s, half_ref[g * SUB + s], half)
            MID[g] = 6.0 - 2.0 * mid
            INV[g] = 0.5 / half
        ones = {}
        for X in range(cx):
            for Y in range(cy):
                total = None
                for dx in range(2):
                    for dy in range(2):
                        k = (2 * X + dx) * ny + 2 * Y + dy
                        row = shape(pot_ref[pl.ds(k, 1), :])
                        DG[k] = 2.0 * row
                        total = row if total is None else total + row
                one = 0.125 * pair_sum(total, 1)
                ones[X, Y] = one
                diagonal = 0.75 + one + shift_mass
                D1[X * cy + Y] = diagonal
                W1[X * cy + Y] = jacobi_weight / diagonal
        two_diagonals = []
        for X in range(ex):
            for Y in range(ey):
                total = (ones[2 * X, 2 * Y] + ones[2 * X + 1, 2 * Y]) + (ones[2 * X, 2 * Y + 1] + ones[2 * X + 1, 2 * Y + 1])
                diagonal = 0.1875 + 0.125 * pair_sum(total, 2) + shift_mass
                two_diagonals.append(jacobi_weight / diagonal)
        WPS[...] = woven(two_diagonals)

    def send(src, dst, s, r, d):
        return pltpu.make_async_remote_copy(
            src_ref=src, dst_ref=dst, send_sem=s, recv_sem=r, device_id=peers[d], device_id_type=MESH)

    def fine(buffer, rnd, c):
        ends = (
            (buffer.at[c, nx, pl.ds(1, ny)], buffer.at[c, 0, pl.ds(1, ny)]),
            (buffer.at[c, 1, pl.ds(1, ny)], buffer.at[c, nx + 1, pl.ds(1, ny)]),
            (buffer.at[c, pl.ds(1, nx), ny], buffer.at[c, pl.ds(1, nx), 0]),
            (buffer.at[c, pl.ds(1, nx), 1], buffer.at[c, pl.ds(1, nx), ny + 1]),
            (FZS.at[rnd, 0, c], FZR.at[rnd, 0, c]),
            (FZS.at[rnd, 1, c], FZR.at[rnd, 1, c]),
        )
        return [send(a, b, sent.at[d // 4], fine_got.at[rnd, c, d // 4], d) for d, (a, b) in enumerate(ends)]

    def whole(ref, sem):
        pltpu.make_async_copy(ref, ref, sem).wait()

    def fine_wait(rnd, c):
        whole(stage.at[pl.ds(0, 2 * deep * (nx + ny) // (nx * ny))], fine_got.at[rnd, c, 0])
        whole(FZR.at[rnd, :, c], fine_got.at[rnd, c, 1])

    def fine_edges(rnd, c, totals):
        odd = (lane() & 1) != 0
        for i in range(inner // 2):
            a, b = totals[2 * i], totals[2 * i + 1]
            FZS[rnd, 0, c, i] = jnp.where(odd, roll(a, 1), b)
            FZS[rnd, 1, c, i] = jnp.where(odd, b, roll(a, -1))

    def fine_rims(rnd, c):
        odd = (lane() & 1) != 0
        rims = []
        for i in range(inner // 2):
            low, high = FZR[rnd, 0, c, i], FZR[rnd, 1, c, i]
            rims.append(jnp.where(odd, low, high))
            rims.append(jnp.where(odd, roll(low, 1), roll(high, -1)))
        return rims

    def start_fine(c):
        load(c).wait()
        totals = [None] * inner
        for j in range(inner):
            for x in range(nx):
                rows = turn([stage[c * deep + j * SUB + i, x * ny:(x + 1) * ny, :] for i in range(SUB)])
                for y in range(ny):
                    A[c, x + 1, y + 1, j * SUB:(j + 1) * SUB, :] = rows[y]
                    totals[j] = packed(totals[j], rows[y], 2 * (x * ny + y), 2)
        fine_edges(0, c, totals)

    def fine_z(buffer, rnd, c):
        rims = fine_rims(rnd, c)
        for j in range(inner):
            band = slice(j * SUB, (j + 1) * SUB)
            for x in range(nx):
                for y in range(ny):
                    k = x * ny + y
                    ZS[k, band, :] = along_z(buffer[c, x + 1, y + 1, band, :], rims[j], 2 * k, 2)

    def apply(buffer, c, x, y, j):
        band = pl.ds(pl.multiple_of(j * SUB, SUB), SUB)
        v = buffer[c, x + 1, y + 1, band, :]
        total = buffer[c, x, y + 1, band, :] + buffer[c, x + 2, y + 1, band, :]
        total = total + buffer[c, x + 1, y, band, :] + buffer[c, x + 1, y + 2, band, :]
        total = total + ZS[x * ny + y, band, :]
        return (DG[x * ny + y] + MID[c * inner + j]) * v - total

    def first_pass(c):
        fine_z(A, 0, c)

        @pl.loop(0, inner)
        def _(j):
            inv = INV[c * inner + j]
            for x in range(nx):
                for y in range(ny):
                    F[c, x + 1, y + 1, pl.ds(pl.multiple_of(j * SUB, SUB), SUB), :] = apply(A, c, x, y, j) * inv

        totals = [None] * inner
        for j in range(inner):
            for x in range(nx):
                for y in range(ny):
                    totals[j] = packed(totals[j], F[c, x + 1, y + 1, j * SUB:(j + 1) * SUB, :], 2 * (x * ny + y), 2)
        fine_edges(1, c, totals)

    def faces(buffer, n, m, tile, count):
        even = (lane() & 1) == 0
        rows = pl.ds(tile, SUB)
        lines = ([(n, y) for y in range(1, m + 1)], [(1, y) for y in range(1, m + 1)],
                 [(x, m) for x in range(1, n + 1)], [(x, 1) for x in range(1, n + 1)])
        return [[jnp.where(even, buffer[l[2 * p][0], l[2 * p][1], rows, :], buffer[l[2 * p + 1][0], l[2 * p + 1][1], rows, :])
                 for p in range(count)] for l in lines]

    def unfaces(buffer, received, rnd, n, m, count, g):
        even = (lane() & 1) == 0
        rows = tile(g)
        lines = ([(0, y) for y in range(1, m + 1)], [(n + 1, y) for y in range(1, m + 1)],
                 [(x, 0) for x in range(1, n + 1)], [(x, m + 1) for x in range(1, n + 1)])
        for d, l in enumerate(lines):
            for p in range(count):
                both = received[rnd, d, p, rows, :]
                buffer[l[2 * p][0], l[2 * p][1], rows, :] = jnp.where(even, both, roll(both, 1))
                buffer[l[2 * p + 1][0], l[2 * p + 1][1], rows, :] = jnp.where(even, roll(both, -1), both)

    def second_pass(c):
        fine_z(F, 1, c)

        @pl.loop(0, inner)
        def _(j):
            band = pl.ds(pl.multiple_of(j * SUB, SUB), SUB)
            scale = 2.0 * INV[c * inner + j]
            for X in range(cx):
                for Y in range(cy):
                    total = None
                    for dx in range(2):
                        for dy in range(2):
                            x, y = 2 * X + dx, 2 * Y + dy
                            value = apply(F, c, x, y, j) * scale - A[c, x + 1, y + 1, band, :]
                            S2[c, x, y, band, :] = value
                            total = value if total is None else total + value
                    TS[X * cy + Y, band, :] = total

        zs = None
        for j in range(inner):
            rows = pl.ds(pl.multiple_of(c * deep + j * SUB, SUB), SUB)
            for X in range(cx):
                for Y in range(cy):
                    source = 0.5 * pair_sum(TS[X * cy + Y, j * SUB:(j + 1) * SUB, :], 1)
                    B1[X * cy + Y, rows, :] = source
                    level = W1[X * cy + Y] * source
                    U1a[X + 1, Y + 1, rows, :] = level
                    zs = packed(zs, level, j * 64 + 4 * (X * cy + Y), 4)
            for d, line in enumerate(faces(U1a, cx, cy, c * deep + j * SUB, cy // 2)):
                for p, value in enumerate(line):
                    X1S[0, d, p, rows, :] = value
        Z1S[0, c] = zs

    def one(rnd, c):
        rows = pl.ds(pl.multiple_of(c * deep, deep), deep)
        copies = [send(X1S.at[rnd, d, :, rows], X1R.at[rnd, d, :, rows], sent.at[2], one_got.at[rnd, c, 0], d)
                  for d in range(4)]
        return copies + [send(Z1S.at[rnd, c], Z1R.at[rnd, d - 4, c], sent.at[3], one_got.at[rnd, c, 1], d) for d in (4, 5)]

    def one_wait(rnd, c):
        rows = pl.ds(pl.multiple_of(c * deep, deep), deep)
        whole(X1R.at[rnd, :, :, rows], one_got.at[rnd, c, 0])
        whole(Z1R.at[rnd, :, c], one_got.at[rnd, c, 1])

    def slot(step):
        return RING.index(step) if step in RING else RING.index((abs(step[0]), abs(step[1])))

    def remote(src, dst, s, r, place):
        return pltpu.make_async_remote_copy(
            src_ref=src, dst_ref=dst, send_sem=s, recv_sem=r, device_id=place, device_id_type=MESH)

    def gather(h):
        copies = []
        for i, (a, b) in enumerate(RING):
            copies.append(remote(MPS.at[h], MPR.at[h, slot((-a, -b))], sent.at[4], got.at[h, 0], around_xy[i]))
        return copies

    def gather_diagonal():
        copies = []
        for i, (a, b) in enumerate(RING):
            copies.append(remote(WPS, WPR.at[slot((-a, -b))], sent.at[5], got_w, around_xy[i]))
        return copies

    def ends(h):
        return [send(EPS.at[h, d], EPR.at[h, d], sent.at[6], got.at[h, 1], 4 + d) for d in range(2)]

    def forward(h):
        copies = []
        for i, (a, b) in enumerate(NEAR):
            copies.append(remote(EPR.at[h], XPR.at[h, slot((-a, -b))], sent.at[7], got.at[h, 2], around_xy[i]))
        return copies

    def tile(g):
        return pl.ds(g * SUB if isinstance(g, int) else pl.multiple_of(g * SUB, SUB), SUB)

    def coarse_z(buffer, rnd, c):
        rims = met(Z1R[rnd, 0, c], Z1R[rnd, 1, c], 4)
        for j in range(inner):
            for X in range(cx):
                for Y in range(cy):
                    k = X * cy + Y
                    value = buffer[X + 1, Y + 1, tile(c * inner + j), :]
                    ZS[k, tile(c * inner + j), :] = along_z(value, rims, 4 * (j * cx * cy + k), 4)

    def coarse_edges(buffer, rnd, c):
        zs = None
        for j in range(inner):
            for X in range(cx):
                for Y in range(cy):
                    zs = packed(zs, buffer[X + 1, Y + 1, tile(c * inner + j), :], 4 * (j * cx * cy + X * cy + Y), 4)
        Z1S[rnd, c] = zs

    def around(buffer, X, Y, m, g):
        rows = tile(g)
        u = buffer[X + 1, Y + 1, rows, :]
        total = buffer[X, Y + 1, rows, :] + buffer[X + 2, Y + 1, rows, :]
        total = total + buffer[X + 1, Y, rows, :] + buffer[X + 1, Y + 2, rows, :]
        return u, total + ZS[X * m + Y, rows, :]

    def send_faces(buffer, out, rnd, n, m, g):
        rows = tile(g)
        for d, line in enumerate(faces(buffer, n, m, rows.start, m // 2)):
            for p, value in enumerate(line):
                out[rnd, d, p, rows, :] = value

    def sweep_one(buffer, g, X, Y):
        u, total = around(buffer, X, Y, cy, g)
        return u * (1.0 - jacobi_weight) + W1[X * cy + Y] * (B1[X * cy + Y, tile(g), :] + 0.125 * total)

    def level_two(h):
        at = lane()
        for b in range(9):
            low, high = (EPR[h, 0], EPR[h, 1]) if b == 8 else (XPR[h, b, 0], XPR[h, b, 1])
            for g in range(share + 1):
                XE[b, g] = jnp.where(at < EDGE, roll(high, -EDGE * g), roll(low, LANES - EDGE - EDGE * g))

        def main(step, g):
            if isinstance(g, int) and g == share:
                return WPS[...] if step == (0, 0) else WPR[slot(step)]
            return MPS[h, g] if step == (0, 0) else MPR[h, slot(step), g]

        def edge(step, g):
            return XE[8 if step == (0, 0) else slot(step), g]

        def know(step):
            return step == (0, 0) or step in RING or (abs(step[0]), abs(step[1])) in RING

        def total(value, other, near):
            x = beside(value, near(-1, 0), near(1, 0), 2)
            y = beside(value, near(0, -1), near(0, 1), 1)
            return x + y + (below(value, other) + above(value, other))

        own = (0, 0)
        first_main = (own,) + NEAR
        first_edge = (own,) + CROSS
        for g in range(share):
            start = {}
            for step in first_main + RING[8:]:
                start[step, 0] = main(step, share) * main(step, g)
            for step in first_main:
                start[step, 1] = edge(step, share) * edge(step, g)

            def near_of(step, part, value):
                def near(a, b):
                    there = (step[0] + a, step[1] + b)
                    there = there if know(there) else step
                    there = there if there == own or there in RING else (abs(there[0]), abs(there[1]))
                    return start.get((there, part), value)
                return near

            for n, step in enumerate(first_main):
                value, other = start[step, 0], start[step, 1]
                PA[g, n] = total(value, other, near_of(step, 0, value))
            for n, step in enumerate(first_edge):
                value, other = start[step, 1], start[step, 0]
                PA[g, 9 + n] = total(value, other, near_of(step, 1, value))

        @pl.loop(0, share)
        def _(g):
            for n, step in enumerate(first_main):
                w, b = main(step, share), main(step, g)
                PB[g, n] = (w * b) * (1.0 - jacobi_weight) + w * (b + 0.03125 * PA[g, n])
            for n, step in enumerate(first_edge):
                w, b = edge(step, share), edge(step, g)
                PB[g, 9 + n] = (w * b) * (1.0 - jacobi_weight) + w * (b + 0.03125 * PA[g, 9 + n])

        for g in range(share):
            def near_of(step, part, value):
                def near(a, b):
                    there = (step[0] + a, step[1] + b)
                    known = first_main if part == 0 else first_edge
                    return PB[g, 9 * part + known.index(there)] if there in known else value
                return near

            for n, step in enumerate(first_edge):
                value, other = PB[g, n], PB[g, 9 + n]
                PA[g, n] = total(value, other, near_of(step, 0, value))
            value, other = PB[g, 9], PB[g, 0]
            PA[g, 9] = total(value, other, near_of(own, 1, value))

        @pl.loop(0, share)
        def _(g):
            for n, step in enumerate(first_edge):
                w, b = main(step, share), main(step, g)
                PB[g, n] = PB[g, n] * (1.0 - jacobi_weight) + w * (b + 0.03125 * PA[g, n])
            w, b = edge(own, share), edge(own, g)
            PB[g, 9] = PB[g, 9] * (1.0 - jacobi_weight) + w * (b + 0.03125 * PA[g, 9])

        for g in range(share):
            value, other = PB[g, 0], PB[g, 9]
            PA[g, 0] = below(value, other)
            PA[g, 1] = above(value, other)
            for X in range(ex):
                for Y in range(ey):
                    TT[X + 1, Y + 1, tile(h * share + g), :] = spread(value, value, 2 * X + Y)
            for n, (a, b) in enumerate(CROSS):
                value = PB[g, 1 + n]
                for k in range(2):
                    X, Y = (k, 0) if a == 0 else (0, k)
                    X, Y = (1 if a < 0 else X), (1 if b < 0 else Y)
                    TT[2 * a + X + 1, 2 * b + Y + 1, tile(h * share + g), :] = spread(value, value, 2 * X + Y)
        for g in range(share):
            for q in range(ex * ey):
                TZ[q, tile(h * share + g), :] = spread(PA[g, 0], PA[g, 1], q)

    with jax.named_scope('barrier'):
        pl.semaphore_wait(barrier, 12)

    @pl.loop(0, chunks)
    def _(c):
        with jax.named_scope('load'):
            start_fine(c)
        for copy in fine(A, 0, c):
            copy.start()

    with jax.named_scope('prologue'):
        prologue()
    for copy in gather_diagonal():
        copy.start()

    @pl.loop(0, chunks)
    def _(c):
        with jax.named_scope('w0'):
            fine_wait(0, c)
        with jax.named_scope('first'):
            first_pass(c)
        for copy in fine(F, 1, c):
            copy.start()

    @pl.loop(0, chunks)
    def _(c):
        with jax.named_scope('w1'):
            fine_wait(1, c)
        with jax.named_scope('second'):
            second_pass(c)
        for copy in one(0, c):
            copy.start()

    @pl.loop(0, chunks)
    def _(c):
        with jax.named_scope('w2'):
            one_wait(0, c)
        with jax.named_scope('sweep'):
            for j in range(inner):
                unfaces(U1a, X1R, 0, cx, cy, cy // 2, c * inner + j)
            coarse_z(U1a, 0, c)

            @pl.loop(0, inner)
            def _(j):
                g = c * inner + j
                for X in range(cx):
                    for Y in range(cy):
                        U1b[X + 1, Y + 1, tile(g), :] = sweep_one(U1a, g, X, Y)
                send_faces(U1b, X1S, 1, cx, cy, g)

            coarse_edges(U1b, 1, c)
        for copy in one(1, c):
            copy.start()

    @pl.loop(0, halves)
    def _(h):
        @pl.loop(0, chunks // halves)
        def _(i):
            c = h * (chunks // halves) + i
            with jax.named_scope('w3'):
                one_wait(1, c)
            with jax.named_scope('residue'):
                for j in range(inner):
                    unfaces(U1b, X1R, 1, cx, cy, cy // 2, c * inner + j)
                coarse_z(U1b, 1, c)

                @pl.loop(0, inner)
                def _(j):
                    g = c * inner + j
                    for X in range(ex):
                        for Y in range(ey):
                            sums = None
                            for dx in range(2):
                                for dy in range(2):
                                    x, y = 2 * X + dx, 2 * Y + dy
                                    u, total = around(U1b, x, y, cy, g)
                                    residue = B1[x * cy + y, tile(g), :] - D1[x * cy + y] * u + 0.125 * total
                                    B1[x * cy + y, tile(g), :] = residue
                                    sums = residue if sums is None else sums + residue
                            B2[X * ey + Y, tile(g), :] = sums

        with jax.named_scope('weave'):
            parts = []
            for g in range(share):
                part = woven([0.5 * pair_sum(B2[q, tile(h * share + g), :], 2) for q in range(ex * ey)])
                MPS[h, g] = part
                parts.append(part)
            parts.append(WPS[...])
            low = high = None
            for g, part in enumerate(parts):
                here = (lane() >= EDGE * g) & (lane() < EDGE * (g + 1))
                up, down = roll(part, EDGE * g + EDGE), roll(part, EDGE * g)
                high = up if high is None else jnp.where(here, up, high)
                low = down if low is None else jnp.where(here, down, low)
            EPS[h, 0], EPS[h, 1] = high, low
        for copy in ends(h) + gather(h):
            copy.start()

    @pl.loop(0, halves)
    def _(h):
        with jax.named_scope('w4'):
            whole(EPR.at[h], got.at[h, 1])
        for copy in forward(h):
            copy.start()

    whole(WPR, got_w)

    def store(g):
        part = pl.ds(g * SUB, SUB)
        return pltpu.make_async_copy(stage.at[part], out_ref.at[part], sent.at[8])

    @pl.loop(0, halves)
    def _(h):
        with jax.named_scope('w5'):
            whole(MPR.at[h], got.at[h, 0])
            whole(XPR.at[h], got.at[h, 2])
        with jax.named_scope('two'):
            level_two(h)
        with jax.named_scope('last'):
            @pl.loop(0, share)
            def _(i):
                g = h * share + i
                c, j = g // inner, g % inner
                rows = tile(g)
                band = pl.ds(pl.multiple_of(j * SUB, SUB), SUB)
                for X in range(cx):
                    levels = []
                    for Y in range(cy):
                        k, q, r = X * cy + Y, X // 2 + 1, Y // 2 + 1
                        t = TT[q, r, rows, :]
                        outer = TT[q + 2 * (X % 2) - 1, r, rows, :] + TT[q, r + 2 * (Y % 2) - 1, rows, :]
                        outer = outer + TZ[(q - 1) * ey + r - 1, rows, :] + 3.0 * t
                        value = U1b[X + 1, Y + 1, rows, :] + t * (1.0 - jacobi_weight)
                        levels.append(value + W1[k] * (B1[k, rows, :] + 0.125 * outer))
                    for x in (2 * X, 2 * X + 1):
                        values = turn([S2[c, x, y, band, :] + levels[y // 2] for y in range(ny)])
                        for i in range(SUB):
                            stage[g * SUB + i, x * ny:(x + 1) * ny, :] = values[i]
                store(g).start()

    with jax.named_scope('sent'):
        whole(S2, sent.at[0])
        whole(FZS, sent.at[1])
        whole(X1S, sent.at[2])
        whole(Z1R, sent.at[3])
        whole(MPR, sent.at[4])
        whole(WPR, sent.at[5])
        whole(EPS, sent.at[6])
        whole(XPR, sent.at[7])
        whole(stage, sent.at[8])


def local(orbitals, potential, centre, half_width):
    bands, nx, ny, nz = orbitals.shape
    chunks = 4
    deep = bands // chunks
    cx, cy, ex, ey = nx // 2, ny // 2, nx // 4, ny // 4
    groups = bands // SUB
    vmem = lambda *s: pltpu.VMEM(s, jnp.float32)
    dma = lambda *s: pltpu.SemaphoreType.DMA(s)
    out = pl.pallas_call(
        functools.partial(kernel, bands, nx, ny, chunks),
        name="filter_orbitals",
        out_shape=jax.ShapeDtypeStruct((bands, nx * ny, nz), jnp.float32),
        in_specs=[pl.BlockSpec(memory_space=pltpu.HBM)] * 4,
        out_specs=pl.BlockSpec(memory_space=pl.ANY),
        scratch_shapes=[
            vmem(bands, nx * ny, nz), vmem(nx * ny, nz), pltpu.SMEM((bands,), jnp.float32), pltpu.SMEM((bands,), jnp.float32),
            vmem(nx * ny, bands, nz), vmem(cx * cy, deep, nz),
            vmem(chunks, nx + 2, ny + 2, deep, nz), vmem(chunks, nx + 2, ny + 2, deep, nz), vmem(chunks, nx, ny, deep, nz),
            vmem(nx * ny, SUB, nz), vmem(cx * cy, SUB, nz), vmem(cx * cy, SUB, nz),
            vmem(groups, SUB, nz), vmem(groups, SUB, nz),
            vmem(2, 2, chunks, deep // 16, SUB, nz), vmem(2, 2, chunks, deep // 16, SUB, nz),
            vmem(cx * cy, bands, nz),
            vmem(cx + 2, cy + 2, bands, nz), vmem(cx + 2, cy + 2, bands, nz), vmem(ex * ey, bands, nz),
            vmem(2, 4, cy // 2, bands, nz), vmem(2, 4, cy // 2, bands, nz),
            vmem(2, groups // 2, SUB, nz), vmem(2, 2, groups // 2, SUB, nz),
            vmem(2, groups // 2, SUB, nz), vmem(2, 10, groups // 2, SUB, nz), vmem(SUB, nz), vmem(10, SUB, nz),
            vmem(2, 2, SUB, nz), vmem(2, 2, SUB, nz), vmem(2, 8, 2, SUB, nz),
            vmem(9, groups // 2 + 1, SUB, nz), vmem(groups // 2, 14, SUB, nz), vmem(groups // 2, 14, SUB, nz),
            vmem(ex + 2, ey + 2, bands, nz), vmem(ex * ey, bands, nz),
            dma(chunks), dma(3), dma(9), dma(2, chunks, 2), dma(2, chunks, 2), dma(2, 3), pltpu.SemaphoreType.DMA,
        ],
        compiler_params=pltpu.CompilerParams(collective_id=0, has_side_effects=True, vmem_limit_bytes=48 * 1024 * 1024),
    )(*(pltpu.with_memory_space_constraint(a, pltpu.HBM) for a in (orbitals.reshape(bands, nx * ny, nz), potential.reshape(nx * ny, nz), centre, half_width)))
    return out.reshape(bands, nx, ny, nz)


def solution(mesh):
    in_specs = (P(None, "gx", "gy", "gz"), P("gx", "gy", "gz"), P(), P())
    out_specs = P(None, "gx", "gy", "gz")
    return jax.shard_map(local, mesh=mesh, in_specs=in_specs, out_specs=out_specs, check_vma=False)
```

```python
import functools

import jax
import jax.numpy as jnp
from jax import lax
from jax.experimental import pallas as pl
from jax.experimental.pallas import tpu as pltpu
from jax.sharding import PartitionSpec as P

MESH = pl.DeviceIdType.MESH
shift_mass = 0.05
jacobi_weight = 2.0 / 3.0
SUB, LANES = 8, 128
AXES = ("gx", "gy", "gz")
SIDES = (("gx", 1), ("gx", -1), ("gy", 1), ("gy", -1), ("gz", 1), ("gz", -1))
RING = ((1, 0), (-1, 0), (0, 1), (0, -1), (1, 1), (1, -1), (-1, 1), (-1, -1), (2, 0), (0, 2))
NEAR = RING[:8]
CROSS = RING[:4]
EDGE = 16


def lane():
    return lax.broadcasted_iota(jnp.int32, (SUB, LANES), 1)


def sublane():
    return lax.broadcasted_iota(jnp.int32, (SUB, LANES), 0)


def roll(value, shift):
    shift = shift % LANES
    return value if shift == 0 else pltpu.roll(value, shift, 1)


def turn(rows):
    at, rows = sublane(), list(rows)
    for d in (4, 2, 1):
        low = (at & d) == 0
        for i in range(SUB):
            if i & d == 0:
                a, b = rows[i], rows[i + d]
                rows[i] = jnp.where(low, a, pltpu.roll(b, d, 0))
                rows[i + d] = jnp.where(low, pltpu.roll(a, SUB - d, 0), b)
    return rows


def woven(columns):
    at = lane() & 3
    total = columns[3]
    for q in range(3):
        total = jnp.where(at == q, columns[q], total)
    return total


def spread(low, high, q):
    at = lane() & 3
    total = roll(high, 3 - q)
    for i, value in ((0, low), (1, low), (2, high)):
        total = jnp.where(at == i, roll(value, i - q), total)
    return total


def beside(own, low, high, bit):
    return jnp.where((lane() & bit) == 0, roll(own + low, -bit), roll(own + high, bit))


def below(main, other):
    return jnp.where(lane() < 4, roll(other, 4), roll(main, 4))


def above(main, other):
    return jnp.where(lane() >= LANES - 4, roll(other, -4), roll(main, -4))


def packed(total, value, start, width):
    at = lane()
    moved = roll(value, start + width // 2)
    if total is None:
        return moved
    return jnp.where((at >= start) & (at < start + width), moved, total)


def along_z(value, rims, start, width):
    at, half = lane(), width // 2
    outer = roll(rims, -(start + half))
    left = jnp.where(at < half, outer, roll(value, half))
    right = jnp.where(at >= LANES - half, outer, roll(value, -half))
    return left + right


def met(from_left, from_right, width):
    half = width // 2
    return jnp.where((lane() & half) != 0, roll(from_left, half), roll(from_right, -half))


def pair_sum(value, cell):
    at = lane()
    return value + jnp.where((at & cell) == 0, roll(value, -cell), roll(value, cell))


def kernel(bands, nx, ny, chunks, orb_hbm, pot_hbm, mid_hbm, half_hbm, out_ref,
           stage, pot_ref, mid_ref, half_ref, ZS, TS, A, F, S2, DG, D1, W1, MID, INV, FZS, FZR,
           B1, U1a, U1b, B2, X1S, X1R, Z1S, Z1R, MPS, MPR, WPS, WPR, EPS, EPR, XPR, XE, PA, PB, TT, TZ,
           in_sem, par_sem, sent, fine_got, one_got, got, got_w):
    deep = bands // chunks
    inner = deep // SUB
    groups = bands // SUB
    halves = 2
    share = groups // halves
    cx, cy = nx // 2, ny // 2
    ex, ey = nx // 4, ny // 4
    peers = []
    for axis, step in SIDES:
        n = lax.axis_size(axis)
        peers.append({axis: lax.rem(lax.axis_index(axis) + (n + step), n)})
    around_xy = []
    for step in RING:
        place = {}
        for axis, k in zip(AXES, step):
            n = lax.axis_size(axis)
            place[axis] = lax.rem(lax.axis_index(axis) + (n + k), n)
        around_xy.append(place)
    around_z = []
    for step in NEAR:
        for k in (1, -1):
            place = {}
            for axis, move in zip(AXES, step + (k,)):
                n = lax.axis_size(axis)
                place[axis] = lax.rem(lax.axis_index(axis) + (n + move), n)
            around_z.append(place)

    def load(c):
        part = pl.ds(c * deep, deep)
        return pltpu.make_async_copy(orb_hbm.at[part], stage.at[part], in_sem.at[c])

    params = [pltpu.make_async_copy(a, b, par_sem.at[i])
              for i, (a, b) in enumerate(((pot_hbm, pot_ref), (mid_hbm, mid_ref), (half_hbm, half_ref)))]
    for copy in params:
        copy.start()
    for c in range(chunks):
        load(c).start()
    barrier = pltpu.get_barrier_semaphore()
    for peer in peers:
        pl.semaphore_signal(barrier, inc=1, device_id=peer, device_id_type=MESH)

    def shape(value):
        return jnp.broadcast_to(value, (SUB, LANES))

    def prologue():
        for copy in params:
            copy.wait()
        at = sublane()
        for g in range(groups):
            mid = jnp.full((SUB, LANES), mid_ref[g * SUB], jnp.float32)
            half = jnp.full((SUB, LANES), half_ref[g * SUB], jnp.float32)
            for s in range(1, SUB):
                mid = jnp.where(at == s, mid_ref[g * SUB + s], mid)
                half = jnp.where(at == s, half_ref[g * SUB + s], half)
            MID[g] = 6.0 - 2.0 * mid
            INV[g] = 0.5 / half
        ones = {}
        for X in range(cx):
            for Y in range(cy):
                total = None
                for dx in range(2):
                    for dy in range(2):
                        k = (2 * X + dx) * ny + 2 * Y + dy
                        row = shape(pot_ref[pl.ds(k, 1), :])
                        DG[k] = 2.0 * row
                        total = row if total is None else total + row
                one = 0.125 * pair_sum(total, 1)
                ones[X, Y] = one
                diagonal = 0.75 + one + shift_mass
                D1[X * cy + Y] = diagonal
                W1[X * cy + Y] = jacobi_weight / diagonal
        two_diagonals = []
        for X in range(ex):
            for Y in range(ey):
                total = (ones[2 * X, 2 * Y] + ones[2 * X + 1, 2 * Y]) + (ones[2 * X, 2 * Y + 1] + ones[2 * X + 1, 2 * Y + 1])
                diagonal = 0.1875 + 0.125 * pair_sum(total, 2) + shift_mass
                two_diagonals.append(jacobi_weight / diagonal)
        WPS[...] = woven(two_diagonals)

    def send(src, dst, s, r, d):
        return pltpu.make_async_remote_copy(
            src_ref=src, dst_ref=dst, send_sem=s, recv_sem=r, device_id=peers[d], device_id_type=MESH)

    def fine(buffer, rnd, c):
        ends = (
            (buffer.at[c, nx, pl.ds(1, ny)], buffer.at[c, 0, pl.ds(1, ny)]),
            (buffer.at[c, 1, pl.ds(1, ny)], buffer.at[c, nx + 1, pl.ds(1, ny)]),
            (buffer.at[c, pl.ds(1, nx), ny], buffer.at[c, pl.ds(1, nx), 0]),
            (buffer.at[c, pl.ds(1, nx), 1], buffer.at[c, pl.ds(1, nx), ny + 1]),
            (FZS.at[rnd, 0, c], FZR.at[rnd, 0, c]),
            (FZS.at[rnd, 1, c], FZR.at[rnd, 1, c]),
        )
        return [send(a, b, sent.at[d // 4], fine_got.at[rnd, c, d // 4], d) for d, (a, b) in enumerate(ends)]

    def whole(ref, sem):
        pltpu.make_async_copy(ref, ref, sem).wait()

    def fine_wait(rnd, c):
        whole(stage.at[pl.ds(0, 2 * deep * (nx + ny) // (nx * ny))], fine_got.at[rnd, c, 0])
        whole(FZR.at[rnd, :, c], fine_got.at[rnd, c, 1])

    def fine_edges(rnd, c, totals):
        odd = (lane() & 1) != 0
        for i in range(inner // 2):
            a, b = totals[2 * i], totals[2 * i + 1]
            FZS[rnd, 0, c, i] = jnp.where(odd, roll(a, 1), b)
            FZS[rnd, 1, c, i] = jnp.where(odd, b, roll(a, -1))

    def fine_rims(rnd, c):
        odd = (lane() & 1) != 0
        rims = []
        for i in range(inner // 2):
            low, high = FZR[rnd, 0, c, i], FZR[rnd, 1, c, i]
            rims.append(jnp.where(odd, low, high))
            rims.append(jnp.where(odd, roll(low, 1), roll(high, -1)))
        return rims

    def start_fine(c):
        load(c).wait()
        totals = [None] * inner
        for j in range(inner):
            for x in range(nx):
                rows = turn([stage[c * deep + j * SUB + i, x * ny:(x + 1) * ny, :] for i in range(SUB)])
                for y in range(ny):
                    A[c, x + 1, y + 1, j * SUB:(j + 1) * SUB, :] = rows[y]
                    totals[j] = packed(totals[j], rows[y], 2 * (x * ny + y), 2)
        fine_edges(0, c, totals)

    def fine_z(buffer, rnd, c):
        rims = fine_rims(rnd, c)
        for j in range(inner):
            band = slice(j * SUB, (j + 1) * SUB)
            for x in range(nx):
                for y in range(ny):
                    k = x * ny + y
                    ZS[k, band, :] = along_z(buffer[c, x + 1, y + 1, band, :], rims[j], 2 * k, 2)

    def apply(buffer, c, x, y, j):
        band = pl.ds(pl.multiple_of(j * SUB, SUB), SUB)
        v = buffer[c, x + 1, y + 1, band, :]
        total = buffer[c, x, y + 1, band, :] + buffer[c, x + 2, y + 1, band, :]
        total = total + buffer[c, x + 1, y, band, :] + buffer[c, x + 1, y + 2, band, :]
        total = total + ZS[x * ny + y, band, :]
        return (DG[x * ny + y] + MID[c * inner + j]) * v - total

    def first_pass(c):
        fine_z(A, 0, c)

        @pl.loop(0, inner)
        def _(j):
            inv = INV[c * inner + j]
            for x in range(nx):
                for y in range(ny):
                    F[c, x + 1, y + 1, pl.ds(pl.multiple_of(j * SUB, SUB), SUB), :] = apply(A, c, x, y, j) * inv

        totals = [None] * inner
        for j in range(inner):
            for x in range(nx):
                for y in range(ny):
                    totals[j] = packed(totals[j], F[c, x + 1, y + 1, j * SUB:(j + 1) * SUB, :], 2 * (x * ny + y), 2)
        fine_edges(1, c, totals)

    def faces(buffer, n, m, tile, count):
        even = (lane() & 1) == 0
        rows = pl.ds(tile, SUB)
        lines = ([(n, y) for y in range(1, m + 1)], [(1, y) for y in range(1, m + 1)],
                 [(x, m) for x in range(1, n + 1)], [(x, 1) for x in range(1, n + 1)])
        return [[jnp.where(even, buffer[l[2 * p][0], l[2 * p][1], rows, :], buffer[l[2 * p + 1][0], l[2 * p + 1][1], rows, :])
                 for p in range(count)] for l in lines]

    def unfaces(buffer, received, rnd, n, m, count, g):
        even = (lane() & 1) == 0
        rows = tile(g)
        lines = ([(0, y) for y in range(1, m + 1)], [(n + 1, y) for y in range(1, m + 1)],
                 [(x, 0) for x in range(1, n + 1)], [(x, m + 1) for x in range(1, n + 1)])
        for d, l in enumerate(lines):
            for p in range(count):
                both = received[rnd, d, p, rows, :]
                buffer[l[2 * p][0], l[2 * p][1], rows, :] = jnp.where(even, both, roll(both, 1))
                buffer[l[2 * p + 1][0], l[2 * p + 1][1], rows, :] = jnp.where(even, roll(both, -1), both)

    def second_pass(c):
        fine_z(F, 1, c)

        @pl.loop(0, inner)
        def _(j):
            band = pl.ds(pl.multiple_of(j * SUB, SUB), SUB)
            scale = 2.0 * INV[c * inner + j]
            for X in range(cx):
                for Y in range(cy):
                    total = None
                    for dx in range(2):
                        for dy in range(2):
                            x, y = 2 * X + dx, 2 * Y + dy
                            value = apply(F, c, x, y, j) * scale - A[c, x + 1, y + 1, band, :]
                            S2[c, x, y, band, :] = value
                            total = value if total is None else total + value
                    TS[X * cy + Y, band, :] = total

        zs = None
        for j in range(inner):
            rows = pl.ds(pl.multiple_of(c * deep + j * SUB, SUB), SUB)
            for X in range(cx):
                for Y in range(cy):
                    source = 0.5 * pair_sum(TS[X * cy + Y, j * SUB:(j + 1) * SUB, :], 1)
                    B1[X * cy + Y, rows, :] = source
                    level = W1[X * cy + Y] * source
                    U1a[X + 1, Y + 1, rows, :] = level
                    zs = packed(zs, level, j * 64 + 4 * (X * cy + Y), 4)
            for d, line in enumerate(faces(U1a, cx, cy, c * deep + j * SUB, cy // 2)):
                for p, value in enumerate(line):
                    X1S[0, d, p, rows, :] = value
        Z1S[0, c] = zs

    def one(rnd, c):
        rows = pl.ds(pl.multiple_of(c * deep, deep), deep)
        copies = [send(X1S.at[rnd, d, :, rows], X1R.at[rnd, d, :, rows], sent.at[2], one_got.at[rnd, c, 0], d)
                  for d in range(4)]
        return copies + [send(Z1S.at[rnd, c], Z1R.at[rnd, d - 4, c], sent.at[3], one_got.at[rnd, c, 1], d) for d in (4, 5)]

    def one_wait(rnd, c):
        rows = pl.ds(pl.multiple_of(c * deep, deep), deep)
        whole(X1R.at[rnd, :, :, rows], one_got.at[rnd, c, 0])
        whole(Z1R.at[rnd, :, c], one_got.at[rnd, c, 1])

    def slot(step):
        return RING.index(step) if step in RING else RING.index((abs(step[0]), abs(step[1])))

    def remote(src, dst, s, r, place):
        return pltpu.make_async_remote_copy(
            src_ref=src, dst_ref=dst, send_sem=s, recv_sem=r, device_id=place, device_id_type=MESH)

    def gather(h):
        copies = []
        for i, (a, b) in enumerate(RING):
            copies.append(remote(MPS.at[h], MPR.at[h, slot((-a, -b))], sent.at[4], got.at[h, 0], around_xy[i]))
        return copies

    def gather_diagonal():
        copies = []
        for i, (a, b) in enumerate(RING):
            copies.append(remote(WPS, WPR.at[slot((-a, -b))], sent.at[5], got_w, around_xy[i]))
        return copies

    def ends(h):
        return [send(EPS.at[h, d], EPR.at[h, d], sent.at[6], got.at[h, 1], 4 + d) for d in range(2)]

    def ends_far(h):
        copies = []
        for i, (a, b) in enumerate(NEAR):
            for d in range(2):
                copies.append(remote(EPS.at[h, d], XPR.at[h, slot((-a, -b)), d], sent.at[7], got.at[h, 2],
                                     around_z[2 * i + d]))
        return copies

    def tile(g):
        return pl.ds(g * SUB if isinstance(g, int) else pl.multiple_of(g * SUB, SUB), SUB)

    def coarse_z(buffer, rnd, c):
        rims = met(Z1R[rnd, 0, c], Z1R[rnd, 1, c], 4)
        for j in range(inner):
            for X in range(cx):
                for Y in range(cy):
                    k = X * cy + Y
                    value = buffer[X + 1, Y + 1, tile(c * inner + j), :]
                    ZS[k, tile(c * inner + j), :] = along_z(value, rims, 4 * (j * cx * cy + k), 4)

    def coarse_edges(buffer, rnd, c):
        zs = None
        for j in range(inner):
            for X in range(cx):
                for Y in range(cy):
                    zs = packed(zs, buffer[X + 1, Y + 1, tile(c * inner + j), :], 4 * (j * cx * cy + X * cy + Y), 4)
        Z1S[rnd, c] = zs

    def around(buffer, X, Y, m, g):
        rows = tile(g)
        u = buffer[X + 1, Y + 1, rows, :]
        total = buffer[X, Y + 1, rows, :] + buffer[X + 2, Y + 1, rows, :]
        total = total + buffer[X + 1, Y, rows, :] + buffer[X + 1, Y + 2, rows, :]
        return u, total + ZS[X * m + Y, rows, :]

    def send_faces(buffer, out, rnd, n, m, g):
        rows = tile(g)
        for d, line in enumerate(faces(buffer, n, m, rows.start, m // 2)):
            for p, value in enumerate(line):
                out[rnd, d, p, rows, :] = value

    def sweep_one(buffer, g, X, Y):
        u, total = around(buffer, X, Y, cy, g)
        return u * (1.0 - jacobi_weight) + W1[X * cy + Y] * (B1[X * cy + Y, tile(g), :] + 0.125 * total)

    def level_two(h):
        at = lane()
        for b in range(9):
            low, high = (EPR[h, 0], EPR[h, 1]) if b == 8 else (XPR[h, b, 0], XPR[h, b, 1])
            for g in range(share + 1):
                XE[b, g] = jnp.where(at < EDGE, roll(high, -EDGE * g), roll(low, LANES - EDGE - EDGE * g))

        def main(step, g):
            if isinstance(g, int) and g == share:
                return WPS[...] if step == (0, 0) else WPR[slot(step)]
            return MPS[h, g] if step == (0, 0) else MPR[h, slot(step), g]

        def edge(step, g):
            return XE[8 if step == (0, 0) else slot(step), g]

        def know(step):
            return step == (0, 0) or step in RING or (abs(step[0]), abs(step[1])) in RING

        def total(value, other, near):
            x = beside(value, near(-1, 0), near(1, 0), 2)
            y = beside(value, near(0, -1), near(0, 1), 1)
            return x + y + (below(value, other) + above(value, other))

        own = (0, 0)
        first_main = (own,) + NEAR
        first_edge = (own,) + CROSS
        for g in range(share):
            start = {}
            for step in first_main + RING[8:]:
                start[step, 0] = main(step, share) * main(step, g)
            for step in first_main:
                start[step, 1] = edge(step, share) * edge(step, g)

            def near_of(step, part, value):
                def near(a, b):
                    there = (step[0] + a, step[1] + b)
                    there = there if know(there) else step
                    there = there if there == own or there in RING else (abs(there[0]), abs(there[1]))
                    return start.get((there, part), value)
                return near

            for n, step in enumerate(first_main):
                value, other = start[step, 0], start[step, 1]
                PA[g, n] = total(value, other, near_of(step, 0, value))
            for n, step in enumerate(first_edge):
                value, other = start[step, 1], start[step, 0]
                PA[g, 9 + n] = total(value, other, near_of(step, 1, value))

        @pl.loop(0, share)
        def _(g):
            for n, step in enumerate(first_main):
                w, b = main(step, share), main(step, g)
                PB[g, n] = (w * b) * (1.0 - jacobi_weight) + w * (b + 0.03125 * PA[g, n])
            for n, step in enumerate(first_edge):
                w, b = edge(step, share), edge(step, g)
                PB[g, 9 + n] = (w * b) * (1.0 - jacobi_weight) + w * (b + 0.03125 * PA[g, 9 + n])

        for g in range(share):
            def near_of(step, part, value):
                def near(a, b):
                    there = (step[0] + a, step[1] + b)
                    known = first_main if part == 0 else first_edge
                    return PB[g, 9 * part + known.index(there)] if there in known else value
                return near

            for n, step in enumerate(first_edge):
                value, other = PB[g, n], PB[g, 9 + n]
                PA[g, n] = total(value, other, near_of(step, 0, value))
            value, other = PB[g, 9], PB[g, 0]
            PA[g, 9] = total(value, other, near_of(own, 1, value))

        @pl.loop(0, share)
        def _(g):
            for n, step in enumerate(first_edge):
                w, b = main(step, share), main(step, g)
                PB[g, n] = PB[g, n] * (1.0 - jacobi_weight) + w * (b + 0.03125 * PA[g, n])
            w, b = edge(own, share), edge(own, g)
            PB[g, 9] = PB[g, 9] * (1.0 - jacobi_weight) + w * (b + 0.03125 * PA[g, 9])

        for g in range(share):
            value, other = PB[g, 0], PB[g, 9]
            PA[g, 0] = below(value, other)
            PA[g, 1] = above(value, other)
            for X in range(ex):
                for Y in range(ey):
                    TT[X + 1, Y + 1, tile(h * share + g), :] = spread(value, value, 2 * X + Y)
            for n, (a, b) in enumerate(CROSS):
                value = PB[g, 1 + n]
                for k in range(2):
                    X, Y = (k, 0) if a == 0 else (0, k)
                    X, Y = (1 if a < 0 else X), (1 if b < 0 else Y)
                    TT[2 * a + X + 1, 2 * b + Y + 1, tile(h * share + g), :] = spread(value, value, 2 * X + Y)
        for g in range(share):
            for q in range(ex * ey):
                TZ[q, tile(h * share + g), :] = spread(PA[g, 0], PA[g, 1], q)

    start_fine(0)
    with jax.named_scope('barrier'):
        pl.semaphore_wait(barrier, 6)
    for copy in fine(A, 0, 0):
        copy.start()

    @pl.loop(1, chunks)
    def _(c):
        with jax.named_scope('load'):
            start_fine(c)
        for copy in fine(A, 0, c):
            copy.start()

    with jax.named_scope('prologue'):
        prologue()

    @pl.loop(0, chunks)
    def _(c):
        with jax.named_scope('w0'):
            fine_wait(0, c)
        with jax.named_scope('first'):
            first_pass(c)
        for copy in fine(F, 1, c):
            copy.start()

    @pl.loop(0, chunks)
    def _(c):
        with jax.named_scope('w1'):
            fine_wait(1, c)
        with jax.named_scope('second'):
            second_pass(c)
        for copy in one(0, c):
            copy.start()

    for copy in gather_diagonal():
        copy.start()

    @pl.loop(0, chunks)
    def _(c):
        with jax.named_scope('w2'):
            one_wait(0, c)
        with jax.named_scope('sweep'):
            for j in range(inner):
                unfaces(U1a, X1R, 0, cx, cy, cy // 2, c * inner + j)
            coarse_z(U1a, 0, c)

            @pl.loop(0, inner)
            def _(j):
                g = c * inner + j
                for X in range(cx):
                    for Y in range(cy):
                        U1b[X + 1, Y + 1, tile(g), :] = sweep_one(U1a, g, X, Y)
                send_faces(U1b, X1S, 1, cx, cy, g)

            coarse_edges(U1b, 1, c)
        for copy in one(1, c):
            copy.start()

    @pl.loop(0, halves)
    def _(h):
        @pl.loop(0, chunks // halves)
        def _(i):
            c = h * (chunks // halves) + i
            with jax.named_scope('w3'):
                one_wait(1, c)
            with jax.named_scope('residue'):
                for j in range(inner):
                    unfaces(U1b, X1R, 1, cx, cy, cy // 2, c * inner + j)
                coarse_z(U1b, 1, c)

                @pl.loop(0, inner)
                def _(j):
                    g = c * inner + j
                    for X in range(ex):
                        for Y in range(ey):
                            sums = None
                            for dx in range(2):
                                for dy in range(2):
                                    x, y = 2 * X + dx, 2 * Y + dy
                                    u, total = around(U1b, x, y, cy, g)
                                    residue = B1[x * cy + y, tile(g), :] - D1[x * cy + y] * u + 0.125 * total
                                    B1[x * cy + y, tile(g), :] = residue
                                    sums = residue if sums is None else sums + residue
                            B2[X * ey + Y, tile(g), :] = sums

        with jax.named_scope('weave'):
            parts = []
            for g in range(share):
                part = woven([0.5 * pair_sum(B2[q, tile(h * share + g), :], 2) for q in range(ex * ey)])
                MPS[h, g] = part
                parts.append(part)
            parts.append(WPS[...])
            low = high = None
            for g, part in enumerate(parts):
                here = (lane() >= EDGE * g) & (lane() < EDGE * (g + 1))
                up, down = roll(part, EDGE * g + EDGE), roll(part, EDGE * g)
                high = up if high is None else jnp.where(here, up, high)
                low = down if low is None else jnp.where(here, down, low)
            EPS[h, 0], EPS[h, 1] = high, low
        for copy in ends_far(h) + ends(h) + gather(h):
            copy.start()

    whole(WPR, got_w)

    def store(g):
        part = pl.ds(g * SUB, SUB)
        return pltpu.make_async_copy(stage.at[part], out_ref.at[part], sent.at[8])

    @pl.loop(0, halves)
    def _(h):
        with jax.named_scope('w5'):
            whole(MPR.at[h], got.at[h, 0])
        with jax.named_scope('w6'):
            whole(EPR.at[h], got.at[h, 1])
            whole(XPR.at[h], got.at[h, 2])
        with jax.named_scope('two'):
            level_two(h)
        with jax.named_scope('last'):
            @pl.loop(0, share)
            def _(i):
                g = h * share + i
                c, j = g // inner, g % inner
                rows = tile(g)
                band = pl.ds(pl.multiple_of(j * SUB, SUB), SUB)
                for X in range(cx):
                    levels = []
                    for Y in range(cy):
                        k, q, r = X * cy + Y, X // 2 + 1, Y // 2 + 1
                        t = TT[q, r, rows, :]
                        outer = TT[q + 2 * (X % 2) - 1, r, rows, :] + TT[q, r + 2 * (Y % 2) - 1, rows, :]
                        outer = outer + TZ[(q - 1) * ey + r - 1, rows, :] + 3.0 * t
                        value = U1b[X + 1, Y + 1, rows, :] + t * (1.0 - jacobi_weight)
                        levels.append(value + W1[k] * (B1[k, rows, :] + 0.125 * outer))
                    for x in (2 * X, 2 * X + 1):
                        values = turn([S2[c, x, y, band, :] + levels[y // 2] for y in range(ny)])
                        for i in range(SUB):
                            stage[g * SUB + i, x * ny:(x + 1) * ny, :] = values[i]
                store(g).start()

    with jax.named_scope('sent'):
        whole(S2, sent.at[0])
        whole(FZS, sent.at[1])
        whole(X1S, sent.at[2])
        whole(Z1R, sent.at[3])
        whole(MPR, sent.at[4])
        whole(WPR, sent.at[5])
        whole(EPS, sent.at[6])
        whole(XPR, sent.at[7])
        whole(stage, sent.at[8])


def local(orbitals, potential, centre, half_width):
    bands, nx, ny, nz = orbitals.shape
    chunks = 4
    deep = bands // chunks
    cx, cy, ex, ey = nx // 2, ny // 2, nx // 4, ny // 4
    groups = bands // SUB
    vmem = lambda *s: pltpu.VMEM(s, jnp.float32)
    dma = lambda *s: pltpu.SemaphoreType.DMA(s)
    out = pl.pallas_call(
        functools.partial(kernel, bands, nx, ny, chunks),
        name="filter_orbitals",
        out_shape=jax.ShapeDtypeStruct((bands, nx * ny, nz), jnp.float32),
        in_specs=[pl.BlockSpec(memory_space=pltpu.HBM)] * 4,
        out_specs=pl.BlockSpec(memory_space=pl.ANY),
        scratch_shapes=[
            vmem(bands, nx * ny, nz), vmem(nx * ny, nz), pltpu.SMEM((bands,), jnp.float32), pltpu.SMEM((bands,), jnp.float32),
            vmem(nx * ny, bands, nz), vmem(cx * cy, deep, nz),
            vmem(chunks, nx + 2, ny + 2, deep, nz), vmem(chunks, nx + 2, ny + 2, deep, nz), vmem(chunks, nx, ny, deep, nz),
            vmem(nx * ny, SUB, nz), vmem(cx * cy, SUB, nz), vmem(cx * cy, SUB, nz),
            vmem(groups, SUB, nz), vmem(groups, SUB, nz),
            vmem(2, 2, chunks, deep // 16, SUB, nz), vmem(2, 2, chunks, deep // 16, SUB, nz),
            vmem(cx * cy, bands, nz),
            vmem(cx + 2, cy + 2, bands, nz), vmem(cx + 2, cy + 2, bands, nz), vmem(ex * ey, bands, nz),
            vmem(2, 4, cy // 2, bands, nz), vmem(2, 4, cy // 2, bands, nz),
            vmem(2, groups // 2, SUB, nz), vmem(2, 2, groups // 2, SUB, nz),
            vmem(2, groups // 2, SUB, nz), vmem(2, 10, groups // 2, SUB, nz), vmem(SUB, nz), vmem(10, SUB, nz),
            vmem(2, 2, SUB, nz), vmem(2, 2, SUB, nz), vmem(2, 8, 2, SUB, nz),
            vmem(9, groups // 2 + 1, SUB, nz), vmem(groups // 2, 14, SUB, nz), vmem(groups // 2, 14, SUB, nz),
            vmem(ex + 2, ey + 2, bands, nz), vmem(ex * ey, bands, nz),
            dma(chunks), dma(3), dma(9), dma(2, chunks, 2), dma(2, chunks, 2), dma(2, 3), pltpu.SemaphoreType.DMA,
        ],
        compiler_params=pltpu.CompilerParams(collective_id=0, has_side_effects=True, vmem_limit_bytes=48 * 1024 * 1024),
    )(*(pltpu.with_memory_space_constraint(a, pltpu.HBM) for a in (orbitals.reshape(bands, nx * ny, nz), potential.reshape(nx * ny, nz), centre, half_width)))
    return out.reshape(bands, nx, ny, nz)


def solution(mesh):
    in_specs = (P(None, "gx", "gy", "gz"), P("gx", "gy", "gz"), P(), P())
    out_specs = P(None, "gx", "gy", "gz")
    return jax.shard_map(local, mesh=mesh, in_specs=in_specs, out_specs=out_specs, check_vma=False)
```

```python
import functools

import jax
import jax.numpy as jnp
from jax import lax
from jax.experimental import pallas as pl
from jax.experimental.pallas import tpu as pltpu
from jax.sharding import PartitionSpec as P

MESH = pl.DeviceIdType.MESH
shift_mass = 0.05
jacobi_weight = 2.0 / 3.0
SUB, LANES = 8, 128
AXES = ("gx", "gy", "gz")
SIDES = (("gx", 1), ("gx", -1), ("gy", 1), ("gy", -1), ("gz", 1), ("gz", -1))
RING = ((1, 0), (-1, 0), (0, 1), (0, -1), (1, 1), (1, -1), (-1, 1), (-1, -1), (2, 0), (0, 2))
NEAR = RING[:8]
CROSS = RING[:4]
CORNERS = RING[4:8]
EDGE = 16


def lane():
    return lax.broadcasted_iota(jnp.int32, (SUB, LANES), 1)


def sublane():
    return lax.broadcasted_iota(jnp.int32, (SUB, LANES), 0)


def roll(value, shift):
    shift = shift % LANES
    return value if shift == 0 else pltpu.roll(value, shift, 1)


def turn(rows):
    at, rows = sublane(), list(rows)
    for d in (4, 2, 1):
        low = (at & d) == 0
        for i in range(SUB):
            if i & d == 0:
                a, b = rows[i], rows[i + d]
                rows[i] = jnp.where(low, a, pltpu.roll(b, d, 0))
                rows[i + d] = jnp.where(low, pltpu.roll(a, SUB - d, 0), b)
    return rows


def woven(columns):
    at = lane() & 3
    total = columns[3]
    for q in range(3):
        total = jnp.where(at == q, columns[q], total)
    return total


def spread(low, high, q):
    at = lane() & 3
    total = roll(high, 3 - q)
    for i, value in ((0, low), (1, low), (2, high)):
        total = jnp.where(at == i, roll(value, i - q), total)
    return total


def beside(own, low, high, bit):
    return jnp.where((lane() & bit) == 0, roll(own + low, -bit), roll(own + high, bit))


def below(main, other):
    return jnp.where(lane() < 4, roll(other, 4), roll(main, 4))


def above(main, other):
    return jnp.where(lane() >= LANES - 4, roll(other, -4), roll(main, -4))


def packed(total, value, start, width):
    at = lane()
    moved = roll(value, start + width // 2)
    if total is None:
        return moved
    return jnp.where((at >= start) & (at < start + width), moved, total)


def along_z(value, rims, start, width):
    at, half = lane(), width // 2
    outer = roll(rims, -(start + half))
    left = jnp.where(at < half, outer, roll(value, half))
    right = jnp.where(at >= LANES - half, outer, roll(value, -half))
    return left + right


def met(from_left, from_right, width):
    half = width // 2
    return jnp.where((lane() & half) != 0, roll(from_left, half), roll(from_right, -half))


def pair_sum(value, cell):
    at = lane()
    return value + jnp.where((at & cell) == 0, roll(value, -cell), roll(value, cell))


def kernel(bands, nx, ny, chunks, orb_hbm, pot_hbm, mid_hbm, half_hbm, out_ref,
           stage, pot_ref, mid_ref, half_ref, ZS, TS, A, F, S2, DG, D1, W1, MID, INV, FZS, FZR,
           B1, U1a, U1b, B2, X1S, X1R, Z1S, Z1R, CS, CR, ZD, W1R, WZS, WZR, HU, ZRING, MPS, MPR, WPS, WPR, EPS, EPR, XPR, XE, PA, PB, TT, TZ,
           in_sem, par_sem, sent, fine_got, one_got, got, got_w):
    third = 1.0 - jacobi_weight
    deep = bands // chunks
    inner = deep // SUB
    groups = bands // SUB
    halves = 2
    share = groups // halves
    cx, cy = nx // 2, ny // 2
    ex, ey = nx // 4, ny // 4
    peers = []
    for axis, step in SIDES:
        n = lax.axis_size(axis)
        peers.append({axis: lax.rem(lax.axis_index(axis) + (n + step), n)})
    around_xy = []
    for step in RING:
        place = {}
        for axis, k in zip(AXES, step):
            n = lax.axis_size(axis)
            place[axis] = lax.rem(lax.axis_index(axis) + (n + k), n)
        around_xy.append(place)
    around_z = []
    for step in NEAR:
        for k in (1, -1):
            place = {}
            for axis, move in zip(AXES, step + (k,)):
                n = lax.axis_size(axis)
                place[axis] = lax.rem(lax.axis_index(axis) + (n + move), n)
            around_z.append(place)

    def load(c):
        part = pl.ds(c * deep, deep)
        return pltpu.make_async_copy(orb_hbm.at[part], stage.at[part], in_sem.at[c])

    params = [pltpu.make_async_copy(a, b, par_sem.at[i])
              for i, (a, b) in enumerate(((pot_hbm, pot_ref), (mid_hbm, mid_ref), (half_hbm, half_ref)))]
    for copy in params:
        copy.start()
    for c in range(chunks):
        load(c).start()
    barrier = pltpu.get_barrier_semaphore()
    for peer in peers:
        pl.semaphore_signal(barrier, inc=1, device_id=peer, device_id_type=MESH)

    def shape(value):
        return jnp.broadcast_to(value, (SUB, LANES))

    def prologue():
        for copy in params:
            copy.wait()
        at = sublane()
        for g in range(groups):
            mid = jnp.full((SUB, LANES), mid_ref[g * SUB], jnp.float32)
            half = jnp.full((SUB, LANES), half_ref[g * SUB], jnp.float32)
            for s in range(1, SUB):
                mid = jnp.where(at == s, mid_ref[g * SUB + s], mid)
                half = jnp.where(at == s, half_ref[g * SUB + s], half)
            MID[g] = 6.0 - 2.0 * mid
            INV[g] = 0.5 / half
        ones = {}
        for X in range(cx):
            for Y in range(cy):
                total = None
                for dx in range(2):
                    for dy in range(2):
                        k = (2 * X + dx) * ny + 2 * Y + dy
                        row = shape(pot_ref[pl.ds(k, 1), :])
                        DG[k] = 2.0 * row
                        total = row if total is None else total + row
                one = 0.125 * pair_sum(total, 1)
                ones[X, Y] = one
                diagonal = 0.75 + one + shift_mass
                D1[X * cy + Y] = diagonal
                W1[X, Y] = jacobi_weight / diagonal
        two_diagonals = []
        for X in range(ex):
            for Y in range(ey):
                total = (ones[2 * X, 2 * Y] + ones[2 * X + 1, 2 * Y]) + (ones[2 * X, 2 * Y + 1] + ones[2 * X + 1, 2 * Y + 1])
                diagonal = 0.1875 + 0.125 * pair_sum(total, 2) + shift_mass
                two_diagonals.append(jacobi_weight / diagonal)
        WPS[...] = woven(two_diagonals)
        total = None
        for j in range(2):
            for k in range(cx * cy):
                total = packed(total, W1[k // cy, k % cy], 4 * (j * cx * cy + k), 4)
        WZS[...] = total

    def send(src, dst, s, r, d):
        return pltpu.make_async_remote_copy(
            src_ref=src, dst_ref=dst, send_sem=s, recv_sem=r, device_id=peers[d], device_id_type=MESH)

    def fine(buffer, rnd, c):
        ends = (
            (buffer.at[c, nx, pl.ds(1, ny)], buffer.at[c, 0, pl.ds(1, ny)]),
            (buffer.at[c, 1, pl.ds(1, ny)], buffer.at[c, nx + 1, pl.ds(1, ny)]),
            (buffer.at[c, pl.ds(1, nx), ny], buffer.at[c, pl.ds(1, nx), 0]),
            (buffer.at[c, pl.ds(1, nx), 1], buffer.at[c, pl.ds(1, nx), ny + 1]),
            (FZS.at[rnd, 0, c], FZR.at[rnd, 0, c]),
            (FZS.at[rnd, 1, c], FZR.at[rnd, 1, c]),
        )
        return [send(a, b, sent.at[d // 4], fine_got.at[rnd, c, d // 4], d) for d, (a, b) in enumerate(ends)]

    def whole(ref, sem):
        pltpu.make_async_copy(ref, ref, sem).wait()

    def fine_wait(rnd, c):
        whole(stage.at[pl.ds(0, 2 * deep * (nx + ny) // (nx * ny))], fine_got.at[rnd, c, 0])
        whole(FZR.at[rnd, :, c], fine_got.at[rnd, c, 1])

    def fine_edges(rnd, c, totals):
        odd = (lane() & 1) != 0
        for i in range(inner // 2):
            a, b = totals[2 * i], totals[2 * i + 1]
            FZS[rnd, 0, c, i] = jnp.where(odd, roll(a, 1), b)
            FZS[rnd, 1, c, i] = jnp.where(odd, b, roll(a, -1))

    def fine_rims(rnd, c):
        odd = (lane() & 1) != 0
        rims = []
        for i in range(inner // 2):
            low, high = FZR[rnd, 0, c, i], FZR[rnd, 1, c, i]
            rims.append(jnp.where(odd, low, high))
            rims.append(jnp.where(odd, roll(low, 1), roll(high, -1)))
        return rims

    def start_fine(c):
        load(c).wait()
        totals = [None] * inner
        for j in range(inner):
            for x in range(nx):
                rows = turn([stage[c * deep + j * SUB + i, x * ny:(x + 1) * ny, :] for i in range(SUB)])
                for y in range(ny):
                    A[c, x + 1, y + 1, j * SUB:(j + 1) * SUB, :] = rows[y]
                    totals[j] = packed(totals[j], rows[y], 2 * (x * ny + y), 2)
        fine_edges(0, c, totals)

    def fine_z(buffer, rnd, c):
        rims = fine_rims(rnd, c)
        for j in range(inner):
            band = slice(j * SUB, (j + 1) * SUB)
            for x in range(nx):
                for y in range(ny):
                    k = x * ny + y
                    ZS[k, band, :] = along_z(buffer[c, x + 1, y + 1, band, :], rims[j], 2 * k, 2)

    def apply(buffer, c, x, y, j):
        band = pl.ds(pl.multiple_of(j * SUB, SUB), SUB)
        v = buffer[c, x + 1, y + 1, band, :]
        total = buffer[c, x, y + 1, band, :] + buffer[c, x + 2, y + 1, band, :]
        total = total + buffer[c, x + 1, y, band, :] + buffer[c, x + 1, y + 2, band, :]
        total = total + ZS[x * ny + y, band, :]
        return (DG[x * ny + y] + MID[c * inner + j]) * v - total

    def first_pass(c):
        fine_z(A, 0, c)

        @pl.loop(0, inner)
        def _(j):
            inv = INV[c * inner + j]
            for x in range(nx):
                for y in range(ny):
                    F[c, x + 1, y + 1, pl.ds(pl.multiple_of(j * SUB, SUB), SUB), :] = apply(A, c, x, y, j) * inv

        totals = [None] * inner
        for j in range(inner):
            for x in range(nx):
                for y in range(ny):
                    totals[j] = packed(totals[j], F[c, x + 1, y + 1, j * SUB:(j + 1) * SUB, :], 2 * (x * ny + y), 2)
        fine_edges(1, c, totals)

    def second_pass(c):
        fine_z(F, 1, c)

        @pl.loop(0, inner)
        def _(j):
            band = pl.ds(pl.multiple_of(j * SUB, SUB), SUB)
            scale = 2.0 * INV[c * inner + j]
            for X in range(cx):
                for Y in range(cy):
                    total = None
                    for dx in range(2):
                        for dy in range(2):
                            x, y = 2 * X + dx, 2 * Y + dy
                            value = apply(F, c, x, y, j) * scale - A[c, x + 1, y + 1, band, :]
                            S2[c, x, y, band, :] = value
                            total = value if total is None else total + value
                    TS[X * cy + Y, band, :] = total

        totals = [None, None]
        for j in range(inner):
            rows = pl.ds(pl.multiple_of(c * deep + j * SUB, SUB), SUB)
            for X in range(cx):
                for Y in range(cy):
                    k = X * cy + Y
                    source = 0.5 * pair_sum(TS[k, j * SUB:(j + 1) * SUB, :], 1)
                    B1[k, rows, :] = source
                    level = W1[X, Y] * source
                    U1a[X + 2, Y + 2, rows, :] = level
                    start = 4 * (j * cx * cy + k)
                    moved = roll(level, start + 2)
                    here = ((lane() + (LANES - start + 2)) & (LANES - 1)) < 8
                    totals[k % 2] = moved if totals[k % 2] is None else jnp.where(here, moved, totals[k % 2])
            even = (lane() & 1) == 0
            for n in range(2):
                lines = ([(cx - 1 - n, y) for y in range(cy)], [(n, y) for y in range(cy)],
                         [(x, cy - 1 - n) for x in range(cx)], [(x, n) for x in range(cx)])
                for d, line in enumerate(lines):
                    for p in range(len(line) // 2):
                        (x0, y0), (x1, y1) = line[2 * p], line[2 * p + 1]
                        X1S[n, d, p, rows, :] = jnp.where(even, U1a[x0 + 2, y0 + 2, rows, :], U1a[x1 + 2, y1 + 2, rows, :])
        turn_even = (lane() & 4) == 0
        Z1S[c, 0] = jnp.where(turn_even, totals[0], totals[1])
        inward = [jnp.where((lane() & 2) == 0, roll(t, 2), roll(t, -2)) for t in totals]
        Z1S[c, 1] = jnp.where(turn_even, inward[0], inward[1])
        for i, (a, b) in enumerate(CORNERS):
            x, y = cx + 1 if a > 0 else 2, cy + 1 if b > 0 else 2
            CS[i, c] = jnp.where((lane() & 1) == 0, U1a[x, y, tile(c * inner), :], U1a[x, y, tile(c * inner + 1), :])

    def one(c):
        rows = pl.ds(pl.multiple_of(c * deep, deep), deep)
        copies = []
        for i, (a, b) in enumerate(CROSS):
            for d in range(2):
                copies.append(remote(Z1S.at[c, 0], ZD.at[slot((-a, -b)), d, c], sent.at[10], one_got.at[c, 3],
                                     around_z[2 * i + d]))
        copies += [send(Z1S.at[c], Z1R.at[d - 4, c], sent.at[3], one_got.at[c, 1], d) for d in (4, 5)]
        for i in range(4):
            copies.append(remote(CS.at[i, c], CR.at[i, c], sent.at[9], one_got.at[c, 2], around_xy[4 + i]))
        return copies + [send(X1S.at[:, d, :, rows], X1R.at[:, d, :, rows], sent.at[2], one_got.at[c, 0], d)
                         for d in range(4)]

    def diagonals():
        faces = (W1.at[cx - 1], W1.at[0], W1.at[:, cy - 1], W1.at[:, 0])
        copies = [send(face, W1R.at[d ^ 1], sent.at[11], got_w.at[1], d) for d, face in enumerate(faces)]
        return copies + [send(WZS, WZR.at[d - 4], sent.at[12], got_w.at[2], d) for d in (4, 5)]

    def slot(step):
        return RING.index(step) if step in RING else RING.index((abs(step[0]), abs(step[1])))

    def remote(src, dst, s, r, place):
        return pltpu.make_async_remote_copy(
            src_ref=src, dst_ref=dst, send_sem=s, recv_sem=r, device_id=place, device_id_type=MESH)

    def gather(h):
        copies = []
        for i, (a, b) in enumerate(RING):
            copies.append(remote(MPS.at[h], MPR.at[h, slot((-a, -b))], sent.at[4], got.at[h, 0], around_xy[i]))
        return copies

    def gather_diagonal():
        copies = []
        for i, (a, b) in enumerate(RING):
            copies.append(remote(WPS, WPR.at[slot((-a, -b))], sent.at[5], got_w.at[0], around_xy[i]))
        return copies

    def ends(h):
        return [send(EPS.at[h, d], EPR.at[h, d], sent.at[6], got.at[h, 1], 4 + d) for d in range(2)]

    def ends_far(h):
        copies = []
        for i, (a, b) in enumerate(NEAR):
            for d in range(2):
                copies.append(remote(EPS.at[h, d], XPR.at[h, slot((-a, -b)), d], sent.at[7], got.at[h, 2],
                                     around_z[2 * i + d]))
        return copies

    def tile(g):
        return pl.ds(g * SUB if isinstance(g, int) else pl.multiple_of(g * SUB, SUB), SUB)

    def coarse_z(buffer, at, rims, c):
        for j in range(inner):
            for X in range(cx):
                for Y in range(cy):
                    k = X * cy + Y
                    value = buffer[X + at, Y + at, tile(c * inner + j), :]
                    ZS[k, tile(c * inner + j), :] = along_z(value, rims, 4 * (j * cx * cy + k), 4)

    def unpack_faces(c):
        even = (lane() & 1) == 0
        for j in range(inner):
            rows = tile(c * inner + j)
            for n in range(2):
                lines = ([(1 - n, y + 2) for y in range(cy)], [(cx + 2 + n, y + 2) for y in range(cy)],
                         [(x + 2, 1 - n) for x in range(cx)], [(x + 2, cy + 2 + n) for x in range(cx)])
                for d, line in enumerate(lines):
                    for p in range(len(line) // 2):
                        both = X1R[n, d, p, rows, :]
                        (x0, y0), (x1, y1) = line[2 * p], line[2 * p + 1]
                        U1a[x0, y0, rows, :] = jnp.where(even, both, roll(both, 1))
                        U1a[x1, y1, rows, :] = jnp.where(even, roll(both, -1), both)
        for i, (a, b) in enumerate(CORNERS):
            both = CR[i, c]
            x, y = 1 if a > 0 else cx + 2, 1 if b > 0 else cy + 2
            U1a[x, y, tile(c * inner), :] = jnp.where(even, both, roll(both, 1))
            U1a[x, y, tile(c * inner + 1), :] = jnp.where(even, roll(both, -1), both)

    def ring(i, t):
        return (((cx, t), t), ((-1, t), (cx - 1) * cy + t), ((t, cy), t * cy), ((t, -1), t * cy + cy - 1))[i]

    def outside(c):
        rims = [met(ZD[i, 0, c], ZD[i, 1, c], 4) for i in range(4)]
        for j in range(inner):
            for i in range(4):
                for t in range(4):
                    (x, y), k = ring(i, t)
                    value = U1a[x + 2, y + 2, tile(c * inner + j), :]
                    ZRING[4 * i + t, j * SUB:(j + 1) * SUB, :] = along_z(value, rims[i], 4 * (j * cx * cy + k), 4)
        own = met(Z1R[0, c, 0], Z1R[1, c, 0], 4)
        X, Y = (lane() >> 4) & 3, (lane() >> 2) & 3
        total = jnp.where(X == 0, roll(rims[1], -48), roll(own, 16)) + jnp.where(X == 3, roll(rims[0], 48), roll(own, -16))
        total = total + jnp.where(Y == 0, roll(rims[3], -12), roll(own, 4)) + jnp.where(Y == 3, roll(rims[2], 12), roll(own, -4))
        total = total + Z1S[c, 0] + met(Z1R[0, c, 1], Z1R[1, c, 1], 4)
        HU[c] = own * (1.0 + third) + 0.125 * met(WZR[0], WZR[1], 4) * total

    def beside_xy(buffer, x, y, rows):
        total = buffer[x - 1, y, rows, :] + buffer[x + 1, y, rows, :]
        return total + buffer[x, y - 1, rows, :] + buffer[x, y + 1, rows, :]

    def level_two(h):
        at = lane()
        for b in range(9):
            low, high = (EPR[h, 0], EPR[h, 1]) if b == 8 else (XPR[h, b, 0], XPR[h, b, 1])
            for g in range(share + 1):
                XE[b, g] = jnp.where(at < EDGE, roll(high, -EDGE * g), roll(low, LANES - EDGE - EDGE * g))

        def main(step, g):
            if isinstance(g, int) and g == share:
                return WPS[...] if step == (0, 0) else WPR[slot(step)]
            return MPS[h, g] if step == (0, 0) else MPR[h, slot(step), g]

        def edge(step, g):
            return XE[8 if step == (0, 0) else slot(step), g]

        def know(step):
            return step == (0, 0) or step in RING or (abs(step[0]), abs(step[1])) in RING

        def total(value, other, near):
            x = beside(value, near(-1, 0), near(1, 0), 2)
            y = beside(value, near(0, -1), near(0, 1), 1)
            return x + y + (below(value, other) + above(value, other))

        own = (0, 0)
        first_main = (own,) + NEAR
        first_edge = (own,) + CROSS
        for g in range(share):
            start = {}
            for step in first_main + RING[8:]:
                start[step, 0] = main(step, share) * main(step, g)
            for step in first_main:
                start[step, 1] = edge(step, share) * edge(step, g)

            def near_of(step, part, value):
                def near(a, b):
                    there = (step[0] + a, step[1] + b)
                    there = there if know(there) else step
                    there = there if there == own or there in RING else (abs(there[0]), abs(there[1]))
                    return start.get((there, part), value)
                return near

            for n, step in enumerate(first_main):
                value, other = start[step, 0], start[step, 1]
                PA[g, n] = total(value, other, near_of(step, 0, value))
            for n, step in enumerate(first_edge):
                value, other = start[step, 1], start[step, 0]
                PA[g, 9 + n] = total(value, other, near_of(step, 1, value))

        @pl.loop(0, share)
        def _(g):
            for n, step in enumerate(first_main):
                w, b = main(step, share), main(step, g)
                PB[g, n] = (w * b) * (1.0 - jacobi_weight) + w * (b + 0.03125 * PA[g, n])
            for n, step in enumerate(first_edge):
                w, b = edge(step, share), edge(step, g)
                PB[g, 9 + n] = (w * b) * (1.0 - jacobi_weight) + w * (b + 0.03125 * PA[g, 9 + n])

        for g in range(share):
            def near_of(step, part, value):
                def near(a, b):
                    there = (step[0] + a, step[1] + b)
                    known = first_main if part == 0 else first_edge
                    return PB[g, 9 * part + known.index(there)] if there in known else value
                return near

            for n, step in enumerate(first_edge):
                value, other = PB[g, n], PB[g, 9 + n]
                PA[g, n] = total(value, other, near_of(step, 0, value))
            value, other = PB[g, 9], PB[g, 0]
            PA[g, 9] = total(value, other, near_of(own, 1, value))

        @pl.loop(0, share)
        def _(g):
            for n, step in enumerate(first_edge):
                w, b = main(step, share), main(step, g)
                PB[g, n] = PB[g, n] * (1.0 - jacobi_weight) + w * (b + 0.03125 * PA[g, n])
            w, b = edge(own, share), edge(own, g)
            PB[g, 9] = PB[g, 9] * (1.0 - jacobi_weight) + w * (b + 0.03125 * PA[g, 9])

        for g in range(share):
            value, other = PB[g, 0], PB[g, 9]
            PA[g, 0] = below(value, other)
            PA[g, 1] = above(value, other)
            for X in range(ex):
                for Y in range(ey):
                    TT[X + 1, Y + 1, tile(h * share + g), :] = spread(value, value, 2 * X + Y)
            for n, (a, b) in enumerate(CROSS):
                value = PB[g, 1 + n]
                for k in range(2):
                    X, Y = (k, 0) if a == 0 else (0, k)
                    X, Y = (1 if a < 0 else X), (1 if b < 0 else Y)
                    TT[2 * a + X + 1, 2 * b + Y + 1, tile(h * share + g), :] = spread(value, value, 2 * X + Y)
        for g in range(share):
            for q in range(ex * ey):
                TZ[q, tile(h * share + g), :] = spread(PA[g, 0], PA[g, 1], q)

    start_fine(0)
    with jax.named_scope('barrier'):
        pl.semaphore_wait(barrier, 6)
    for copy in fine(A, 0, 0):
        copy.start()

    @pl.loop(1, chunks)
    def _(c):
        with jax.named_scope('load'):
            start_fine(c)
        for copy in fine(A, 0, c):
            copy.start()

    with jax.named_scope('prologue'):
        prologue()
    for copy in diagonals():
        copy.start()

    @pl.loop(0, chunks)
    def _(c):
        with jax.named_scope('w0'):
            fine_wait(0, c)
        with jax.named_scope('first'):
            first_pass(c)
        for copy in fine(F, 1, c):
            copy.start()

    @pl.loop(0, chunks)
    def _(c):
        with jax.named_scope('w1'):
            fine_wait(1, c)
        with jax.named_scope('second'):
            second_pass(c)
        for copy in one(c):
            copy.start()

    for copy in gather_diagonal():
        copy.start()

    whole(W1R, got_w.at[1])
    whole(WZR, got_w.at[2])

    @pl.loop(0, halves)
    def _(h):
        @pl.loop(0, chunks // halves)
        def _(i):
            c = h * (chunks // halves) + i
            with jax.named_scope('w2'):
                whole(X1R.at[:, :, :, pl.ds(pl.multiple_of(c * deep, deep), deep)], one_got.at[c, 0])
                whole(Z1R.at[:, c], one_got.at[c, 1])
                whole(CR.at[:, c], one_got.at[c, 2])
            with jax.named_scope('sweep'):
                unpack_faces(c)
                coarse_z(U1a, 2, met(Z1R[0, c, 0], Z1R[1, c, 0], 4), c)

                @pl.loop(0, inner)
                def _(j):
                    rows = tile(c * inner + j)
                    for X in range(cx):
                        for Y in range(cy):
                            k = X * cy + Y
                            total = beside_xy(U1a, X + 2, Y + 2, rows) + ZS[k, rows, :]
                            value = U1a[X + 2, Y + 2, rows, :] * third
                            U1b[X + 1, Y + 1, rows, :] = value + W1[X, Y] * (B1[k, rows, :] + 0.125 * total)

            with jax.named_scope('w3'):
                whole(ZD.at[:, :, c], one_got.at[c, 3])
            with jax.named_scope('ring'):
                outside(c)

                @pl.loop(0, inner)
                def _(j):
                    rows = tile(c * inner + j)
                    for side in range(4):
                        for t in range(4):
                            (x, y), _k = ring(side, t)
                            total = beside_xy(U1a, x + 2, y + 2, rows) + ZRING[4 * side + t, pl.ds(pl.multiple_of(j * SUB, SUB), SUB), :]
                            value = U1a[x + 2, y + 2, rows, :] * (1.0 + third)
                            U1b[x + 1, y + 1, rows, :] = value + 0.125 * W1R[side, t] * total

            with jax.named_scope('residue'):
                coarse_z(U1b, 1, HU[c], c)

                @pl.loop(0, inner)
                def _(j):
                    rows = tile(c * inner + j)
                    for X in range(ex):
                        for Y in range(ey):
                            sums = None
                            for dx in range(2):
                                for dy in range(2):
                                    x, y = 2 * X + dx, 2 * Y + dy
                                    k = x * cy + y
                                    total = beside_xy(U1b, x + 1, y + 1, rows) + ZS[k, rows, :]
                                    residue = B1[k, rows, :] - D1[k] * U1b[x + 1, y + 1, rows, :] + 0.125 * total
                                    B1[k, rows, :] = residue
                                    sums = residue if sums is None else sums + residue
                            B2[X * ey + Y, rows, :] = sums

        with jax.named_scope('weave'):
            parts = []
            for g in range(share):
                part = woven([0.5 * pair_sum(B2[q, tile(h * share + g), :], 2) for q in range(ex * ey)])
                MPS[h, g] = part
                parts.append(part)
            parts.append(WPS[...])
            low = high = None
            for g, part in enumerate(parts):
                here = (lane() >= EDGE * g) & (lane() < EDGE * (g + 1))
                up, down = roll(part, EDGE * g + EDGE), roll(part, EDGE * g)
                high = up if high is None else jnp.where(here, up, high)
                low = down if low is None else jnp.where(here, down, low)
            EPS[h, 0], EPS[h, 1] = high, low
        for copy in ends_far(h) + ends(h) + gather(h):
            copy.start()

    whole(WPR, got_w.at[0])

    def store(g):
        part = pl.ds(g * SUB, SUB)
        return pltpu.make_async_copy(stage.at[part], out_ref.at[part], sent.at[8])

    @pl.loop(0, halves)
    def _(h):
        with jax.named_scope('w5'):
            whole(MPR.at[h], got.at[h, 0])
        with jax.named_scope('w6'):
            whole(EPR.at[h], got.at[h, 1])
            whole(XPR.at[h], got.at[h, 2])
        with jax.named_scope('two'):
            level_two(h)
        with jax.named_scope('last'):
            @pl.loop(0, share)
            def _(i):
                g = h * share + i
                c, j = g // inner, g % inner
                rows = tile(g)
                band = pl.ds(pl.multiple_of(j * SUB, SUB), SUB)
                for X in range(cx):
                    levels = []
                    for Y in range(cy):
                        k, q, r = X * cy + Y, X // 2 + 1, Y // 2 + 1
                        t = TT[q, r, rows, :]
                        outer = TT[q + 2 * (X % 2) - 1, r, rows, :] + TT[q, r + 2 * (Y % 2) - 1, rows, :]
                        outer = outer + TZ[(q - 1) * ey + r - 1, rows, :] + 3.0 * t
                        value = U1b[X + 1, Y + 1, rows, :] + t * (1.0 - jacobi_weight)
                        levels.append(value + W1[X, Y] * (B1[k, rows, :] + 0.125 * outer))
                    for x in (2 * X, 2 * X + 1):
                        values = turn([S2[c, x, y, band, :] + levels[y // 2] for y in range(ny)])
                        for i in range(SUB):
                            stage[g * SUB + i, x * ny:(x + 1) * ny, :] = values[i]
                store(g).start()

    with jax.named_scope('sent'):
        whole(S2, sent.at[0])
        whole(FZS, sent.at[1])
        whole(X1S, sent.at[2])
        whole(Z1R, sent.at[3])
        whole(MPR, sent.at[4])
        whole(WPR, sent.at[5])
        whole(EPS, sent.at[6])
        whole(XPR, sent.at[7])
        whole(stage, sent.at[8])
        whole(CS, sent.at[9])
        whole(ZD, sent.at[10])
        whole(W1R, sent.at[11])
        whole(WZR, sent.at[12])


def local(orbitals, potential, centre, half_width):
    bands, nx, ny, nz = orbitals.shape
    chunks = 4
    deep = bands // chunks
    cx, cy, ex, ey = nx // 2, ny // 2, nx // 4, ny // 4
    groups = bands // SUB
    vmem = lambda *s: pltpu.VMEM(s, jnp.float32)
    dma = lambda *s: pltpu.SemaphoreType.DMA(s)
    out = pl.pallas_call(
        functools.partial(kernel, bands, nx, ny, chunks),
        name="filter_orbitals",
        out_shape=jax.ShapeDtypeStruct((bands, nx * ny, nz), jnp.float32),
        in_specs=[pl.BlockSpec(memory_space=pltpu.HBM)] * 4,
        out_specs=pl.BlockSpec(memory_space=pl.ANY),
        scratch_shapes=[
            vmem(bands, nx * ny, nz), vmem(nx * ny, nz), pltpu.SMEM((bands,), jnp.float32), pltpu.SMEM((bands,), jnp.float32),
            vmem(nx * ny, bands, nz), vmem(cx * cy, deep, nz),
            vmem(chunks, nx + 2, ny + 2, deep, nz), vmem(chunks, nx + 2, ny + 2, deep, nz), vmem(chunks, nx, ny, deep, nz),
            vmem(nx * ny, SUB, nz), vmem(cx * cy, SUB, nz), vmem(cx, cy, SUB, nz),
            vmem(groups, SUB, nz), vmem(groups, SUB, nz),
            vmem(2, 2, chunks, deep // 16, SUB, nz), vmem(2, 2, chunks, deep // 16, SUB, nz),
            vmem(cx * cy, bands, nz),
            vmem(cx + 4, cy + 4, bands, nz), vmem(cx + 2, cy + 2, bands, nz), vmem(ex * ey, bands, nz),
            vmem(2, 4, cy // 2, bands, nz), vmem(2, 4, cy // 2, bands, nz),
            vmem(chunks, 2, SUB, nz), vmem(2, chunks, 2, SUB, nz),
            vmem(4, chunks, SUB, nz), vmem(4, chunks, SUB, nz), vmem(4, 2, chunks, SUB, nz),
            vmem(4, 4, SUB, nz), vmem(SUB, nz), vmem(2, SUB, nz), vmem(chunks, SUB, nz), vmem(16, deep, nz),
            vmem(2, groups // 2, SUB, nz), vmem(2, 10, groups // 2, SUB, nz), vmem(SUB, nz), vmem(10, SUB, nz),
            vmem(2, 2, SUB, nz), vmem(2, 2, SUB, nz), vmem(2, 8, 2, SUB, nz),
            vmem(9, groups // 2 + 1, SUB, nz), vmem(groups // 2, 14, SUB, nz), vmem(groups // 2, 14, SUB, nz),
            vmem(ex + 2, ey + 2, bands, nz), vmem(ex * ey, bands, nz),
            dma(chunks), dma(3), dma(13), dma(2, chunks, 2), dma(chunks, 4), dma(2, 3), dma(3),
        ],
        compiler_params=pltpu.CompilerParams(collective_id=0, has_side_effects=True, vmem_limit_bytes=48 * 1024 * 1024),
    )(*(pltpu.with_memory_space_constraint(a, pltpu.HBM) for a in (orbitals.reshape(bands, nx * ny, nz), potential.reshape(nx * ny, nz), centre, half_width)))
    return out.reshape(bands, nx, ny, nz)


def solution(mesh):
    in_specs = (P(None, "gx", "gy", "gz"), P("gx", "gy", "gz"), P(), P())
    out_specs = P(None, "gx", "gy", "gz")
    return jax.shard_map(local, mesh=mesh, in_specs=in_specs, out_specs=out_specs, check_vma=False)
```

```python
import functools

import jax
import jax.numpy as jnp
from jax import lax
from jax.experimental import pallas as pl
from jax.experimental.pallas import tpu as pltpu
from jax.sharding import PartitionSpec as P

MESH = pl.DeviceIdType.MESH
shift_mass = 0.05
jacobi_weight = 2.0 / 3.0
SUB, LANES = 8, 128
AXES = ("gx", "gy", "gz")
SIDES = (("gx", 1), ("gx", -1), ("gy", 1), ("gy", -1), ("gz", 1), ("gz", -1))
RING = ((1, 0), (-1, 0), (0, 1), (0, -1), (1, 1), (1, -1), (-1, 1), (-1, -1), (2, 0), (0, 2))
NEAR = RING[:8]
CROSS = RING[:4]
CORNERS = RING[4:8]
EDGE = 16


def lane():
    return lax.broadcasted_iota(jnp.int32, (SUB, LANES), 1)


def sublane():
    return lax.broadcasted_iota(jnp.int32, (SUB, LANES), 0)


def roll(value, shift):
    shift = shift % LANES
    return value if shift == 0 else pltpu.roll(value, shift, 1)


def turn(rows):
    at, rows = sublane(), list(rows)
    for d in (4, 2, 1):
        low = (at & d) == 0
        for i in range(SUB):
            if i & d == 0:
                a, b = rows[i], rows[i + d]
                rows[i] = jnp.where(low, a, pltpu.roll(b, d, 0))
                rows[i + d] = jnp.where(low, pltpu.roll(a, SUB - d, 0), b)
    return rows


def woven(columns):
    at = lane() & 3
    total = columns[3]
    for q in range(3):
        total = jnp.where(at == q, columns[q], total)
    return total


def spread(low, high, q):
    at = lane() & 3
    total = roll(high, 3 - q)
    for i, value in ((0, low), (1, low), (2, high)):
        total = jnp.where(at == i, roll(value, i - q), total)
    return total


def beside(own, low, high, bit):
    return jnp.where((lane() & bit) == 0, roll(own + low, -bit), roll(own + high, bit))


def below(main, other):
    return roll(jnp.where(lane() >= LANES - 4, other, main), 4)


def above(main, other):
    return roll(jnp.where(lane() < 4, other, main), -4)


def packed(total, value, start, width):
    at = lane()
    moved = roll(value, start + width // 2)
    if total is None:
        return moved
    return jnp.where((at >= start) & (at < start + width), moved, total)


def inner_z(value, width):
    at, half = lane(), width // 2
    return jnp.where(at < half, 0.0, roll(value, half)) + jnp.where(at >= LANES - half, 0.0, roll(value, -half))


def outer_z(rims, start, width):
    half = width // 2
    return jnp.where(((lane() + half) & (LANES - 1)) < width, roll(rims, -(start + half)), 0.0)


def met(from_left, from_right, width):
    half = width // 2
    return jnp.where((lane() & half) != 0, roll(from_left, half), roll(from_right, -half))


def first_cells(from_left, from_right):
    return jnp.where((lane() & 2) == 0, from_right, roll(from_left, 2))


def pair_sum(value, cell):
    at = lane()
    return value + jnp.where((at & cell) == 0, roll(value, -cell), roll(value, cell))


def kernel(bands, nx, ny, chunks, orb_hbm, pot_hbm, mid_hbm, half_hbm, out_ref,
           stage, pot_ref, mid_ref, half_ref, ZS, TS, A, F, S2, DG, D1, W1, MID, INV, FZS, FZR,
           B1, U1a, U1b, B2, X1S, X1R, Z1S, Z1R, CS, CR, ZD, ENDS, W1R, WZS, WZR, HU, ZRING, MPS, MPR, WPS, WPR, EPS, EPR, XPR, XE, PA, PB, TT, TZ,
           in_sem, par_sem, sent, fine_got, one_got, got, got_w):
    third = 1.0 - jacobi_weight
    deep = bands // chunks
    inner = deep // SUB
    groups = bands // SUB
    halves = 2
    share = groups // halves
    cx, cy = nx // 2, ny // 2
    ex, ey = nx // 4, ny // 4
    peers = []
    for axis, step in SIDES:
        n = lax.axis_size(axis)
        peers.append({axis: lax.rem(lax.axis_index(axis) + (n + step), n)})
    around_xy = []
    for step in RING:
        place = {}
        for axis, k in zip(AXES, step):
            n = lax.axis_size(axis)
            place[axis] = lax.rem(lax.axis_index(axis) + (n + k), n)
        around_xy.append(place)
    around_z = []
    for step in NEAR:
        for k in (1, -1):
            place = {}
            for axis, move in zip(AXES, step + (k,)):
                n = lax.axis_size(axis)
                place[axis] = lax.rem(lax.axis_index(axis) + (n + move), n)
            around_z.append(place)

    def load(c):
        part = pl.ds(c * deep, deep)
        return pltpu.make_async_copy(orb_hbm.at[part], stage.at[part], in_sem.at[c])

    params = [pltpu.make_async_copy(a, b, par_sem.at[i])
              for i, (a, b) in enumerate(((pot_hbm, pot_ref), (mid_hbm, mid_ref), (half_hbm, half_ref)))]
    for copy in params:
        copy.start()
    for c in range(chunks):
        load(c).start()
    barrier = pltpu.get_barrier_semaphore()
    for peer in peers:
        pl.semaphore_signal(barrier, inc=1, device_id=peer, device_id_type=MESH)

    def shape(value):
        return jnp.broadcast_to(value, (SUB, LANES))

    def prologue():
        for copy in params:
            copy.wait()
        at = sublane()
        for g in range(groups):
            mid = jnp.full((SUB, LANES), mid_ref[g * SUB], jnp.float32)
            half = jnp.full((SUB, LANES), half_ref[g * SUB], jnp.float32)
            for s in range(1, SUB):
                mid = jnp.where(at == s, mid_ref[g * SUB + s], mid)
                half = jnp.where(at == s, half_ref[g * SUB + s], half)
            MID[g] = 6.0 - 2.0 * mid
            INV[g] = 0.5 / half
        ones = {}
        for X in range(cx):
            for Y in range(cy):
                total = None
                for dx in range(2):
                    for dy in range(2):
                        k = (2 * X + dx) * ny + 2 * Y + dy
                        row = shape(pot_ref[pl.ds(k, 1), :])
                        DG[k] = 2.0 * row
                        total = row if total is None else total + row
                one = 0.125 * pair_sum(total, 1)
                ones[X, Y] = one
                diagonal = 0.75 + one + shift_mass
                D1[X * cy + Y] = diagonal
                W1[X, Y] = jacobi_weight / diagonal
        two_diagonals = []
        for X in range(ex):
            for Y in range(ey):
                total = (ones[2 * X, 2 * Y] + ones[2 * X + 1, 2 * Y]) + (ones[2 * X, 2 * Y + 1] + ones[2 * X + 1, 2 * Y + 1])
                diagonal = 0.1875 + 0.125 * pair_sum(total, 2) + shift_mass
                two_diagonals.append(jacobi_weight / diagonal)
        WPS[...] = woven(two_diagonals)
        total = None
        for j in range(2):
            for k in range(cx * cy):
                total = packed(total, W1[k // cy, k % cy], 4 * (j * cx * cy + k), 4)
        WZS[...] = total

    def send(src, dst, s, r, d):
        return pltpu.make_async_remote_copy(
            src_ref=src, dst_ref=dst, send_sem=s, recv_sem=r, device_id=peers[d], device_id_type=MESH)

    def fine(buffer, rnd, c):
        ends = (
            (buffer.at[c, nx, pl.ds(1, ny)], buffer.at[c, 0, pl.ds(1, ny)]),
            (buffer.at[c, 1, pl.ds(1, ny)], buffer.at[c, nx + 1, pl.ds(1, ny)]),
            (buffer.at[c, pl.ds(1, nx), ny], buffer.at[c, pl.ds(1, nx), 0]),
            (buffer.at[c, pl.ds(1, nx), 1], buffer.at[c, pl.ds(1, nx), ny + 1]),
            (FZS.at[rnd, 0, c], FZR.at[rnd, 0, c]),
            (FZS.at[rnd, 1, c], FZR.at[rnd, 1, c]),
        )
        return [send(a, b, sent.at[d // 4], fine_got.at[rnd, c], d) for d, (a, b) in enumerate(ends)]

    def whole(ref, sem):
        pltpu.make_async_copy(ref, ref, sem).wait()

    def fine_wait(rnd, c):
        whole(stage.at[pl.ds(0, 2 * (nx + ny) + 1), pl.ds(0, deep)], fine_got.at[rnd, c])

    def fine_edges(rnd, c, totals):
        odd = (lane() & 1) != 0
        for i in range(inner // 2):
            a, b = totals[2 * i], totals[2 * i + 1]
            FZS[rnd, 0, c, i] = jnp.where(odd, roll(a, 1), b)
            FZS[rnd, 1, c, i] = jnp.where(odd, b, roll(a, -1))

    def fine_rims(rnd, c):
        odd = (lane() & 1) != 0
        rims = []
        for i in range(inner // 2):
            low, high = FZR[rnd, 0, c, i], FZR[rnd, 1, c, i]
            rims.append(jnp.where(odd, low, high))
            rims.append(jnp.where(odd, roll(low, 1), roll(high, -1)))
        return rims

    def start_fine(c):
        load(c).wait()
        totals = [None] * inner
        for j in range(inner):
            for x in range(nx):
                rows = turn([stage[c * deep + j * SUB + i, x * ny:(x + 1) * ny, :] for i in range(SUB)])
                for y in range(ny):
                    A[c, x + 1, y + 1, j * SUB:(j + 1) * SUB, :] = rows[y]
                    totals[j] = packed(totals[j], rows[y], 2 * (x * ny + y), 2)
        fine_edges(0, c, totals)

    def fine_inner(buffer, c):
        for j in range(inner):
            for x in range(nx):
                for y in range(ny):
                    value = buffer[c, x + 1, y + 1, j * SUB:(j + 1) * SUB, :]
                    ZS[x * ny + y, tile(c * inner + j), :] = inner_z(value, 2)

    def fine_outer(rnd, c):
        rims = fine_rims(rnd, c)
        for j in range(inner):
            for k in range(nx * ny):
                ZS[k, tile(c * inner + j), :] += outer_z(rims[j], 2 * k, 2)

    def apply(buffer, c, x, y, j):
        band = pl.ds(pl.multiple_of(j * SUB, SUB), SUB)
        v = buffer[c, x + 1, y + 1, band, :]
        total = buffer[c, x, y + 1, band, :] + buffer[c, x + 2, y + 1, band, :]
        total = total + buffer[c, x + 1, y, band, :] + buffer[c, x + 1, y + 2, band, :]
        total = total + ZS[x * ny + y, tile(c * inner + j), :]
        return (DG[x * ny + y] + MID[c * inner + j]) * v - total

    def first_pass(c):
        fine_outer(0, c)

        @pl.loop(0, inner)
        def _(j):
            inv = INV[c * inner + j]
            for x in range(nx):
                for y in range(ny):
                    F[c, x + 1, y + 1, pl.ds(pl.multiple_of(j * SUB, SUB), SUB), :] = apply(A, c, x, y, j) * inv

        totals = [None] * inner
        for j in range(inner):
            for x in range(nx):
                for y in range(ny):
                    totals[j] = packed(totals[j], F[c, x + 1, y + 1, j * SUB:(j + 1) * SUB, :], 2 * (x * ny + y), 2)
        fine_edges(1, c, totals)

    def second_pass(c):
        fine_outer(1, c)

        @pl.loop(0, inner)
        def _(j):
            band = pl.ds(pl.multiple_of(j * SUB, SUB), SUB)
            scale = 2.0 * INV[c * inner + j]
            for X in range(cx):
                for Y in range(cy):
                    total = None
                    for dx in range(2):
                        for dy in range(2):
                            x, y = 2 * X + dx, 2 * Y + dy
                            value = apply(F, c, x, y, j) * scale - A[c, x + 1, y + 1, band, :]
                            S2[c, x, y, band, :] = value
                            total = value if total is None else total + value
                    TS[X * cy + Y, band, :] = total

        totals = [None, None]
        for j in range(inner):
            rows = pl.ds(pl.multiple_of(c * deep + j * SUB, SUB), SUB)
            for X in range(cx):
                for Y in range(cy):
                    k = X * cy + Y
                    source = 0.5 * pair_sum(TS[k, j * SUB:(j + 1) * SUB, :], 1)
                    B1[k, rows, :] = source
                    level = W1[X, Y] * source
                    U1a[X + 2, Y + 2, rows, :] = level
                    start = 4 * (j * cx * cy + k)
                    moved = roll(level, start + 2)
                    here = ((lane() + (LANES - start + 2)) & (LANES - 1)) < 8
                    totals[k % 2] = moved if totals[k % 2] is None else jnp.where(here, moved, totals[k % 2])
            even = (lane() & 1) == 0
            for n in range(2):
                lines = ([(cx - 1 - n, y) for y in range(cy)], [(n, y) for y in range(cy)],
                         [(x, cy - 1 - n) for x in range(cx)], [(x, n) for x in range(cx)])
                for d, line in enumerate(lines):
                    for p in range(len(line) // 2):
                        (x0, y0), (x1, y1) = line[2 * p], line[2 * p + 1]
                        X1S[n, d, p, rows, :] = jnp.where(even, U1a[x0 + 2, y0 + 2, rows, :], U1a[x1 + 2, y1 + 2, rows, :])
        turn_even = (lane() & 4) == 0
        near = jnp.where(turn_even, totals[0], totals[1])
        ENDS[c] = near
        inward = [jnp.where((lane() & 2) == 0, roll(t, 2), roll(t, -2)) for t in totals]
        far = jnp.where(turn_even, inward[0], inward[1])
        Z1S[c, 0] = jnp.where((lane() & 2) == 0, near, roll(far, 2))
        Z1S[c, 1] = jnp.where((lane() & 2) == 0, roll(near, -2), far)
        for i, (a, b) in enumerate(CORNERS):
            x, y = cx + 1 if a > 0 else 2, cy + 1 if b > 0 else 2
            CS[i, c] = jnp.where((lane() & 1) == 0, U1a[x, y, tile(c * inner), :], U1a[x, y, tile(c * inner + 1), :])

    def one(c):
        rows = pl.ds(pl.multiple_of(c * deep, deep), deep)
        copies = []
        for i, (a, b) in enumerate(CROSS):
            for d in range(2):
                copies.append(remote(Z1S.at[c, d], ZD.at[slot((-a, -b)), d, c], sent.at[10], one_got.at[c, 1],
                                     around_z[2 * i + d]))
        copies += [send(Z1S.at[c, d - 4], Z1R.at[d - 4, c], sent.at[3], one_got.at[c, 0], d) for d in (4, 5)]
        for i in range(4):
            copies.append(remote(CS.at[i, c], CR.at[i, c], sent.at[9], one_got.at[c, 0], around_xy[4 + i]))
        return copies + [send(X1S.at[:, d, :, rows], X1R.at[:, d, :, rows], sent.at[2], one_got.at[c, 0], d)
                         for d in range(4)]

    def diagonals():
        faces = (W1.at[cx - 1], W1.at[0], W1.at[:, cy - 1], W1.at[:, 0])
        copies = [send(face, W1R.at[d ^ 1], sent.at[11], got_w.at[1], d) for d, face in enumerate(faces)]
        return copies + [send(WZS, WZR.at[d - 4], sent.at[12], got_w.at[2], d) for d in (4, 5)]

    def slot(step):
        return RING.index(step) if step in RING else RING.index((abs(step[0]), abs(step[1])))

    def remote(src, dst, s, r, place):
        return pltpu.make_async_remote_copy(
            src_ref=src, dst_ref=dst, send_sem=s, recv_sem=r, device_id=place, device_id_type=MESH)

    def gather(h):
        copies = []
        for i, (a, b) in enumerate(RING):
            copies.append(remote(MPS.at[h], MPR.at[h, slot((-a, -b))], sent.at[4], got.at[h, 0], around_xy[i]))
        return copies

    def gather_diagonal():
        copies = []
        for i, (a, b) in enumerate(RING):
            copies.append(remote(WPS, WPR.at[slot((-a, -b))], sent.at[5], got_w.at[0], around_xy[i]))
        return copies

    def ends(h):
        return [send(EPS.at[h, d], EPR.at[h, d], sent.at[6], got.at[h, 1], 4 + d) for d in range(2)]

    def ends_far(h):
        copies = []
        for i, (a, b) in enumerate(NEAR):
            for d in range(2):
                copies.append(remote(EPS.at[h, d], XPR.at[h, slot((-a, -b)), d], sent.at[7], got.at[h, 2],
                                     around_z[2 * i + d]))
        return copies

    def tile(g):
        return pl.ds(g * SUB if isinstance(g, int) else pl.multiple_of(g * SUB, SUB), SUB)

    def coarse_inner(buffer, at, c):
        for j in range(inner):
            for X in range(cx):
                for Y in range(cy):
                    ZS[X * cy + Y, tile(c * inner + j), :] = inner_z(buffer[X + at, Y + at, tile(c * inner + j), :], 4)

    def coarse_outer(rims, c):
        for j in range(inner):
            for k in range(cx * cy):
                ZS[k, tile(c * inner + j), :] += outer_z(rims, 4 * (j * cx * cy + k), 4)

    def ring_inner(c):
        for j in range(inner):
            for i in range(4):
                for t in range(4):
                    (x, y), _ = ring(i, t)
                    value = U1a[x + 2, y + 2, tile(c * inner + j), :]
                    ZRING[4 * i + t, j * SUB:(j + 1) * SUB, :] = inner_z(value, 4)

    def unpack_faces(c):
        even = (lane() & 1) == 0
        for j in range(inner):
            rows = tile(c * inner + j)
            for n in range(2):
                lines = ([(1 - n, y + 2) for y in range(cy)], [(cx + 2 + n, y + 2) for y in range(cy)],
                         [(x + 2, 1 - n) for x in range(cx)], [(x + 2, cy + 2 + n) for x in range(cx)])
                for d, line in enumerate(lines):
                    for p in range(len(line) // 2):
                        both = X1R[n, d, p, rows, :]
                        (x0, y0), (x1, y1) = line[2 * p], line[2 * p + 1]
                        U1a[x0, y0, rows, :] = jnp.where(even, both, roll(both, 1))
                        U1a[x1, y1, rows, :] = jnp.where(even, roll(both, -1), both)
        for i, (a, b) in enumerate(CORNERS):
            both = CR[i, c]
            x, y = 1 if a > 0 else cx + 2, 1 if b > 0 else cy + 2
            U1a[x, y, tile(c * inner), :] = jnp.where(even, both, roll(both, 1))
            U1a[x, y, tile(c * inner + 1), :] = jnp.where(even, roll(both, -1), both)

    def ring(i, t):
        return (((cx, t), t), ((-1, t), (cx - 1) * cy + t), ((t, cy), t * cy), ((t, -1), t * cy + cy - 1))[i]

    def outside(c):
        rims = [first_cells(ZD[i, 0, c], ZD[i, 1, c]) for i in range(4)]
        for j in range(inner):
            for i in range(4):
                for t in range(4):
                    _, k = ring(i, t)
                    ZRING[4 * i + t, j * SUB:(j + 1) * SUB, :] += outer_z(rims[i], 4 * (j * cx * cy + k), 4)
        own = first_cells(Z1R[0, c], Z1R[1, c])
        X, Y = (lane() >> 4) & 3, (lane() >> 2) & 3
        total = jnp.where(X == 0, roll(rims[1], -48), roll(own, 16)) + jnp.where(X == 3, roll(rims[0], 48), roll(own, -16))
        total = total + jnp.where(Y == 0, roll(rims[3], -12), roll(own, 4)) + jnp.where(Y == 3, roll(rims[2], 12), roll(own, -4))
        second_cells = jnp.where((lane() & 2) == 0, roll(Z1R[1, c], -2), Z1R[0, c])
        total = total + ENDS[c] + second_cells
        HU[c] = own * (1.0 + third) + 0.125 * met(WZR[0], WZR[1], 4) * total

    def beside_xy(buffer, x, y, rows):
        total = buffer[x - 1, y, rows, :] + buffer[x + 1, y, rows, :]
        return total + buffer[x, y - 1, rows, :] + buffer[x, y + 1, rows, :]

    def level_two(h):
        at = lane()
        for b in range(9):
            low, high = (EPR[h, 0], EPR[h, 1]) if b == 8 else (XPR[h, b, 0], XPR[h, b, 1])
            for g in range(share + 1):
                XE[b, g] = jnp.where(at < EDGE, roll(high, -EDGE * g), roll(low, LANES - EDGE - EDGE * g))

        def main(step, g):
            if isinstance(g, int) and g == share:
                return WPS[...] if step == (0, 0) else WPR[slot(step)]
            return MPS[h, g] if step == (0, 0) else MPR[h, slot(step), g]

        def edge(step, g):
            return XE[8 if step == (0, 0) else slot(step), g]

        def know(step):
            return step == (0, 0) or step in RING or (abs(step[0]), abs(step[1])) in RING

        def total(value, other, near):
            x = beside(value, near(-1, 0), near(1, 0), 2)
            y = beside(value, near(0, -1), near(0, 1), 1)
            return x + y + (below(value, other) + above(value, other))

        own = (0, 0)
        first_main = (own,) + NEAR
        first_edge = (own,) + CROSS
        for g in range(share):
            start = {}
            for step in first_main + RING[8:]:
                start[step, 0] = main(step, share) * main(step, g)
            for step in first_main:
                start[step, 1] = edge(step, share) * edge(step, g)

            def near_of(step, part, value):
                def near(a, b):
                    there = (step[0] + a, step[1] + b)
                    there = there if know(there) else step
                    there = there if there == own or there in RING else (abs(there[0]), abs(there[1]))
                    return start.get((there, part), value)
                return near

            for n, step in enumerate(first_main):
                value, other = start[step, 0], start[step, 1]
                PA[g, n] = total(value, other, near_of(step, 0, value))
            for n, step in enumerate(first_edge):
                value, other = start[step, 1], start[step, 0]
                PA[g, 9 + n] = total(value, other, near_of(step, 1, value))

        for g in range(share):
            for n, step in enumerate(first_main):
                w, b = main(step, share), main(step, g)
                PB[g, n] = (w * b) * (1.0 - jacobi_weight) + w * (b + 0.03125 * PA[g, n])
            for n, step in enumerate(first_edge):
                w, b = edge(step, share), edge(step, g)
                PB[g, 9 + n] = (w * b) * (1.0 - jacobi_weight) + w * (b + 0.03125 * PA[g, 9 + n])

        for g in range(share):
            def near_of(step, part, value):
                def near(a, b):
                    there = (step[0] + a, step[1] + b)
                    known = first_main if part == 0 else first_edge
                    return PB[g, 9 * part + known.index(there)] if there in known else value
                return near

            for n, step in enumerate(first_edge):
                value, other = PB[g, n], PB[g, 9 + n]
                PA[g, n] = total(value, other, near_of(step, 0, value))
            value, other = PB[g, 9], PB[g, 0]
            PA[g, 9] = total(value, other, near_of(own, 1, value))

        for g in range(share):
            for n, step in enumerate(first_edge):
                w, b = main(step, share), main(step, g)
                PB[g, n] = PB[g, n] * (1.0 - jacobi_weight) + w * (b + 0.03125 * PA[g, n])
            w, b = edge(own, share), edge(own, g)
            PB[g, 9] = PB[g, 9] * (1.0 - jacobi_weight) + w * (b + 0.03125 * PA[g, 9])

        for g in range(share):
            value, other = PB[g, 0], PB[g, 9]
            PA[g, 0] = below(value, other)
            PA[g, 1] = above(value, other)
            for X in range(ex):
                for Y in range(ey):
                    TT[X + 1, Y + 1, tile(h * share + g), :] = spread(value, value, 2 * X + Y)
            for n, (a, b) in enumerate(CROSS):
                value = PB[g, 1 + n]
                for k in range(2):
                    X, Y = (k, 0) if a == 0 else (0, k)
                    X, Y = (1 if a < 0 else X), (1 if b < 0 else Y)
                    TT[2 * a + X + 1, 2 * b + Y + 1, tile(h * share + g), :] = spread(value, value, 2 * X + Y)
        for g in range(share):
            for q in range(ex * ey):
                TZ[q, tile(h * share + g), :] = spread(PA[g, 0], PA[g, 1], q)

    start_fine(0)
    with jax.named_scope('barrier'):
        pl.semaphore_wait(barrier, 6)
    for copy in fine(A, 0, 0):
        copy.start()

    @pl.loop(1, chunks)
    def _(c):
        with jax.named_scope('load'):
            start_fine(c)
        for copy in fine(A, 0, c):
            copy.start()

    with jax.named_scope('prologue'):
        prologue()
    for copy in diagonals():
        copy.start()

    @pl.loop(0, chunks)
    def _(c):
        fine_inner(A, c)

    @pl.loop(0, chunks)
    def _(c):
        with jax.named_scope('w0'):
            fine_wait(0, c)
        with jax.named_scope('first'):
            first_pass(c)
        for copy in fine(F, 1, c):
            copy.start()
        fine_inner(F, c)

    @pl.loop(0, chunks)
    def _(c):
        with jax.named_scope('w1'):
            fine_wait(1, c)
        with jax.named_scope('second'):
            second_pass(c)
        for copy in one(c):
            copy.start()
        coarse_inner(U1a, 2, c)

    for copy in gather_diagonal():
        copy.start()

    whole(W1R, got_w.at[1])
    whole(WZR, got_w.at[2])

    @pl.loop(0, halves)
    def _(h):
        @pl.loop(0, chunks // halves)
        def _(i):
            c = h * (chunks // halves) + i
            with jax.named_scope('w2'):
                whole(stage.at[pl.ds(0, 4 * (cx + cy) // 2 + 3), pl.ds(0, deep)], one_got.at[c, 0])
            with jax.named_scope('sweep'):
                unpack_faces(c)
                coarse_outer(first_cells(Z1R[0, c], Z1R[1, c]), c)

                @pl.loop(0, inner)
                def _(j):
                    rows = tile(c * inner + j)
                    for X in range(cx):
                        for Y in range(cy):
                            k = X * cy + Y
                            total = beside_xy(U1a, X + 2, Y + 2, rows) + ZS[k, rows, :]
                            value = U1a[X + 2, Y + 2, rows, :] * third
                            U1b[X + 1, Y + 1, rows, :] = value + W1[X, Y] * (B1[k, rows, :] + 0.125 * total)

                coarse_inner(U1b, 1, c)
                ring_inner(c)
            with jax.named_scope('w3'):
                whole(ZD.at[:, :, c], one_got.at[c, 1])
            with jax.named_scope('ring'):
                outside(c)

                @pl.loop(0, inner)
                def _(j):
                    rows = tile(c * inner + j)
                    for side in range(4):
                        for t in range(4):
                            (x, y), _k = ring(side, t)
                            total = beside_xy(U1a, x + 2, y + 2, rows) + ZRING[4 * side + t, pl.ds(pl.multiple_of(j * SUB, SUB), SUB), :]
                            value = U1a[x + 2, y + 2, rows, :] * (1.0 + third)
                            U1b[x + 1, y + 1, rows, :] = value + 0.125 * W1R[side, t] * total

            with jax.named_scope('residue'):
                coarse_outer(HU[c], c)

                @pl.loop(0, inner)
                def _(j):
                    rows = tile(c * inner + j)
                    for X in range(ex):
                        for Y in range(ey):
                            sums = None
                            for dx in range(2):
                                for dy in range(2):
                                    x, y = 2 * X + dx, 2 * Y + dy
                                    k = x * cy + y
                                    total = beside_xy(U1b, x + 1, y + 1, rows) + ZS[k, rows, :]
                                    residue = B1[k, rows, :] - D1[k] * U1b[x + 1, y + 1, rows, :] + 0.125 * total
                                    B1[k, rows, :] = residue
                                    sums = residue if sums is None else sums + residue
                            B2[X * ey + Y, rows, :] = sums

        with jax.named_scope('weave'):
            parts = []
            for g in range(share):
                part = woven([0.5 * pair_sum(B2[q, tile(h * share + g), :], 2) for q in range(ex * ey)])
                MPS[h, g] = part
                parts.append(part)
            parts.append(WPS[...])
            low = high = None
            for g, part in enumerate(parts):
                here = (lane() >= EDGE * g) & (lane() < EDGE * (g + 1))
                up, down = roll(part, EDGE * g + EDGE), roll(part, EDGE * g)
                high = up if high is None else jnp.where(here, up, high)
                low = down if low is None else jnp.where(here, down, low)
            EPS[h, 0], EPS[h, 1] = high, low
        for copy in ends_far(h) + ends(h) + gather(h):
            copy.start()

    whole(WPR, got_w.at[0])

    def store(g):
        part = pl.ds(g * SUB, SUB)
        return pltpu.make_async_copy(stage.at[part], out_ref.at[part], sent.at[8])

    @pl.loop(0, halves)
    def _(h):
        with jax.named_scope('w5'):
            whole(MPR.at[h], got.at[h, 0])
        with jax.named_scope('w6'):
            whole(EPR.at[h], got.at[h, 1])
            whole(XPR.at[h], got.at[h, 2])
        with jax.named_scope('two'):
            level_two(h)
        with jax.named_scope('last'):
            @pl.loop(0, share)
            def _(i):
                g = h * share + i
                c, j = g // inner, g % inner
                rows = tile(g)
                band = pl.ds(pl.multiple_of(j * SUB, SUB), SUB)
                for X in range(cx):
                    levels = []
                    for Y in range(cy):
                        k, q, r = X * cy + Y, X // 2 + 1, Y // 2 + 1
                        t = TT[q, r, rows, :]
                        outer = TT[q + 2 * (X % 2) - 1, r, rows, :] + TT[q, r + 2 * (Y % 2) - 1, rows, :]
                        outer = outer + TZ[(q - 1) * ey + r - 1, rows, :] + 3.0 * t
                        value = U1b[X + 1, Y + 1, rows, :] + t * (1.0 - jacobi_weight)
                        levels.append(value + W1[X, Y] * (B1[k, rows, :] + 0.125 * outer))
                    for x in (2 * X, 2 * X + 1):
                        values = turn([S2[c, x, y, band, :] + levels[y // 2] for y in range(ny)])
                        for i in range(SUB):
                            stage[g * SUB + i, x * ny:(x + 1) * ny, :] = values[i]
                store(g).start()

    with jax.named_scope('sent'):
        whole(S2, sent.at[0])
        whole(FZS, sent.at[1])
        whole(X1S, sent.at[2])
        whole(Z1R, sent.at[3])
        whole(MPR, sent.at[4])
        whole(WPR, sent.at[5])
        whole(EPS, sent.at[6])
        whole(XPR, sent.at[7])
        whole(stage, sent.at[8])
        whole(CS, sent.at[9])
        whole(ZD, sent.at[10])
        whole(W1R, sent.at[11])
        whole(WZR, sent.at[12])


def local(orbitals, potential, centre, half_width):
    bands, nx, ny, nz = orbitals.shape
    chunks = 4
    deep = bands // chunks
    cx, cy, ex, ey = nx // 2, ny // 2, nx // 4, ny // 4
    groups = bands // SUB
    vmem = lambda *s: pltpu.VMEM(s, jnp.float32)
    dma = lambda *s: pltpu.SemaphoreType.DMA(s)
    out = pl.pallas_call(
        functools.partial(kernel, bands, nx, ny, chunks),
        name="filter_orbitals",
        out_shape=jax.ShapeDtypeStruct((bands, nx * ny, nz), jnp.float32),
        in_specs=[pl.BlockSpec(memory_space=pltpu.HBM)] * 4,
        out_specs=pl.BlockSpec(memory_space=pl.ANY),
        scratch_shapes=[
            vmem(bands, nx * ny, nz), vmem(nx * ny, nz), pltpu.SMEM((bands,), jnp.float32), pltpu.SMEM((bands,), jnp.float32),
            vmem(nx * ny, bands, nz), vmem(cx * cy, deep, nz),
            vmem(chunks, nx + 2, ny + 2, deep, nz), vmem(chunks, nx + 2, ny + 2, deep, nz), vmem(chunks, nx, ny, deep, nz),
            vmem(nx * ny, SUB, nz), vmem(cx * cy, SUB, nz), vmem(cx, cy, SUB, nz),
            vmem(groups, SUB, nz), vmem(groups, SUB, nz),
            vmem(2, 2, chunks, deep // 16, SUB, nz), vmem(2, 2, chunks, deep // 16, SUB, nz),
            vmem(cx * cy, bands, nz),
            vmem(cx + 4, cy + 4, bands, nz), vmem(cx + 2, cy + 2, bands, nz), vmem(ex * ey, bands, nz),
            vmem(2, 4, cy // 2, bands, nz), vmem(2, 4, cy // 2, bands, nz),
            vmem(chunks, 2, SUB, nz), vmem(2, chunks, SUB, nz),
            vmem(4, chunks, SUB, nz), vmem(4, chunks, SUB, nz), vmem(4, 2, chunks, SUB, nz), vmem(chunks, SUB, nz),
            vmem(4, 4, SUB, nz), vmem(SUB, nz), vmem(2, SUB, nz), vmem(chunks, SUB, nz), vmem(16, deep, nz),
            vmem(2, groups // 2, SUB, nz), vmem(2, 10, groups // 2, SUB, nz), vmem(SUB, nz), vmem(10, SUB, nz),
            vmem(2, 2, SUB, nz), vmem(2, 2, SUB, nz), vmem(2, 8, 2, SUB, nz),
            vmem(9, groups // 2 + 1, SUB, nz), vmem(groups // 2, 14, SUB, nz), vmem(groups // 2, 14, SUB, nz),
            vmem(ex + 2, ey + 2, bands, nz), vmem(ex * ey, bands, nz),
            dma(chunks), dma(3), dma(13), dma(2, chunks), dma(chunks, 2), dma(2, 3), dma(3),
        ],
        compiler_params=pltpu.CompilerParams(collective_id=0, has_side_effects=True, vmem_limit_bytes=48 * 1024 * 1024),
    )(*(pltpu.with_memory_space_constraint(a, pltpu.HBM) for a in (orbitals.reshape(bands, nx * ny, nz), potential.reshape(nx * ny, nz), centre, half_width)))
    return out.reshape(bands, nx, ny, nz)


def solution(mesh):
    in_specs = (P(None, "gx", "gy", "gz"), P("gx", "gy", "gz"), P(), P())
    out_specs = P(None, "gx", "gy", "gz")
    return jax.shard_map(local, mesh=mesh, in_specs=in_specs, out_specs=out_specs, check_vma=False)
```

```python
import functools

import jax
import jax.numpy as jnp
from jax import lax
from jax.experimental import pallas as pl
from jax.experimental.pallas import tpu as pltpu
from jax.sharding import PartitionSpec as P

MESH = pl.DeviceIdType.MESH
shift_mass = 0.05
jacobi_weight = 2.0 / 3.0
SUB, LANES = 8, 128
AXES = ("gx", "gy", "gz")
SIDES = (("gx", 1), ("gx", -1), ("gy", 1), ("gy", -1), ("gz", 1), ("gz", -1))
RING = ((1, 0), (-1, 0), (0, 1), (0, -1), (1, 1), (1, -1), (-1, 1), (-1, -1), (2, 0), (0, 2))
NEAR = RING[:8]
CROSS = RING[:4]
CORNERS = RING[4:8]
EDGE = 16


def lane():
    return lax.broadcasted_iota(jnp.int32, (SUB, LANES), 1)


def sublane():
    return lax.broadcasted_iota(jnp.int32, (SUB, LANES), 0)


def roll(value, shift):
    shift = shift % LANES
    return value if shift == 0 else pltpu.roll(value, shift, 1)


def turn(rows):
    at, rows = sublane(), list(rows)
    for d in (4, 2, 1):
        low = (at & d) == 0
        for i in range(SUB):
            if i & d == 0:
                a, b = rows[i], rows[i + d]
                rows[i] = jnp.where(low, a, pltpu.roll(b, d, 0))
                rows[i + d] = jnp.where(low, pltpu.roll(a, SUB - d, 0), b)
    return rows


def woven(columns):
    at = lane() & 3
    total = columns[3]
    for q in range(3):
        total = jnp.where(at == q, columns[q], total)
    return total


def spread(low, high, q):
    at = lane() & 3
    total = roll(high, 3 - q)
    for i, value in ((0, low), (1, low), (2, high)):
        total = jnp.where(at == i, roll(value, i - q), total)
    return total


def beside(own, low, high, bit):
    return jnp.where((lane() & bit) == 0, roll(own + low, -bit), roll(own + high, bit))


def below(main, other):
    return roll(jnp.where(lane() >= LANES - 4, other, main), 4)


def above(main, other):
    return roll(jnp.where(lane() < 4, other, main), -4)


def packed(total, value, start, width):
    at = lane()
    moved = roll(value, start + width // 2)
    if total is None:
        return moved
    return jnp.where((at >= start) & (at < start + width), moved, total)


def inner_z(value, width):
    at, half = lane(), width // 2
    return jnp.where(at < half, 0.0, roll(value, half)) + jnp.where(at >= LANES - half, 0.0, roll(value, -half))


def outer_z(rims, start, width):
    half = width // 2
    return jnp.where(((lane() + half) & (LANES - 1)) < width, roll(rims, -(start + half)), 0.0)


def met(from_left, from_right, width):
    half = width // 2
    return jnp.where((lane() & half) != 0, roll(from_left, half), roll(from_right, -half))


def first_cells(from_left, from_right):
    return jnp.where((lane() & 2) == 0, from_right, roll(from_left, 2))


def pair_sum(value, cell):
    at = lane()
    return value + jnp.where((at & cell) == 0, roll(value, -cell), roll(value, cell))


def kernel(bands, nx, ny, chunks, orb_hbm, pot_hbm, mid_hbm, half_hbm, out_ref,
           stage, pot_ref, mid_ref, half_ref, ZS, TS, A, F, S2, DG, D1, W1, MID, INV, FZS, FZR,
           B1, U1a, U1b, B2, X1S, X1R, Z1S, Z1R, CS, CR, ZD, ENDS, W1S, W1R, WZS, WZR, HU, ZRING, MPS, MPR, WPS, WPR, EPS, EPR, XPR, XE, PA, PB, TT, TZ,
           in_sem, par_sem, sent, fine_got, one_got, got, got_w):
    third = 1.0 - jacobi_weight
    deep = bands // chunks
    inner = deep // SUB
    groups = bands // SUB
    halves = 2
    share = groups // halves
    cx, cy = nx // 2, ny // 2
    ex, ey = nx // 4, ny // 4
    peers = []
    for axis, step in SIDES:
        n = lax.axis_size(axis)
        peers.append({axis: lax.rem(lax.axis_index(axis) + (n + step), n)})
    around_xy = []
    for step in RING:
        place = {}
        for axis, k in zip(AXES, step):
            n = lax.axis_size(axis)
            place[axis] = lax.rem(lax.axis_index(axis) + (n + k), n)
        around_xy.append(place)
    around_z = []
    for step in NEAR:
        for k in (1, -1):
            place = {}
            for axis, move in zip(AXES, step + (k,)):
                n = lax.axis_size(axis)
                place[axis] = lax.rem(lax.axis_index(axis) + (n + move), n)
            around_z.append(place)

    def load(c):
        part = pl.ds(c * deep, deep)
        return pltpu.make_async_copy(orb_hbm.at[part], stage.at[part], in_sem.at[c])

    params = [pltpu.make_async_copy(a, b, par_sem.at[i])
              for i, (a, b) in enumerate(((pot_hbm, pot_ref), (mid_hbm, mid_ref), (half_hbm, half_ref)))]
    for copy in params:
        copy.start()
    for c in range(chunks):
        load(c).start()
    barrier = pltpu.get_barrier_semaphore()
    for peer in peers:
        pl.semaphore_signal(barrier, inc=1, device_id=peer, device_id_type=MESH)

    def shape(value):
        return jnp.broadcast_to(value, (SUB, LANES))

    def prologue():
        for copy in params:
            copy.wait()
        at = sublane()
        for g in range(groups):
            mid = jnp.full((SUB, LANES), mid_ref[g * SUB], jnp.float32)
            half = jnp.full((SUB, LANES), half_ref[g * SUB], jnp.float32)
            for s in range(1, SUB):
                mid = jnp.where(at == s, mid_ref[g * SUB + s], mid)
                half = jnp.where(at == s, half_ref[g * SUB + s], half)
            MID[g] = 6.0 - 2.0 * mid
            INV[g] = 0.5 / half
        ones = {}
        for X in range(cx):
            for Y in range(cy):
                total = None
                for dx in range(2):
                    for dy in range(2):
                        k = (2 * X + dx) * ny + 2 * Y + dy
                        row = shape(pot_ref[pl.ds(k, 1), :])
                        DG[k] = 2.0 * row
                        total = row if total is None else total + row
                one = 0.125 * pair_sum(total, 1)
                ones[X, Y] = one
                diagonal = 0.75 + one + shift_mass
                D1[X * cy + Y] = diagonal
                W1[X, Y] = jacobi_weight / diagonal
        two_diagonals = []
        for X in range(ex):
            for Y in range(ey):
                total = (ones[2 * X, 2 * Y] + ones[2 * X + 1, 2 * Y]) + (ones[2 * X, 2 * Y + 1] + ones[2 * X + 1, 2 * Y + 1])
                diagonal = 0.1875 + 0.125 * pair_sum(total, 2) + shift_mass
                two_diagonals.append(jacobi_weight / diagonal)
        WPS[...] = woven(two_diagonals)
        total = None
        for j in range(2):
            for k in range(cx * cy):
                total = packed(total, W1[k // cy, k % cy], 4 * (j * cx * cy + k), 4)
        WZS[...] = total
        for d in range(4):
            face = [W1[((cx - 1, t), (0, t), (t, cy - 1), (t, 0))[d]] for t in range(4)]
            rows = face[0]
            for t in range(1, 4):
                rows = jnp.where(sublane() == t, face[t], rows)
            W1S[d] = rows

    def send(src, dst, s, r, d):
        return pltpu.make_async_remote_copy(
            src_ref=src, dst_ref=dst, send_sem=s, recv_sem=r, device_id=peers[d], device_id_type=MESH)

    def fine(buffer, rnd, c):
        ends = (
            (buffer.at[c, nx, pl.ds(1, ny)], buffer.at[c, 0, pl.ds(1, ny)]),
            (buffer.at[c, 1, pl.ds(1, ny)], buffer.at[c, nx + 1, pl.ds(1, ny)]),
            (buffer.at[c, pl.ds(1, nx), ny], buffer.at[c, pl.ds(1, nx), 0]),
            (buffer.at[c, pl.ds(1, nx), 1], buffer.at[c, pl.ds(1, nx), ny + 1]),
            (FZS.at[rnd, 0, c], FZR.at[rnd, 0, c]),
            (FZS.at[rnd, 1, c], FZR.at[rnd, 1, c]),
        )
        copies = [send(a, b, sent.at[d // 4], fine_got.at[rnd, c], d) for d, (a, b) in enumerate(ends)]
        return copies[4:] + copies[:4]

    def whole(ref, sem):
        pltpu.make_async_copy(ref, ref, sem).wait()

    def fine_wait(rnd, c):
        whole(stage.at[pl.ds(0, 2 * (nx + ny) + 1), pl.ds(0, deep)], fine_got.at[rnd, c])

    def fine_edges(rnd, c, totals):
        odd = (lane() & 1) != 0
        for i in range(inner // 2):
            a, b = totals[2 * i], totals[2 * i + 1]
            FZS[rnd, 0, c, i] = jnp.where(odd, roll(a, 1), b)
            FZS[rnd, 1, c, i] = jnp.where(odd, b, roll(a, -1))

    def fine_rims(rnd, c):
        odd = (lane() & 1) != 0
        rims = []
        for i in range(inner // 2):
            low, high = FZR[rnd, 0, c, i], FZR[rnd, 1, c, i]
            rims.append(jnp.where(odd, low, high))
            rims.append(jnp.where(odd, roll(low, 1), roll(high, -1)))
        return rims

    def start_fine(c):
        load(c).wait()
        totals = [None] * inner
        for j in range(inner):
            for x in range(nx):
                rows = turn([stage[c * deep + j * SUB + i, x * ny:(x + 1) * ny, :] for i in range(SUB)])
                for y in range(ny):
                    A[c, x + 1, y + 1, j * SUB:(j + 1) * SUB, :] = rows[y]
                    totals[j] = packed(totals[j], rows[y], 2 * (x * ny + y), 2)
        fine_edges(0, c, totals)

    def fine_inner(buffer, c):
        for j in range(inner):
            for x in range(nx):
                for y in range(ny):
                    value = buffer[c, x + 1, y + 1, j * SUB:(j + 1) * SUB, :]
                    ZS[x * ny + y, tile(c * inner + j), :] = inner_z(value, 2)

    def fine_outer(rnd, c):
        rims = fine_rims(rnd, c)
        for j in range(inner):
            for k in range(nx * ny):
                ZS[k, tile(c * inner + j), :] += outer_z(rims[j], 2 * k, 2)

    def apply(buffer, c, x, y, j):
        band = pl.ds(pl.multiple_of(j * SUB, SUB), SUB)
        v = buffer[c, x + 1, y + 1, band, :]
        total = buffer[c, x, y + 1, band, :] + buffer[c, x + 2, y + 1, band, :]
        total = total + buffer[c, x + 1, y, band, :] + buffer[c, x + 1, y + 2, band, :]
        total = total + ZS[x * ny + y, tile(c * inner + j), :]
        return (DG[x * ny + y] + MID[c * inner + j]) * v - total

    def first_pass(c):
        fine_outer(0, c)

        @pl.loop(0, inner)
        def _(j):
            inv = INV[c * inner + j]
            for x in range(nx):
                for y in range(ny):
                    F[c, x + 1, y + 1, pl.ds(pl.multiple_of(j * SUB, SUB), SUB), :] = apply(A, c, x, y, j) * inv

        totals = [None] * inner
        for j in range(inner):
            for x in range(nx):
                for y in range(ny):
                    totals[j] = packed(totals[j], F[c, x + 1, y + 1, j * SUB:(j + 1) * SUB, :], 2 * (x * ny + y), 2)
        fine_edges(1, c, totals)

    def second_pass(c):
        fine_outer(1, c)

        @pl.loop(0, inner)
        def _(j):
            band = pl.ds(pl.multiple_of(j * SUB, SUB), SUB)
            scale = 2.0 * INV[c * inner + j]
            for X in range(cx):
                for Y in range(cy):
                    total = None
                    for dx in range(2):
                        for dy in range(2):
                            x, y = 2 * X + dx, 2 * Y + dy
                            value = apply(F, c, x, y, j) * scale - A[c, x + 1, y + 1, band, :]
                            S2[c, x, y, band, :] = value
                            total = value if total is None else total + value
                    TS[X * cy + Y, band, :] = total

        totals = [None, None]
        for j in range(inner):
            rows = pl.ds(pl.multiple_of(c * deep + j * SUB, SUB), SUB)
            for X in range(cx):
                for Y in range(cy):
                    k = X * cy + Y
                    source = 0.5 * pair_sum(TS[k, j * SUB:(j + 1) * SUB, :], 1)
                    B1[k, rows, :] = source
                    level = W1[X, Y] * source
                    U1a[X + 2, Y + 2, rows, :] = level
                    start = 4 * (j * cx * cy + k)
                    moved = roll(level, start + 2)
                    here = ((lane() + (LANES - start + 2)) & (LANES - 1)) < 8
                    totals[k % 2] = moved if totals[k % 2] is None else jnp.where(here, moved, totals[k % 2])
            even = (lane() & 1) == 0
            for n in range(2):
                lines = ([(cx - 1 - n, y) for y in range(cy)], [(n, y) for y in range(cy)],
                         [(x, cy - 1 - n) for x in range(cx)], [(x, n) for x in range(cx)])
                for d, line in enumerate(lines):
                    for p in range(len(line) // 2):
                        (x0, y0), (x1, y1) = line[2 * p], line[2 * p + 1]
                        X1S[n, d, p, rows, :] = jnp.where(even, U1a[x0 + 2, y0 + 2, rows, :], U1a[x1 + 2, y1 + 2, rows, :])
        turn_even = (lane() & 4) == 0
        near = jnp.where(turn_even, totals[0], totals[1])
        ENDS[c] = near
        inward = [jnp.where((lane() & 2) == 0, roll(t, 2), roll(t, -2)) for t in totals]
        far = jnp.where(turn_even, inward[0], inward[1])
        Z1S[c, 0] = jnp.where((lane() & 2) == 0, near, roll(far, 2))
        Z1S[c, 1] = jnp.where((lane() & 2) == 0, roll(near, -2), far)
        for i, (a, b) in enumerate(CORNERS):
            x, y = cx + 1 if a > 0 else 2, cy + 1 if b > 0 else 2
            CS[i, c] = jnp.where((lane() & 1) == 0, U1a[x, y, tile(c * inner), :], U1a[x, y, tile(c * inner + 1), :])

    def one(c):
        rows = pl.ds(pl.multiple_of(c * deep, deep), deep)
        copies = []
        for i, (a, b) in enumerate(CROSS):
            for d in range(2):
                copies.append(remote(Z1S.at[c, d], ZD.at[slot((-a, -b)), d, c], sent.at[10], one_got.at[c, 1],
                                     around_z[2 * i + d]))
        copies += [send(Z1S.at[c, d - 4], Z1R.at[d - 4, c], sent.at[3], one_got.at[c, 0], d) for d in (4, 5)]
        for i in range(4):
            copies.append(remote(CS.at[i, c], CR.at[i, c], sent.at[9], one_got.at[c, 0], around_xy[4 + i]))
        return copies + [send(X1S.at[:, d, :, rows], X1R.at[:, d, :, rows], sent.at[2], one_got.at[c, 0], d)
                         for d in range(4)]

    def diagonals():
        copies = [send(W1S.at[d], W1R.at[d ^ 1], sent.at[11], got_w.at[1], d) for d in range(4)]
        return copies + [send(WZS, WZR.at[d - 4], sent.at[12], got_w.at[2], d) for d in (4, 5)]

    def slot(step):
        return RING.index(step) if step in RING else RING.index((abs(step[0]), abs(step[1])))

    def remote(src, dst, s, r, place):
        return pltpu.make_async_remote_copy(
            src_ref=src, dst_ref=dst, send_sem=s, recv_sem=r, device_id=place, device_id_type=MESH)

    def gather(h):
        copies = []
        for i, (a, b) in enumerate(RING):
            copies.append(remote(MPS.at[h], MPR.at[h, slot((-a, -b))], sent.at[4], got.at[h, 0], around_xy[i]))
        return copies

    def gather_diagonal():
        copies = []
        for i, (a, b) in enumerate(RING):
            copies.append(remote(WPS, WPR.at[slot((-a, -b))], sent.at[5], got_w.at[0], around_xy[i]))
        return copies

    def ends(h):
        return [send(EPS.at[h, d], EPR.at[h, d], sent.at[6], got.at[h, 1], 4 + d) for d in range(2)]

    def ends_far(h):
        copies = []
        for i, (a, b) in enumerate(NEAR):
            for d in range(2):
                copies.append(remote(EPS.at[h, d], XPR.at[h, slot((-a, -b)), d], sent.at[7], got.at[h, 2],
                                     around_z[2 * i + d]))
        return copies

    def tile(g):
        return pl.ds(g * SUB if isinstance(g, int) else pl.multiple_of(g * SUB, SUB), SUB)

    def coarse_inner(buffer, at, c):
        for j in range(inner):
            for X in range(cx):
                for Y in range(cy):
                    ZS[X * cy + Y, tile(c * inner + j), :] = inner_z(buffer[X + at, Y + at, tile(c * inner + j), :], 4)

    def coarse_outer(rims, c):
        for j in range(inner):
            for k in range(cx * cy):
                ZS[k, tile(c * inner + j), :] += outer_z(rims, 4 * (j * cx * cy + k), 4)

    def ring_inner(c):
        for j in range(inner):
            for i in range(4):
                for t in range(4):
                    (x, y), _ = ring(i, t)
                    value = U1a[x + 2, y + 2, tile(c * inner + j), :]
                    ZRING[4 * i + t, j * SUB:(j + 1) * SUB, :] = inner_z(value, 4)

    def unpack_faces(c):
        even = (lane() & 1) == 0
        for j in range(inner):
            rows = tile(c * inner + j)
            for n in range(2):
                lines = ([(1 - n, y + 2) for y in range(cy)], [(cx + 2 + n, y + 2) for y in range(cy)],
                         [(x + 2, 1 - n) for x in range(cx)], [(x + 2, cy + 2 + n) for x in range(cx)])
                for d, line in enumerate(lines):
                    for p in range(len(line) // 2):
                        both = X1R[n, d, p, rows, :]
                        (x0, y0), (x1, y1) = line[2 * p], line[2 * p + 1]
                        U1a[x0, y0, rows, :] = jnp.where(even, both, roll(both, 1))
                        U1a[x1, y1, rows, :] = jnp.where(even, roll(both, -1), both)
        for i, (a, b) in enumerate(CORNERS):
            both = CR[i, c]
            x, y = 1 if a > 0 else cx + 2, 1 if b > 0 else cy + 2
            U1a[x, y, tile(c * inner), :] = jnp.where(even, both, roll(both, 1))
            U1a[x, y, tile(c * inner + 1), :] = jnp.where(even, roll(both, -1), both)

    def ring(i, t):
        return (((cx, t), t), ((-1, t), (cx - 1) * cy + t), ((t, cy), t * cy), ((t, -1), t * cy + cy - 1))[i]

    def outside(c):
        rims = [first_cells(ZD[i, 0, c], ZD[i, 1, c]) for i in range(4)]
        for j in range(inner):
            for i in range(4):
                for t in range(4):
                    _, k = ring(i, t)
                    ZRING[4 * i + t, j * SUB:(j + 1) * SUB, :] += outer_z(rims[i], 4 * (j * cx * cy + k), 4)
        own = first_cells(Z1R[0, c], Z1R[1, c])
        X, Y = (lane() >> 4) & 3, (lane() >> 2) & 3
        total = jnp.where(X == 0, roll(rims[1], -48), roll(own, 16)) + jnp.where(X == 3, roll(rims[0], 48), roll(own, -16))
        total = total + jnp.where(Y == 0, roll(rims[3], -12), roll(own, 4)) + jnp.where(Y == 3, roll(rims[2], 12), roll(own, -4))
        second_cells = jnp.where((lane() & 2) == 0, roll(Z1R[1, c], -2), Z1R[0, c])
        total = total + ENDS[c] + second_cells
        HU[c] = own * (1.0 + third) + 0.125 * met(WZR[0], WZR[1], 4) * total

    def beside_xy(buffer, x, y, rows):
        total = buffer[x - 1, y, rows, :] + buffer[x + 1, y, rows, :]
        return total + buffer[x, y - 1, rows, :] + buffer[x, y + 1, rows, :]

    def level_two(h, early):
        at = lane()
        for b in range(0 if early else 9):
            low, high = (EPR[h, 0], EPR[h, 1]) if b == 8 else (XPR[h, b, 0], XPR[h, b, 1])
            for g in range(share + 1):
                XE[b, g] = jnp.where(at < EDGE, roll(high, -EDGE * g), roll(low, LANES - EDGE - EDGE * g))

        def main(step, g):
            if isinstance(g, int) and g == share:
                return WPS[...] if step == (0, 0) else WPR[slot(step)]
            return MPS[h, g] if step == (0, 0) else MPR[h, slot(step), g]

        def edge(step, g):
            return XE[8 if step == (0, 0) else slot(step), g]

        def know(step):
            return step == (0, 0) or step in RING or (abs(step[0]), abs(step[1])) in RING

        def total(value, other, near):
            x = beside(value, near(-1, 0), near(1, 0), 2)
            y = beside(value, near(0, -1), near(0, 1), 1)
            return x + y + (below(value, other) + above(value, other))

        own = (0, 0)
        first_main = (own,) + NEAR
        first_edge = (own,) + CROSS
        for g in range(share):
            start = {}
            for step in first_main + RING[8:]:
                start[step, 0] = main(step, share) * main(step, g)
            for step in () if early else first_main:
                start[step, 1] = edge(step, share) * edge(step, g)

            def near_of(step, part, value):
                def near(a, b):
                    there = (step[0] + a, step[1] + b)
                    there = there if know(there) else step
                    there = there if there == own or there in RING else (abs(there[0]), abs(there[1]))
                    return start.get((there, part), value)
                return near

            for n, step in enumerate(first_main):
                value = start[step, 0]
                if early:
                    near = near_of(step, 0, value)
                    PA[g, n] = beside(value, near(-1, 0), near(1, 0), 2) + beside(value, near(0, -1), near(0, 1), 1)
                else:
                    PA[g, n] += below(value, start[step, 1]) + above(value, start[step, 1])
            if early:
                continue
            for n, step in enumerate(first_edge):
                value, other = start[step, 1], start[step, 0]
                PA[g, 9 + n] = total(value, other, near_of(step, 1, value))

        if early:
            return

        for g in range(share):
            for n, step in enumerate(first_main):
                w, b = main(step, share), main(step, g)
                PB[g, n] = (w * b) * (1.0 - jacobi_weight) + w * (b + 0.03125 * PA[g, n])
            for n, step in enumerate(first_edge):
                w, b = edge(step, share), edge(step, g)
                PB[g, 9 + n] = (w * b) * (1.0 - jacobi_weight) + w * (b + 0.03125 * PA[g, 9 + n])

        for g in range(share):
            def near_of(step, part, value):
                def near(a, b):
                    there = (step[0] + a, step[1] + b)
                    known = first_main if part == 0 else first_edge
                    return PB[g, 9 * part + known.index(there)] if there in known else value
                return near

            for n, step in enumerate(first_edge):
                value, other = PB[g, n], PB[g, 9 + n]
                PA[g, n] = total(value, other, near_of(step, 0, value))
            value, other = PB[g, 9], PB[g, 0]
            PA[g, 9] = total(value, other, near_of(own, 1, value))

        for g in range(share):
            for n, step in enumerate(first_edge):
                w, b = main(step, share), main(step, g)
                PB[g, n] = PB[g, n] * (1.0 - jacobi_weight) + w * (b + 0.03125 * PA[g, n])
            w, b = edge(own, share), edge(own, g)
            PB[g, 9] = PB[g, 9] * (1.0 - jacobi_weight) + w * (b + 0.03125 * PA[g, 9])

        for g in range(share):
            value, other = PB[g, 0], PB[g, 9]
            PA[g, 0] = below(value, other)
            PA[g, 1] = above(value, other)
            for X in range(ex):
                for Y in range(ey):
                    TT[X + 1, Y + 1, tile(h * share + g), :] = spread(value, value, 2 * X + Y)
            for n, (a, b) in enumerate(CROSS):
                value = PB[g, 1 + n]
                for k in range(2):
                    X, Y = (k, 0) if a == 0 else (0, k)
                    X, Y = (1 if a < 0 else X), (1 if b < 0 else Y)
                    TT[2 * a + X + 1, 2 * b + Y + 1, tile(h * share + g), :] = spread(value, value, 2 * X + Y)
        for g in range(share):
            for q in range(ex * ey):
                TZ[q, tile(h * share + g), :] = spread(PA[g, 0], PA[g, 1], q)

    start_fine(0)
    with jax.named_scope('barrier'):
        pl.semaphore_wait(barrier, 6)
    for copy in fine(A, 0, 0):
        copy.start()

    @pl.loop(1, chunks)
    def _(c):
        with jax.named_scope('load'):
            start_fine(c)
        for copy in fine(A, 0, c):
            copy.start()

    with jax.named_scope('prologue'):
        prologue()
    for copy in diagonals():
        copy.start()

    @pl.loop(0, chunks)
    def _(c):
        fine_inner(A, c)

    @pl.loop(0, chunks)
    def _(c):
        with jax.named_scope('w0'):
            fine_wait(0, c)
        with jax.named_scope('first'):
            first_pass(c)
        for copy in fine(F, 1, c):
            copy.start()
        fine_inner(F, c)

    @pl.loop(0, chunks)
    def _(c):
        with jax.named_scope('w1'):
            fine_wait(1, c)
        with jax.named_scope('second'):
            second_pass(c)
        for copy in one(c):
            copy.start()
        coarse_inner(U1a, 2, c)

    for copy in gather_diagonal():
        copy.start()

    whole(W1R, got_w.at[1])
    whole(WZR, got_w.at[2])

    @pl.loop(0, halves)
    def _(h):
        @pl.loop(0, chunks // halves)
        def _(i):
            c = h * (chunks // halves) + i
            with jax.named_scope('w2'):
                whole(stage.at[pl.ds(0, 4 * (cx + cy) // 2 + 3), pl.ds(0, deep)], one_got.at[c, 0])
            with jax.named_scope('sweep'):
                unpack_faces(c)
                coarse_outer(first_cells(Z1R[0, c], Z1R[1, c]), c)

                @pl.loop(0, inner)
                def _(j):
                    rows = tile(c * inner + j)
                    for X in range(cx):
                        for Y in range(cy):
                            k = X * cy + Y
                            total = beside_xy(U1a, X + 2, Y + 2, rows) + ZS[k, rows, :]
                            value = U1a[X + 2, Y + 2, rows, :] * third
                            U1b[X + 1, Y + 1, rows, :] = value + W1[X, Y] * (B1[k, rows, :] + 0.125 * total)

                coarse_inner(U1b, 1, c)
                ring_inner(c)
            with jax.named_scope('w3'):
                whole(ZD.at[:, :, c], one_got.at[c, 1])
            with jax.named_scope('ring'):
                outside(c)

                @pl.loop(0, inner)
                def _(j):
                    rows = tile(c * inner + j)
                    for side in range(4):
                        for t in range(4):
                            (x, y), _k = ring(side, t)
                            total = beside_xy(U1a, x + 2, y + 2, rows) + ZRING[4 * side + t, pl.ds(pl.multiple_of(j * SUB, SUB), SUB), :]
                            value = U1a[x + 2, y + 2, rows, :] * (1.0 + third)
                            U1b[x + 1, y + 1, rows, :] = value + 0.125 * shape(W1R[side, t:t + 1, :]) * total

            with jax.named_scope('residue'):
                coarse_outer(HU[c], c)

                @pl.loop(0, inner)
                def _(j):
                    rows = tile(c * inner + j)
                    for X in range(ex):
                        for Y in range(ey):
                            sums = None
                            for dx in range(2):
                                for dy in range(2):
                                    x, y = 2 * X + dx, 2 * Y + dy
                                    k = x * cy + y
                                    total = beside_xy(U1b, x + 1, y + 1, rows) + ZS[k, rows, :]
                                    residue = B1[k, rows, :] - D1[k] * U1b[x + 1, y + 1, rows, :] + 0.125 * total
                                    B1[k, rows, :] = residue
                                    sums = residue if sums is None else sums + residue
                            B2[X * ey + Y, rows, :] = sums

        with jax.named_scope('weave'):
            parts = []
            for g in range(share):
                part = woven([0.5 * pair_sum(B2[q, tile(h * share + g), :], 2) for q in range(ex * ey)])
                MPS[h, g] = part
                parts.append(part)
            parts.append(WPS[...])
            low = high = None
            for g, part in enumerate(parts):
                here = (lane() >= EDGE * g) & (lane() < EDGE * (g + 1))
                up, down = roll(part, EDGE * g + EDGE), roll(part, EDGE * g)
                high = up if high is None else jnp.where(here, up, high)
                low = down if low is None else jnp.where(here, down, low)
            EPS[h, 0], EPS[h, 1] = high, low
        for copy in ends_far(h) + ends(h) + gather(h):
            copy.start()

    whole(WPR, got_w.at[0])

    def store(g):
        part = pl.ds(g * SUB, SUB)
        return pltpu.make_async_copy(stage.at[part], out_ref.at[part], sent.at[8])

    @pl.loop(0, halves)
    def _(h):
        with jax.named_scope('w5'):
            whole(MPR.at[h], got.at[h, 0])
        level_two(h, True)
        with jax.named_scope('w6'):
            whole(EPR.at[h], got.at[h, 1])
            whole(XPR.at[h], got.at[h, 2])
        with jax.named_scope('two'):
            level_two(h, False)
        with jax.named_scope('last'):
            @pl.loop(0, share)
            def _(i):
                g = h * share + i
                c, j = g // inner, g % inner
                rows = tile(g)
                band = pl.ds(pl.multiple_of(j * SUB, SUB), SUB)
                for X in range(cx):
                    levels = []
                    for Y in range(cy):
                        k, q, r = X * cy + Y, X // 2 + 1, Y // 2 + 1
                        t = TT[q, r, rows, :]
                        outer = TT[q + 2 * (X % 2) - 1, r, rows, :] + TT[q, r + 2 * (Y % 2) - 1, rows, :]
                        outer = outer + TZ[(q - 1) * ey + r - 1, rows, :] + 3.0 * t
                        value = U1b[X + 1, Y + 1, rows, :] + t * (1.0 - jacobi_weight)
                        levels.append(value + W1[X, Y] * (B1[k, rows, :] + 0.125 * outer))
                    for x in (2 * X, 2 * X + 1):
                        values = turn([S2[c, x, y, band, :] + levels[y // 2] for y in range(ny)])
                        for i in range(SUB):
                            stage[g * SUB + i, x * ny:(x + 1) * ny, :] = values[i]
                store(g).start()

    with jax.named_scope('sent'):
        whole(S2, sent.at[0])
        whole(FZS, sent.at[1])
        whole(X1S, sent.at[2])
        whole(Z1R, sent.at[3])
        whole(MPR, sent.at[4])
        whole(WPR, sent.at[5])
        whole(EPS, sent.at[6])
        whole(XPR, sent.at[7])
        whole(stage, sent.at[8])
        whole(CS, sent.at[9])
        whole(ZD, sent.at[10])
        whole(W1R, sent.at[11])
        whole(WZR, sent.at[12])


def local(orbitals, potential, centre, half_width):
    bands, nx, ny, nz = orbitals.shape
    chunks = 4
    deep = bands // chunks
    cx, cy, ex, ey = nx // 2, ny // 2, nx // 4, ny // 4
    groups = bands // SUB
    vmem = lambda *s: pltpu.VMEM(s, jnp.float32)
    dma = lambda *s: pltpu.SemaphoreType.DMA(s)
    out = pl.pallas_call(
        functools.partial(kernel, bands, nx, ny, chunks),
        name="filter_orbitals",
        out_shape=jax.ShapeDtypeStruct((bands, nx * ny, nz), jnp.float32),
        in_specs=[pl.BlockSpec(memory_space=pltpu.HBM)] * 4,
        out_specs=pl.BlockSpec(memory_space=pl.ANY),
        scratch_shapes=[
            vmem(bands, nx * ny, nz), vmem(nx * ny, nz), pltpu.SMEM((bands,), jnp.float32), pltpu.SMEM((bands,), jnp.float32),
            vmem(nx * ny, bands, nz), vmem(cx * cy, deep, nz),
            vmem(chunks, nx + 2, ny + 2, deep, nz), vmem(chunks, nx + 2, ny + 2, deep, nz), vmem(chunks, nx, ny, deep, nz),
            vmem(nx * ny, SUB, nz), vmem(cx * cy, SUB, nz), vmem(cx, cy, SUB, nz),
            vmem(groups, SUB, nz), vmem(groups, SUB, nz),
            vmem(2, 2, chunks, deep // 16, SUB, nz), vmem(2, 2, chunks, deep // 16, SUB, nz),
            vmem(cx * cy, bands, nz),
            vmem(cx + 4, cy + 4, bands, nz), vmem(cx + 2, cy + 2, bands, nz), vmem(ex * ey, bands, nz),
            vmem(2, 4, cy // 2, bands, nz), vmem(2, 4, cy // 2, bands, nz),
            vmem(chunks, 2, SUB, nz), vmem(2, chunks, SUB, nz),
            vmem(4, chunks, SUB, nz), vmem(4, chunks, SUB, nz), vmem(4, 2, chunks, SUB, nz), vmem(chunks, SUB, nz),
            vmem(4, SUB, nz), vmem(4, SUB, nz), vmem(SUB, nz), vmem(2, SUB, nz), vmem(chunks, SUB, nz), vmem(16, deep, nz),
            vmem(2, groups // 2, SUB, nz), vmem(2, 10, groups // 2, SUB, nz), vmem(SUB, nz), vmem(10, SUB, nz),
            vmem(2, 2, SUB, nz), vmem(2, 2, SUB, nz), vmem(2, 8, 2, SUB, nz),
            vmem(9, groups // 2 + 1, SUB, nz), vmem(groups // 2, 14, SUB, nz), vmem(groups // 2, 14, SUB, nz),
            vmem(ex + 2, ey + 2, bands, nz), vmem(ex * ey, bands, nz),
            dma(chunks), dma(3), dma(13), dma(2, chunks), dma(chunks, 2), dma(2, 3), dma(3),
        ],
        compiler_params=pltpu.CompilerParams(collective_id=0, has_side_effects=True, vmem_limit_bytes=48 * 1024 * 1024),
    )(*(pltpu.with_memory_space_constraint(a, pltpu.HBM) for a in (orbitals.reshape(bands, nx * ny, nz), potential.reshape(nx * ny, nz), centre, half_width)))
    return out.reshape(bands, nx, ny, nz)


def solution(mesh):
    in_specs = (P(None, "gx", "gy", "gz"), P("gx", "gy", "gz"), P(), P())
    out_specs = P(None, "gx", "gy", "gz")
    return jax.shard_map(local, mesh=mesh, in_specs=in_specs, out_specs=out_specs, check_vma=False)
```

```python
import functools
import math

import jax
import jax.numpy as jnp
from jax import lax
from jax.experimental import pallas as pl
from jax.experimental.pallas import tpu as pltpu
from jax.sharding import PartitionSpec as P

MESH = pl.DeviceIdType.MESH
shift_mass = 0.05
jacobi_weight = 2.0 / 3.0
SUB, LANES = 8, 128
AXES = ("gx", "gy", "gz")
SIDES = (("gx", 1), ("gx", -1), ("gy", 1), ("gy", -1), ("gz", 1), ("gz", -1))
RING = ((1, 0), (-1, 0), (0, 1), (0, -1), (1, 1), (1, -1), (-1, 1), (-1, -1), (2, 0), (0, 2))
NEAR = RING[:8]
CROSS = RING[:4]
CORNERS = RING[4:8]
EDGE = 16


def lane():
    return lax.broadcasted_iota(jnp.int32, (SUB, LANES), 1)


def sublane():
    return lax.broadcasted_iota(jnp.int32, (SUB, LANES), 0)


def roll(value, shift):
    shift = shift % LANES
    return value if shift == 0 else pltpu.roll(value, shift, 1)


def turn(rows):
    at, rows = sublane(), list(rows)
    for d in (4, 2, 1):
        low = (at & d) == 0
        for i in range(SUB):
            if i & d == 0:
                a, b = rows[i], rows[i + d]
                rows[i] = jnp.where(low, a, pltpu.roll(b, d, 0))
                rows[i + d] = jnp.where(low, pltpu.roll(a, SUB - d, 0), b)
    return rows


def woven(columns):
    at = lane() & 3
    total = columns[3]
    for q in range(3):
        total = jnp.where(at == q, columns[q], total)
    return total


def spread(low, high, q):
    at = lane() & 3
    total = roll(high, 3 - q)
    for i, value in ((0, low), (1, low), (2, high)):
        total = jnp.where(at == i, roll(value, i - q), total)
    return total


def beside(own, low, high, bit):
    return jnp.where((lane() & bit) == 0, roll(own + low, -bit), roll(own + high, bit))


def below(main, other):
    return roll(jnp.where(lane() >= LANES - 4, other, main), 4)


def above(main, other):
    return roll(jnp.where(lane() < 4, other, main), -4)


def packed(total, value, start, width):
    at = lane()
    moved = roll(value, start + width // 2)
    if total is None:
        return moved
    return jnp.where((at >= start) & (at < start + width), moved, total)


def inner_z(value, width):
    at, half = lane(), width // 2
    return jnp.where(at < half, 0.0, roll(value, half)) + jnp.where(at >= LANES - half, 0.0, roll(value, -half))


def outer_z(rims, start, width):
    half = width // 2
    return jnp.where(((lane() + half) & (LANES - 1)) < width, roll(rims, -(start + half)), 0.0)


def met(from_left, from_right, width):
    half = width // 2
    return jnp.where((lane() & half) != 0, roll(from_left, half), roll(from_right, -half))


def first_cells(from_left, from_right):
    return jnp.where((lane() & 2) == 0, from_right, roll(from_left, 2))


def pair_sum(value, cell):
    at = lane()
    return value + jnp.where((at & cell) == 0, roll(value, -cell), roll(value, cell))


def kernel(bands, nx, ny, chunks, orb_hbm, pot_hbm, mid_hbm, half_hbm, out_ref,
           stage, pot_ref, mid_ref, half_ref, ZS, TS, A, F, S2, DG, D1, W1, MID, INV, FZS, FZR,
           B1, U1a, U1b, B2, X1S, X1R, Z1S, Z1R, CS, CR, ZD, ENDS, W1S, W1R, WZS, WZR, HU, ZRING, MPS, MPR, WPS, WPR, EPS, EPR, XPR, XE, PA, PB, TT, TZ,
           in_sem, par_sem, sent, fine_got, one_got, got, got_w):
    third = 1.0 - jacobi_weight
    deep = bands // chunks
    inner = deep // SUB
    groups = bands // SUB
    halves = 2
    share = groups // halves
    cx, cy = nx // 2, ny // 2
    ex, ey = nx // 4, ny // 4
    peers = []
    for axis, step in SIDES:
        n = lax.axis_size(axis)
        peers.append({axis: lax.rem(lax.axis_index(axis) + (n + step), n)})
    around_xy = []
    for step in RING:
        place = {}
        for axis, k in zip(AXES, step):
            n = lax.axis_size(axis)
            place[axis] = lax.rem(lax.axis_index(axis) + (n + k), n)
        around_xy.append(place)
    around_z = []
    for step in NEAR:
        for k in (1, -1):
            place = {}
            for axis, move in zip(AXES, step + (k,)):
                n = lax.axis_size(axis)
                place[axis] = lax.rem(lax.axis_index(axis) + (n + move), n)
            around_z.append(place)

    def load(c):
        part = pl.ds(c * deep, deep)
        return pltpu.make_async_copy(orb_hbm.at[part], stage.at[part], in_sem.at[c])

    params = [pltpu.make_async_copy(a, b, par_sem.at[i])
              for i, (a, b) in enumerate(((pot_hbm, pot_ref), (mid_hbm, mid_ref), (half_hbm, half_ref)))]
    for copy in params:
        copy.start()
    for c in range(chunks):
        load(c).start()
    barrier = pltpu.get_barrier_semaphore()
    for peer in peers:
        pl.semaphore_signal(barrier, inc=1, device_id=peer, device_id_type=MESH)

    def shape(value):
        return jnp.broadcast_to(value, (SUB, LANES))

    def prologue():
        for copy in params:
            copy.wait()
        at = sublane()
        for g in range(groups):
            mid = jnp.full((SUB, LANES), mid_ref[g * SUB], jnp.float32)
            half = jnp.full((SUB, LANES), half_ref[g * SUB], jnp.float32)
            for s in range(1, SUB):
                mid = jnp.where(at == s, mid_ref[g * SUB + s], mid)
                half = jnp.where(at == s, half_ref[g * SUB + s], half)
            MID[g] = 6.0 - 2.0 * mid
            INV[g] = 0.5 / half
        ones = {}
        for X in range(cx):
            for Y in range(cy):
                total = None
                for dx in range(2):
                    for dy in range(2):
                        k = (2 * X + dx) * ny + 2 * Y + dy
                        row = shape(pot_ref[pl.ds(k, 1), :])
                        DG[k] = 2.0 * row
                        total = row if total is None else total + row
                one = 0.125 * pair_sum(total, 1)
                ones[X, Y] = one
                diagonal = 0.75 + one + shift_mass
                D1[X * cy + Y] = diagonal
                W1[X, Y] = jacobi_weight / diagonal
        two_diagonals = []
        for X in range(ex):
            for Y in range(ey):
                total = (ones[2 * X, 2 * Y] + ones[2 * X + 1, 2 * Y]) + (ones[2 * X, 2 * Y + 1] + ones[2 * X + 1, 2 * Y + 1])
                diagonal = 0.1875 + 0.125 * pair_sum(total, 2) + shift_mass
                two_diagonals.append(jacobi_weight / diagonal)
        WPS[...] = woven(two_diagonals)
        total = None
        for j in range(2):
            for k in range(cx * cy):
                total = packed(total, W1[k // cy, k % cy], 4 * (j * cx * cy + k), 4)
        WZS[...] = total
        for d in range(4):
            face = [W1[((cx - 1, t), (0, t), (t, cy - 1), (t, 0))[d]] for t in range(4)]
            rows = face[0]
            for t in range(1, 4):
                rows = jnp.where(sublane() == t, face[t], rows)
            W1S[d] = rows

    def send(src, dst, s, r, d):
        return pltpu.make_async_remote_copy(
            src_ref=src, dst_ref=dst, send_sem=s, recv_sem=r, device_id=peers[d], device_id_type=MESH)

    def fine(buffer, rnd, c):
        ends = (
            (buffer.at[c, nx, pl.ds(1, ny)], buffer.at[c, 0, pl.ds(1, ny)]),
            (buffer.at[c, 1, pl.ds(1, ny)], buffer.at[c, nx + 1, pl.ds(1, ny)]),
            (buffer.at[c, pl.ds(1, nx), ny], buffer.at[c, pl.ds(1, nx), 0]),
            (buffer.at[c, pl.ds(1, nx), 1], buffer.at[c, pl.ds(1, nx), ny + 1]),
            (FZS.at[rnd, 0, c], FZR.at[rnd, 0, c]),
            (FZS.at[rnd, 1, c], FZR.at[rnd, 1, c]),
        )
        copies = [send(a, b, sent.at[d // 4], fine_got.at[rnd, c], d) for d, (a, b) in enumerate(ends)]
        return copies[4:] + copies[:4]

    def whole(ref, sem):
        pltpu.make_async_copy(ref, ref, sem).wait()

    def fine_wait(rnd, c):
        whole(stage.at[pl.ds(0, 2 * (nx + ny) + 1), pl.ds(0, deep)], fine_got.at[rnd, c])

    def fine_edges(rnd, c, totals):
        odd = (lane() & 1) != 0
        for i in range(inner // 2):
            a, b = totals[2 * i], totals[2 * i + 1]
            FZS[rnd, 0, c, i] = jnp.where(odd, roll(a, 1), b)
            FZS[rnd, 1, c, i] = jnp.where(odd, b, roll(a, -1))

    def fine_rims(rnd, c):
        odd = (lane() & 1) != 0
        rims = []
        for i in range(inner // 2):
            low, high = FZR[rnd, 0, c, i], FZR[rnd, 1, c, i]
            rims.append(jnp.where(odd, low, high))
            rims.append(jnp.where(odd, roll(low, 1), roll(high, -1)))
        return rims

    def start_fine(c):
        load(c).wait()
        totals = [None] * inner
        for j in range(inner):
            for x in range(nx):
                rows = turn([stage[c * deep + j * SUB + i, x * ny:(x + 1) * ny, :] for i in range(SUB)])
                for y in range(ny):
                    A[c, x + 1, y + 1, j * SUB:(j + 1) * SUB, :] = rows[y]
                    totals[j] = packed(totals[j], rows[y], 2 * (x * ny + y), 2)
        fine_edges(0, c, totals)

    def fine_inner(buffer, c):
        for j in range(inner):
            for x in range(nx):
                for y in range(ny):
                    value = buffer[c, x + 1, y + 1, j * SUB:(j + 1) * SUB, :]
                    ZS[x * ny + y, tile(c * inner + j), :] = inner_z(value, 2)

    def fine_outer(rnd, c):
        rims = fine_rims(rnd, c)
        for j in range(inner):
            for k in range(nx * ny):
                ZS[k, tile(c * inner + j), :] += outer_z(rims[j], 2 * k, 2)

    def apply(buffer, c, x, y, j):
        band = pl.ds(pl.multiple_of(j * SUB, SUB), SUB)
        v = buffer[c, x + 1, y + 1, band, :]
        total = buffer[c, x, y + 1, band, :] + buffer[c, x + 2, y + 1, band, :]
        total = total + buffer[c, x + 1, y, band, :] + buffer[c, x + 1, y + 2, band, :]
        total = total + ZS[x * ny + y, tile(c * inner + j), :]
        return (DG[x * ny + y] + MID[c * inner + j]) * v - total

    def first_pass(c):
        fine_outer(0, c)

        @pl.loop(0, inner)
        def _(j):
            inv = INV[c * inner + j]
            for x in range(nx):
                for y in range(ny):
                    F[c, x + 1, y + 1, pl.ds(pl.multiple_of(j * SUB, SUB), SUB), :] = apply(A, c, x, y, j) * inv

        totals = [None] * inner
        for j in range(inner):
            for x in range(nx):
                for y in range(ny):
                    totals[j] = packed(totals[j], F[c, x + 1, y + 1, j * SUB:(j + 1) * SUB, :], 2 * (x * ny + y), 2)
        fine_edges(1, c, totals)

    def second_pass(c):
        fine_outer(1, c)

        @pl.loop(0, inner)
        def _(j):
            band = pl.ds(pl.multiple_of(j * SUB, SUB), SUB)
            scale = 2.0 * INV[c * inner + j]
            for X in range(cx):
                for Y in range(cy):
                    total = None
                    for dx in range(2):
                        for dy in range(2):
                            x, y = 2 * X + dx, 2 * Y + dy
                            value = apply(F, c, x, y, j) * scale - A[c, x + 1, y + 1, band, :]
                            S2[c, x, y, band, :] = value
                            total = value if total is None else total + value
                    TS[X * cy + Y, band, :] = total

        totals = [None, None]
        for j in range(inner):
            rows = pl.ds(pl.multiple_of(c * deep + j * SUB, SUB), SUB)
            for X in range(cx):
                for Y in range(cy):
                    k = X * cy + Y
                    source = 0.5 * pair_sum(TS[k, j * SUB:(j + 1) * SUB, :], 1)
                    B1[k, rows, :] = source
                    level = W1[X, Y] * source
                    U1a[X + 2, Y + 2, rows, :] = level
                    start = 4 * (j * cx * cy + k)
                    moved = roll(level, start + 2)
                    here = ((lane() + (LANES - start + 2)) & (LANES - 1)) < 8
                    totals[k % 2] = moved if totals[k % 2] is None else jnp.where(here, moved, totals[k % 2])
            even = (lane() & 1) == 0
            for n in range(2):
                lines = ([(cx - 1 - n, y) for y in range(cy)], [(n, y) for y in range(cy)],
                         [(x, cy - 1 - n) for x in range(cx)], [(x, n) for x in range(cx)])
                for d, line in enumerate(lines):
                    for p in range(len(line) // 2):
                        (x0, y0), (x1, y1) = line[2 * p], line[2 * p + 1]
                        X1S[n, d, p, rows, :] = jnp.where(even, U1a[x0 + 2, y0 + 2, rows, :], U1a[x1 + 2, y1 + 2, rows, :])
        turn_even = (lane() & 4) == 0
        near = jnp.where(turn_even, totals[0], totals[1])
        ENDS[c] = near
        inward = [jnp.where((lane() & 2) == 0, roll(t, 2), roll(t, -2)) for t in totals]
        far = jnp.where(turn_even, inward[0], inward[1])
        Z1S[c, 0] = jnp.where((lane() & 2) == 0, near, roll(far, 2))
        Z1S[c, 1] = jnp.where((lane() & 2) == 0, roll(near, -2), far)
        for i, (a, b) in enumerate(CORNERS):
            x, y = cx + 1 if a > 0 else 2, cy + 1 if b > 0 else 2
            CS[i, c] = jnp.where((lane() & 1) == 0, U1a[x, y, tile(c * inner), :], U1a[x, y, tile(c * inner + 1), :])

    def one(c):
        rows = pl.ds(pl.multiple_of(c * deep, deep), deep)
        copies = []
        for i, (a, b) in enumerate(CROSS):
            for d in range(2):
                copies.append(remote(Z1S.at[c, d], ZD.at[slot((-a, -b)), d, c], sent.at[1], one_got.at[c, 1],
                                     around_z[2 * i + d]))
        copies += [send(Z1S.at[c, d - 4], Z1R.at[d - 4, c], sent.at[1], one_got.at[c, 0], d) for d in (4, 5)]
        for i in range(4):
            copies.append(remote(CS.at[i, c], CR.at[i, c], sent.at[1], one_got.at[c, 0], around_xy[4 + i]))
        return copies + [send(X1S.at[:, d, :, rows], X1R.at[:, d, :, rows], sent.at[2], one_got.at[c, 0], d)
                         for d in range(4)]

    def diagonals():
        copies = [send(W1S.at[d], W1R.at[d ^ 1], sent.at[1], got_w.at[1], d) for d in range(4)]
        return copies + [send(WZS, WZR.at[d - 4], sent.at[1], got_w.at[2], d) for d in (4, 5)]

    def slot(step):
        return RING.index(step) if step in RING else RING.index((abs(step[0]), abs(step[1])))

    def remote(src, dst, s, r, place):
        return pltpu.make_async_remote_copy(
            src_ref=src, dst_ref=dst, send_sem=s, recv_sem=r, device_id=place, device_id_type=MESH)

    def gather(h):
        copies = []
        for i, (a, b) in enumerate(RING):
            copies.append(remote(MPS.at[h], MPR.at[h, slot((-a, -b))], sent.at[2], got.at[h, 0], around_xy[i]))
        return copies

    def gather_diagonal():
        copies = []
        for i, (a, b) in enumerate(RING):
            copies.append(remote(WPS, WPR.at[slot((-a, -b))], sent.at[1], got_w.at[0], around_xy[i]))
        return copies

    def ends(h):
        return [send(EPS.at[h, d], EPR.at[h, d], sent.at[1], got.at[h, 1], 4 + d) for d in range(2)]

    def ends_far(h):
        copies = []
        for i, (a, b) in enumerate(NEAR):
            for d in range(2):
                copies.append(remote(EPS.at[h, d], XPR.at[h, slot((-a, -b)), d], sent.at[2], got.at[h, 2],
                                     around_z[2 * i + d]))
        return copies

    def tile(g):
        return pl.ds(g * SUB if isinstance(g, int) else pl.multiple_of(g * SUB, SUB), SUB)

    def coarse_inner(buffer, at, c):
        for j in range(inner):
            for X in range(cx):
                for Y in range(cy):
                    ZS[X * cy + Y, tile(c * inner + j), :] = inner_z(buffer[X + at, Y + at, tile(c * inner + j), :], 4)

    def coarse_outer(rims, c):
        for j in range(inner):
            for k in range(cx * cy):
                ZS[k, tile(c * inner + j), :] += outer_z(rims, 4 * (j * cx * cy + k), 4)

    def ring_inner(c):
        for j in range(inner):
            for i in range(4):
                for t in range(4):
                    (x, y), _ = ring(i, t)
                    value = U1a[x + 2, y + 2, tile(c * inner + j), :]
                    ZRING[4 * i + t, j * SUB:(j + 1) * SUB, :] = inner_z(value, 4)

    def unpack_faces(c):
        even = (lane() & 1) == 0
        for j in range(inner):
            rows = tile(c * inner + j)
            for n in range(2):
                lines = ([(1 - n, y + 2) for y in range(cy)], [(cx + 2 + n, y + 2) for y in range(cy)],
                         [(x + 2, 1 - n) for x in range(cx)], [(x + 2, cy + 2 + n) for x in range(cx)])
                for d, line in enumerate(lines):
                    for p in range(len(line) // 2):
                        both = X1R[n, d, p, rows, :]
                        (x0, y0), (x1, y1) = line[2 * p], line[2 * p + 1]
                        U1a[x0, y0, rows, :] = jnp.where(even, both, roll(both, 1))
                        U1a[x1, y1, rows, :] = jnp.where(even, roll(both, -1), both)
        for i, (a, b) in enumerate(CORNERS):
            both = CR[i, c]
            x, y = 1 if a > 0 else cx + 2, 1 if b > 0 else cy + 2
            U1a[x, y, tile(c * inner), :] = jnp.where(even, both, roll(both, 1))
            U1a[x, y, tile(c * inner + 1), :] = jnp.where(even, roll(both, -1), both)

    def ring(i, t):
        return (((cx, t), t), ((-1, t), (cx - 1) * cy + t), ((t, cy), t * cy), ((t, -1), t * cy + cy - 1))[i]

    def outside(c):
        rims = [first_cells(ZD[i, 0, c], ZD[i, 1, c]) for i in range(4)]
        for j in range(inner):
            for i in range(4):
                for t in range(4):
                    _, k = ring(i, t)
                    ZRING[4 * i + t, j * SUB:(j + 1) * SUB, :] += outer_z(rims[i], 4 * (j * cx * cy + k), 4)
        own = first_cells(Z1R[0, c], Z1R[1, c])
        X, Y = (lane() >> 4) & 3, (lane() >> 2) & 3
        total = jnp.where(X == 0, roll(rims[1], -48), roll(own, 16)) + jnp.where(X == 3, roll(rims[0], 48), roll(own, -16))
        total = total + jnp.where(Y == 0, roll(rims[3], -12), roll(own, 4)) + jnp.where(Y == 3, roll(rims[2], 12), roll(own, -4))
        second_cells = jnp.where((lane() & 2) == 0, roll(Z1R[1, c], -2), Z1R[0, c])
        total = total + ENDS[c] + second_cells
        HU[c] = own * (1.0 + third) + 0.125 * met(WZR[0], WZR[1], 4) * total

    def beside_xy(buffer, x, y, rows):
        total = buffer[x - 1, y, rows, :] + buffer[x + 1, y, rows, :]
        return total + buffer[x, y - 1, rows, :] + buffer[x, y + 1, rows, :]

    def level_two(h, early):
        at = lane()
        for b in range(0 if early else 9):
            low, high = (EPR[h, 0], EPR[h, 1]) if b == 8 else (XPR[h, b, 0], XPR[h, b, 1])
            for g in range(share + 1):
                XE[b, g] = jnp.where(at < EDGE, roll(high, -EDGE * g), roll(low, LANES - EDGE - EDGE * g))

        def main(step, g):
            if isinstance(g, int) and g == share:
                return WPS[...] if step == (0, 0) else WPR[slot(step)]
            return MPS[h, g] if step == (0, 0) else MPR[h, slot(step), g]

        def edge(step, g):
            return XE[8 if step == (0, 0) else slot(step), g]

        def know(step):
            return step == (0, 0) or step in RING or (abs(step[0]), abs(step[1])) in RING

        def total(value, other, near):
            x = beside(value, near(-1, 0), near(1, 0), 2)
            y = beside(value, near(0, -1), near(0, 1), 1)
            return x + y + (below(value, other) + above(value, other))

        own = (0, 0)
        first_main = (own,) + NEAR
        first_edge = (own,) + CROSS
        for g in range(share):
            start = {}
            for step in first_main + RING[8:]:
                start[step, 0] = main(step, share) * main(step, g)
            for step in () if early else first_main:
                start[step, 1] = edge(step, share) * edge(step, g)

            def near_of(step, part, value):
                def near(a, b):
                    there = (step[0] + a, step[1] + b)
                    there = there if know(there) else step
                    there = there if there == own or there in RING else (abs(there[0]), abs(there[1]))
                    return start.get((there, part), value)
                return near

            for n, step in enumerate(first_main):
                value = start[step, 0]
                if early:
                    near = near_of(step, 0, value)
                    PA[g, n] = beside(value, near(-1, 0), near(1, 0), 2) + beside(value, near(0, -1), near(0, 1), 1)
                else:
                    PA[g, n] += below(value, start[step, 1]) + above(value, start[step, 1])
            if early:
                continue
            for n, step in enumerate(first_edge):
                value, other = start[step, 1], start[step, 0]
                PA[g, 9 + n] = total(value, other, near_of(step, 1, value))

        if early:
            return

        for g in range(share):
            for n, step in enumerate(first_main):
                w, b = main(step, share), main(step, g)
                PB[g, n] = (w * b) * (1.0 - jacobi_weight) + w * (b + 0.03125 * PA[g, n])
            for n, step in enumerate(first_edge):
                w, b = edge(step, share), edge(step, g)
                PB[g, 9 + n] = (w * b) * (1.0 - jacobi_weight) + w * (b + 0.03125 * PA[g, 9 + n])

        for g in range(share):
            def near_of(step, part, value):
                def near(a, b):
                    there = (step[0] + a, step[1] + b)
                    known = first_main if part == 0 else first_edge
                    return PB[g, 9 * part + known.index(there)] if there in known else value
                return near

            for n, step in enumerate(first_edge):
                value, other = PB[g, n], PB[g, 9 + n]
                PA[g, n] = total(value, other, near_of(step, 0, value))
            value, other = PB[g, 9], PB[g, 0]
            PA[g, 9] = total(value, other, near_of(own, 1, value))

        for g in range(share):
            for n, step in enumerate(first_edge):
                w, b = main(step, share), main(step, g)
                PB[g, n] = PB[g, n] * (1.0 - jacobi_weight) + w * (b + 0.03125 * PA[g, n])
            w, b = edge(own, share), edge(own, g)
            PB[g, 9] = PB[g, 9] * (1.0 - jacobi_weight) + w * (b + 0.03125 * PA[g, 9])

        for g in range(share):
            value, other = PB[g, 0], PB[g, 9]
            PA[g, 0] = below(value, other)
            PA[g, 1] = above(value, other)
            for X in range(ex):
                for Y in range(ey):
                    TT[X + 1, Y + 1, tile(h * share + g), :] = spread(value, value, 2 * X + Y)
            for n, (a, b) in enumerate(CROSS):
                value = PB[g, 1 + n]
                for k in range(2):
                    X, Y = (k, 0) if a == 0 else (0, k)
                    X, Y = (1 if a < 0 else X), (1 if b < 0 else Y)
                    TT[2 * a + X + 1, 2 * b + Y + 1, tile(h * share + g), :] = spread(value, value, 2 * X + Y)
        for g in range(share):
            for q in range(ex * ey):
                TZ[q, tile(h * share + g), :] = spread(PA[g, 0], PA[g, 1], q)

    start_fine(0)
    with jax.named_scope('barrier'):
        pl.semaphore_wait(barrier, 6)
    for copy in fine(A, 0, 0):
        copy.start()

    @pl.loop(1, chunks)
    def _(c):
        with jax.named_scope('load'):
            start_fine(c)
        for copy in fine(A, 0, c):
            copy.start()

    with jax.named_scope('prologue'):
        prologue()
    for copy in diagonals():
        copy.start()

    @pl.loop(0, chunks)
    def _(c):
        fine_inner(A, c)

    @pl.loop(0, chunks)
    def _(c):
        with jax.named_scope('w0'):
            fine_wait(0, c)
        with jax.named_scope('first'):
            first_pass(c)
        for copy in fine(F, 1, c):
            copy.start()
        fine_inner(F, c)

    @pl.loop(0, chunks)
    def _(c):
        with jax.named_scope('w1'):
            fine_wait(1, c)
        with jax.named_scope('second'):
            second_pass(c)
        for copy in one(c):
            copy.start()
        coarse_inner(U1a, 2, c)

    for copy in gather_diagonal():
        copy.start()

    whole(W1R, got_w.at[1])
    whole(WZR, got_w.at[2])

    @pl.loop(0, halves)
    def _(h):
        @pl.loop(0, chunks // halves)
        def _(i):
            c = h * (chunks // halves) + i
            with jax.named_scope('w2'):
                whole(stage.at[pl.ds(0, 4 * (cx + cy) // 2 + 3), pl.ds(0, deep)], one_got.at[c, 0])
            with jax.named_scope('sweep'):
                unpack_faces(c)
                coarse_outer(first_cells(Z1R[0, c], Z1R[1, c]), c)

                @pl.loop(0, inner)
                def _(j):
                    rows = tile(c * inner + j)
                    for X in range(cx):
                        for Y in range(cy):
                            k = X * cy + Y
                            total = beside_xy(U1a, X + 2, Y + 2, rows) + ZS[k, rows, :]
                            value = U1a[X + 2, Y + 2, rows, :] * third
                            U1b[X + 1, Y + 1, rows, :] = value + W1[X, Y] * (B1[k, rows, :] + 0.125 * total)

                coarse_inner(U1b, 1, c)
                ring_inner(c)
            with jax.named_scope('w3'):
                whole(ZD.at[:, :, c], one_got.at[c, 1])
            with jax.named_scope('ring'):
                outside(c)

                @pl.loop(0, inner)
                def _(j):
                    rows = tile(c * inner + j)
                    for side in range(4):
                        for t in range(4):
                            (x, y), _k = ring(side, t)
                            total = beside_xy(U1a, x + 2, y + 2, rows) + ZRING[4 * side + t, pl.ds(pl.multiple_of(j * SUB, SUB), SUB), :]
                            value = U1a[x + 2, y + 2, rows, :] * (1.0 + third)
                            U1b[x + 1, y + 1, rows, :] = value + 0.125 * shape(W1R[side, t:t + 1, :]) * total

            with jax.named_scope('residue'):
                coarse_outer(HU[c], c)

                @pl.loop(0, inner)
                def _(j):
                    rows = tile(c * inner + j)
                    for X in range(ex):
                        for Y in range(ey):
                            sums = None
                            for dx in range(2):
                                for dy in range(2):
                                    x, y = 2 * X + dx, 2 * Y + dy
                                    k = x * cy + y
                                    total = beside_xy(U1b, x + 1, y + 1, rows) + ZS[k, rows, :]
                                    residue = B1[k, rows, :] - D1[k] * U1b[x + 1, y + 1, rows, :] + 0.125 * total
                                    B1[k, rows, :] = residue
                                    sums = residue if sums is None else sums + residue
                            B2[X * ey + Y, rows, :] = sums

        with jax.named_scope('weave'):
            parts = []
            for g in range(share):
                part = woven([0.5 * pair_sum(B2[q, tile(h * share + g), :], 2) for q in range(ex * ey)])
                MPS[h, g] = part
                parts.append(part)
            parts.append(WPS[...])
            low = high = None
            for g, part in enumerate(parts):
                here = (lane() >= EDGE * g) & (lane() < EDGE * (g + 1))
                up, down = roll(part, EDGE * g + EDGE), roll(part, EDGE * g)
                high = up if high is None else jnp.where(here, up, high)
                low = down if low is None else jnp.where(here, down, low)
            EPS[h, 0], EPS[h, 1] = high, low
        for copy in ends_far(h) + ends(h) + gather(h):
            copy.start()

    whole(WPR, got_w.at[0])

    def store(g):
        part = pl.ds(g * SUB, SUB)
        return pltpu.make_async_copy(stage.at[part], out_ref.at[part], sent.at[3])

    @pl.loop(0, halves)
    def _(h):
        with jax.named_scope('w5'):
            whole(MPR.at[h], got.at[h, 0])
        level_two(h, True)
        with jax.named_scope('w6'):
            whole(EPR.at[h], got.at[h, 1])
            whole(XPR.at[h], got.at[h, 2])
        with jax.named_scope('two'):
            level_two(h, False)
        with jax.named_scope('last'):
            @pl.loop(0, share)
            def _(i):
                g = h * share + i
                c, j = g // inner, g % inner
                rows = tile(g)
                band = pl.ds(pl.multiple_of(j * SUB, SUB), SUB)
                for X in range(cx):
                    levels = []
                    for Y in range(cy):
                        k, q, r = X * cy + Y, X // 2 + 1, Y // 2 + 1
                        t = TT[q, r, rows, :]
                        outer = TT[q + 2 * (X % 2) - 1, r, rows, :] + TT[q, r + 2 * (Y % 2) - 1, rows, :]
                        outer = outer + TZ[(q - 1) * ey + r - 1, rows, :] + 3.0 * t
                        value = U1b[X + 1, Y + 1, rows, :] + t * (1.0 - jacobi_weight)
                        levels.append(value + W1[X, Y] * (B1[k, rows, :] + 0.125 * outer))
                    for x in (2 * X, 2 * X + 1):
                        values = turn([S2[c, x, y, band, :] + levels[y // 2] for y in range(ny)])
                        for i in range(SUB):
                            stage[g * SUB + i, x * ny:(x + 1) * ny, :] = values[i]
                store(g).start()

    with jax.named_scope('sent'):
        small = (FZS, Z1R, CS, ZD, W1R, WZR, WPR, EPS)
        large = (X1S, MPR, XPR)
        small, large = (sum(math.prod(ref.shape) for ref in refs) // (2 * SUB * LANES) for refs in (small, large))
        whole(S2, sent.at[0])
        whole(stage.at[pl.ds(0, small), pl.ds(0, 2 * SUB)], sent.at[1])
        whole(stage.at[pl.ds(0, large // 2), pl.ds(0, 4 * SUB)], sent.at[2])
        whole(stage, sent.at[3])


def local(orbitals, potential, centre, half_width):
    bands, nx, ny, nz = orbitals.shape
    chunks = 4
    deep = bands // chunks
    cx, cy, ex, ey = nx // 2, ny // 2, nx // 4, ny // 4
    groups = bands // SUB
    vmem = lambda *s: pltpu.VMEM(s, jnp.float32)
    dma = lambda *s: pltpu.SemaphoreType.DMA(s)
    out = pl.pallas_call(
        functools.partial(kernel, bands, nx, ny, chunks),
        name="filter_orbitals",
        out_shape=jax.ShapeDtypeStruct((bands, nx * ny, nz), jnp.float32),
        in_specs=[pl.BlockSpec(memory_space=pltpu.HBM)] * 4,
        out_specs=pl.BlockSpec(memory_space=pl.ANY),
        scratch_shapes=[
            vmem(bands, nx * ny, nz), vmem(nx * ny, nz), pltpu.SMEM((bands,), jnp.float32), pltpu.SMEM((bands,), jnp.float32),
            vmem(nx * ny, bands, nz), vmem(cx * cy, deep, nz),
            vmem(chunks, nx + 2, ny + 2, deep, nz), vmem(chunks, nx + 2, ny + 2, deep, nz), vmem(chunks, nx, ny, deep, nz),
            vmem(nx * ny, SUB, nz), vmem(cx * cy, SUB, nz), vmem(cx, cy, SUB, nz),
            vmem(groups, SUB, nz), vmem(groups, SUB, nz),
            vmem(2, 2, chunks, deep // 16, SUB, nz), vmem(2, 2, chunks, deep // 16, SUB, nz),
            vmem(cx * cy, bands, nz),
            vmem(cx + 4, cy + 4, bands, nz), vmem(cx + 2, cy + 2, bands, nz), vmem(ex * ey, bands, nz),
            vmem(2, 4, cy // 2, bands, nz), vmem(2, 4, cy // 2, bands, nz),
            vmem(chunks, 2, SUB, nz), vmem(2, chunks, SUB, nz),
            vmem(4, chunks, SUB, nz), vmem(4, chunks, SUB, nz), vmem(4, 2, chunks, SUB, nz), vmem(chunks, SUB, nz),
            vmem(4, SUB, nz), vmem(4, SUB, nz), vmem(SUB, nz), vmem(2, SUB, nz), vmem(chunks, SUB, nz), vmem(16, deep, nz),
            vmem(2, groups // 2, SUB, nz), vmem(2, 10, groups // 2, SUB, nz), vmem(SUB, nz), vmem(10, SUB, nz),
            vmem(2, 2, SUB, nz), vmem(2, 2, SUB, nz), vmem(2, 8, 2, SUB, nz),
            vmem(9, groups // 2 + 1, SUB, nz), vmem(groups // 2, 14, SUB, nz), vmem(groups // 2, 14, SUB, nz),
            vmem(ex + 2, ey + 2, bands, nz), vmem(ex * ey, bands, nz),
            dma(chunks), dma(3), dma(4), dma(2, chunks), dma(chunks, 2), dma(2, 3), dma(3),
        ],
        compiler_params=pltpu.CompilerParams(collective_id=0, has_side_effects=True, vmem_limit_bytes=48 * 1024 * 1024),
    )(*(pltpu.with_memory_space_constraint(a, pltpu.HBM) for a in (orbitals.reshape(bands, nx * ny, nz), potential.reshape(nx * ny, nz), centre, half_width)))
    return out.reshape(bands, nx, ny, nz)


def solution(mesh):
    in_specs = (P(None, "gx", "gy", "gz"), P("gx", "gy", "gz"), P(), P())
    out_specs = P(None, "gx", "gy", "gz")
    return jax.shard_map(local, mesh=mesh, in_specs=in_specs, out_specs=out_specs, check_vma=False)
```
